32 devices in a mesh: dp: 1 (over z), tp: 4 (over y), ep: 8 (over x, core).
Axes of the slice: x: 4, y: 4, z: 1, core: 2. Of those that a mesh axis runs over, the one named last changes fastest.
The devices are a block of a 4x4x8 slice.
Arguments:
- hidden_in: bfloat16 [1024, 2048], P(('dp', 'ep'))
- positions: int32 [1024], P(('dp', 'ep'))
- expert_ids: int32 [1024, 2], P(('dp', 'ep'))
- k_cache: bfloat16 [1024, 64, 4, 128], P(('dp', 'ep'), None, 'tp')
- v_cache: bfloat16 [1024, 64, 4, 128], P(('dp', 'ep'), None, 'tp')
- norm_in: bfloat16 [2048], replicated
- norm_res: bfloat16 [2048], replicated
- norm_post: bfloat16 [2048], replicated
- w_q: bfloat16 [2048, 4096], P(None, 'tp')
- w_k: bfloat16 [2048, 512], P(None, 'tp')
- w_v: bfloat16 [2048, 512], P(None, 'tp')
- w_o: bfloat16 [4096, 2048], P('tp')
- w_gate: bfloat16 [2048, 6144], P(None, 'tp')
- w_up: bfloat16 [2048, 6144], P(None, 'tp')
- w_down: bfloat16 [6144, 2048], P('tp')
- w_router: bfloat16 [2048, 128], replicated
- e_gate: bfloat16 [128, 2048, 768], P('ep', None, 'tp')
- e_up: bfloat16 [128, 2048, 768], P('ep', None, 'tp')
- e_down: bfloat16 [128, 768, 2048], P('ep', 'tp')
Outputs:
- output 1: bfloat16 [1024, 2048], P(('dp', 'ep'))
- output 2: bfloat16 [1024, 64, 4, 128], P(('dp', 'ep'), None, 'tp')
- output 3: bfloat16 [1024, 64, 4, 128], P(('dp', 'ep'), None, 'tp')
All inputs are finite; a program needn't handle non-finite values.
Results may differ from the reference program's by a relative error of at most 0.0136629.
Values are sent between devices in bfloat16 or wider.
A program may use at most 768 MiB of HBM per device.

```python
import jax
import jax.numpy as jnp
from jax import lax

TOKENS = 128
EP_SHARDS = 8
CACHE_LEN = 64
MODEL_DIM = 2048
Q_HEADS = 32
KV_HEADS = 4
HEAD_DIM = 128
DENSE_FF = 6144
EXPERTS = 128
EXPERT_FF = 768
ROPE_BASE = 10000
BATCH = TOKENS * EP_SHARDS
NORM_EPS = 1e-5


def draw_routes(route_key):
    mean_count = 2 * TOKENS // EP_SHARDS
    local_count = EXPERTS // EP_SHARDS
    sub_keys = jax.random.split(route_key, 5)
    shard_perm = jax.random.permutation(sub_keys[0], EP_SHARDS)
    lift_count = jax.random.randint(sub_keys[1], (EP_SHARDS, EP_SHARDS // 2), 0, mean_count + 1)
    lift_count = lift_count.at[0, 0].set(mean_count)
    paired = jnp.stack([lift_count, -lift_count], axis=-1).reshape(EP_SHARDS, EP_SHARDS)
    counts = mean_count + paired[:, jnp.argsort(shard_perm)]
    bounds = jnp.cumsum(counts, axis=1)
    slot_ids = jnp.arange(2 * TOKENS)
    dest_sorted = jnp.sum((bounds[:, None, :] <= slot_ids[None, :, None]).astype(jnp.int32), axis=2)

    def shuffle_tokens(sub_key):
        return jax.random.permutation(sub_key, TOKENS)

    token_perm = jax.vmap(shuffle_tokens)(jax.random.split(sub_keys[2], EP_SHARDS))
    first_dest = jnp.take_along_axis(dest_sorted, token_perm, axis=1)
    second_dest = jnp.take_along_axis(dest_sorted, token_perm + TOKENS, axis=1)
    swap_flag = jax.random.randint(sub_keys[3], (EP_SHARDS, TOKENS), 0, 2) == 1
    dest_pair = jnp.stack([jnp.where(swap_flag, second_dest, first_dest), jnp.where(swap_flag, first_dest, second_dest)], axis=-1)
    within = jax.random.randint(sub_keys[4], (EP_SHARDS, TOKENS, 2), 0, local_count)
    return (dest_pair * local_count + within).reshape(BATCH, 2).astype(jnp.int32)


def draw_matrix(sub_key, mat_shape, fan_in, factor):
    return (jax.random.normal(sub_key, mat_shape, jnp.float32) * (factor * fan_in ** -0.5)).astype(jnp.bfloat16)


def draw_expert_stack(stack_key, fan_in, fan_out):
    def one_expert(sub_key):
        return draw_matrix(sub_key, (fan_in, fan_out), fan_in, 1.0)
    return lax.map(one_expert, jax.random.split(stack_key, EXPERTS))


def draw_gain(sub_key):
    return jax.random.uniform(sub_key, (MODEL_DIM,), jnp.float32, 0.5, 1.5).astype(jnp.bfloat16)


def setup_inputs(seed: int = 0, part: int = 0) -> dict:
    part_key = jax.random.fold_in(jax.random.key(seed), part)
    part_keys = jax.random.split(part_key, 5)
    weight_keys = jax.random.split(jax.random.key(seed + 1), 15)
    attn_width = Q_HEADS * HEAD_DIM
    kv_width = KV_HEADS * HEAD_DIM
    cache_shape = (BATCH, CACHE_LEN, KV_HEADS, HEAD_DIM)
    return {
        'hidden_in': jax.random.normal(part_keys[0], (BATCH, MODEL_DIM), jnp.float32).astype(jnp.bfloat16),
        'positions': jax.random.randint(part_keys[1], (BATCH,), CACHE_LEN // 2, CACHE_LEN).at[0].set(CACHE_LEN - 1).astype(jnp.int32),
        'expert_ids': draw_routes(part_keys[2]),
        'k_cache': jax.random.normal(part_keys[3], cache_shape, jnp.float32).astype(jnp.bfloat16),
        'v_cache': jax.random.normal(part_keys[4], cache_shape, jnp.float32).astype(jnp.bfloat16),
        'norm_in': draw_gain(weight_keys[0]),
        'norm_res': draw_gain(weight_keys[1]),
        'norm_post': draw_gain(weight_keys[2]),
        'w_q': draw_matrix(weight_keys[3], (MODEL_DIM, attn_width), MODEL_DIM, 1.0),
        'w_k': draw_matrix(weight_keys[4], (MODEL_DIM, kv_width), MODEL_DIM, 1.0),
        'w_v': draw_matrix(weight_keys[5], (MODEL_DIM, kv_width), MODEL_DIM, 1.0),
        'w_o': draw_matrix(weight_keys[6], (attn_width, MODEL_DIM), attn_width, 0.5 * CACHE_LEN ** 0.5),
        'w_gate': draw_matrix(weight_keys[7], (MODEL_DIM, DENSE_FF), MODEL_DIM, 1.0),
        'w_up': draw_matrix(weight_keys[8], (MODEL_DIM, DENSE_FF), MODEL_DIM, 1.0),
        'w_down': draw_matrix(weight_keys[9], (DENSE_FF, MODEL_DIM), DENSE_FF, 1.0),
        'w_router': draw_matrix(weight_keys[10], (MODEL_DIM, EXPERTS), MODEL_DIM, 1.0),
        'e_gate': draw_expert_stack(weight_keys[11], MODEL_DIM, EXPERT_FF),
        'e_up': draw_expert_stack(weight_keys[12], MODEL_DIM, EXPERT_FF),
        'e_down': draw_expert_stack(weight_keys[13], EXPERT_FF, MODEL_DIM),
    }


def rms_norm(values, gain_vec):
    wide_vals = values.astype(jnp.float32)
    inv_rms = lax.rsqrt(jnp.mean(wide_vals * wide_vals, axis=-1, keepdims=True) + NORM_EPS)
    return (wide_vals * inv_rms * gain_vec.astype(jnp.float32)).astype(jnp.bfloat16)


def rope_rotate(values, positions):
    half_dim = HEAD_DIM // 2
    inv_freq = 1.0 / (ROPE_BASE ** (jnp.arange(0, HEAD_DIM, 2, dtype=jnp.float32) / HEAD_DIM))
    angles = positions.astype(jnp.float32)[:, None] * inv_freq[None, :]
    cosine = jnp.cos(angles)[:, None, :]
    sine_part = jnp.sin(angles)[:, None, :]
    first_half = values[..., :half_dim]
    second_half = values[..., half_dim:]
    return jnp.concatenate([first_half * cosine - second_half * sine_part, second_half * cosine + first_half * sine_part], axis=-1)


def reference(hidden_in, positions, expert_ids, k_cache, v_cache, norm_in, norm_res, norm_post, w_q, w_k, w_v, w_o, w_gate, w_up, w_down, w_router, e_gate, e_up, e_down):
    group_size = Q_HEADS // KV_HEADS
    normed = rms_norm(hidden_in, norm_in)
    q_proj = jnp.dot(normed, w_q, preferred_element_type=jnp.float32).reshape(BATCH, Q_HEADS, HEAD_DIM)
    k_proj = jnp.dot(normed, w_k, preferred_element_type=jnp.float32).reshape(BATCH, KV_HEADS, HEAD_DIM)
    v_new = jnp.dot(normed, w_v, preferred_element_type=jnp.float32).astype(jnp.bfloat16).reshape(BATCH, KV_HEADS, HEAD_DIM)
    q_rot = rope_rotate(q_proj, positions).astype(jnp.bfloat16)
    k_rot = rope_rotate(k_proj, positions).astype(jnp.bfloat16)
    slot_hit = (jnp.arange(CACHE_LEN)[None, :] == positions[:, None])[:, :, None, None]
    k_out = jnp.where(slot_hit, k_rot[:, None], k_cache)
    v_out = jnp.where(slot_hit, v_new[:, None], v_cache)

    def attend_token(operands):
        q_tok, k_tok, v_tok, pos_tok = operands
        q_grp = q_tok.reshape(KV_HEADS, group_size, HEAD_DIM).astype(jnp.float32)
        scores = jnp.einsum('kgd,tkd->kgt', q_grp, k_tok.astype(jnp.float32)) * (HEAD_DIM ** -0.5)
        visible = jnp.arange(CACHE_LEN)[None, None, :] <= pos_tok
        attn_probs = jax.nn.softmax(jnp.where(visible, scores, -jnp.inf), axis=-1)
        attn_probs = attn_probs.astype(jnp.bfloat16).astype(jnp.float32)
        mixed_vals = jnp.einsum('kgt,tkd->kgd', attn_probs, v_tok.astype(jnp.float32))
        return mixed_vals.astype(jnp.bfloat16).reshape(Q_HEADS * HEAD_DIM)

    attn_mix = lax.map(attend_token, (q_rot, k_out, v_out, positions))
    hidden_mid = (hidden_in.astype(jnp.float32) + jnp.dot(attn_mix, w_o, preferred_element_type=jnp.float32)).astype(jnp.bfloat16)
    res_in = rms_norm(hidden_mid, norm_res)
    gate_val = jnp.dot(res_in, w_gate, preferred_element_type=jnp.float32)
    up_val = jnp.dot(res_in, w_up, preferred_element_type=jnp.float32)
    dense_out = jnp.dot((jax.nn.silu(gate_val) * up_val).astype(jnp.bfloat16), w_down, preferred_element_type=jnp.float32)
    moe_in = rms_norm(hidden_in, norm_post)
    gate_probs = jax.nn.softmax(jnp.dot(moe_in, w_router, preferred_element_type=jnp.float32), axis=-1)
    picked = jnp.take_along_axis(gate_probs, expert_ids, axis=1)
    route_wts = picked / jnp.sum(picked, axis=1, keepdims=True)

    def expert_token(operands):
        row_vec, id_pair, wt_pair = operands
        moe_sum = jnp.zeros((MODEL_DIM,), jnp.float32)
        for choice in range(2):
            expert = id_pair[choice]
            gate_e = jnp.dot(row_vec[None, :], e_gate[expert], preferred_element_type=jnp.float32)
            up_e = jnp.dot(row_vec[None, :], e_up[expert], preferred_element_type=jnp.float32)
            act_e = (jax.nn.silu(gate_e) * up_e).astype(jnp.bfloat16)
            moe_sum = moe_sum + wt_pair[choice] * jnp.dot(act_e, e_down[expert], preferred_element_type=jnp.float32)[0]
        return moe_sum

    moe_out = lax.map(expert_token, (moe_in, expert_ids, route_wts))
    hidden_out = (hidden_mid.astype(jnp.float32) + dense_out + moe_out).astype(jnp.bfloat16)
    return (hidden_out, k_out, v_out)
```

```python
import functools

import jax
import jax.numpy as jnp
import numpy as np
from jax import lax
from jax.experimental import pallas as pl
from jax.experimental.pallas import tpu as pltpu
from jax.sharding import PartitionSpec as P

NORM_EPS = 1e-5
ROPE_BASE = 10000.0
MESH = pl.DeviceIdType.MESH
F32 = jnp.float32
BF16 = jnp.bfloat16
WIN = 32
ALIGN = 16
CHUNK = 256
VMEM_LIMIT = 60 * 1024 * 1024

ANY = pl.BlockSpec(memory_space=pl.ANY)
VMEM = pl.BlockSpec(memory_space=pltpu.VMEM)
SMEM = pl.BlockSpec(memory_space=pltpu.SMEM)


def nt_dot(a, b):
    return lax.dot_general(a, b, (((1,), (1,)), ((), ())), preferred_element_type=F32)


def mm(a, b):
    return jnp.dot(a, b, preferred_element_type=F32)


def iota(shape, dim):
    return lax.broadcasted_iota(jnp.int32, shape, dim)


class Links:
    def __init__(self, send_sems, recv_sems):
        self.send_sems, self.recv_sems, self.started = send_sems, recv_sems, {}

    def send(self, i, src, dst, device):
        copy = pltpu.make_async_remote_copy(
            src_ref=src, dst_ref=dst, send_sem=self.send_sems.at[i], recv_sem=self.recv_sems.at[i],
            device_id=device, device_id_type=MESH)
        copy.start()
        self.started[i] = copy

    def recv(self, *ids):
        for i in ids:
            self.started[i].wait_recv()

    def drain(self):
        for copy in self.started.values():
            copy.wait_send()


class RowSum:
    sends = 12

    def __init__(self, links, base, part, relay, got, full, axis):
        self.links, self.base, self.part, self.relay, self.got, self.full = links, base, part, relay, got, full
        self.size = lax.axis_size(axis)
        self.me = lax.axis_index(axis)
        self.right = lax.rem(self.me + 1, self.size)
        self.left = lax.rem(self.me + self.size - 1, self.size)
        self.far = lax.rem(self.me + 2, self.size)
        self.to_right, self.to_left = {axis: self.right}, {axis: self.left}
        self.block = part.shape[0] // self.size
        self.half = self.block // 2

    def rows(self, rank, half):
        return pl.ds(pl.multiple_of(rank * self.block + half * self.half, self.half), self.half)

    def send(self, i, src, dst, device):
        self.links.send(self.base + i, src, dst, device)

    def recv(self, *ids):
        self.links.recv(*[self.base + i for i in ids])

    def start(self):
        part = self.part
        self.send(0, part.at[self.rows(self.far, 0)], self.relay.at[0], self.to_right)
        self.send(1, part.at[self.rows(self.far, 1)], self.relay.at[1], self.to_left)
        self.send(2, part.at[self.rows(self.right, 1)], self.got.at[0, 1], self.to_right)
        self.send(3, part.at[self.rows(self.left, 0)], self.got.at[1, 0], self.to_left)

    def pass_on(self):
        part, relay = self.part, self.relay
        self.recv(0)
        relay[2] = (part[self.rows(self.right, 0), :].astype(F32) + relay[0].astype(F32)).astype(BF16)
        self.send(4, relay.at[2], self.got.at[0, 0], self.to_right)
        self.recv(1)
        relay[3] = (part[self.rows(self.left, 1), :].astype(F32) + relay[1].astype(F32)).astype(BF16)
        self.send(5, relay.at[3], self.got.at[1, 1], self.to_left)

    def finish_sum(self, own, rest):
        full = self.full
        self.recv(2, 3, 4, 5)
        for half in (0, 1):
            at = self.rows(self.me, half)
            total = own[at, :] + self.got[0, half].astype(F32) + self.got[1, half].astype(F32)
            full[at, :] = (rest[at, :].astype(F32) + total).astype(BF16)
        self.send(6, full.at[self.rows(self.me, 0)], full.at[self.rows(self.me, 0)], self.to_right)
        self.send(7, full.at[self.rows(self.me, 1)], full.at[self.rows(self.me, 1)], self.to_left)
        self.send(8, full.at[self.rows(self.me, 1)], full.at[self.rows(self.me, 1)], self.to_right)
        self.send(9, full.at[self.rows(self.me, 0)], full.at[self.rows(self.me, 0)], self.to_left)

    def forward(self):
        full = self.full
        self.recv(6)
        self.send(10, full.at[self.rows(self.left, 0)], full.at[self.rows(self.left, 0)], self.to_right)
        self.recv(7)
        self.send(11, full.at[self.rows(self.right, 1)], full.at[self.rows(self.right, 1)], self.to_left)

    def finish(self):
        self.recv(8, 9, 10, 11)


def row_sum_scratch(rows, cols, tp):
    half = rows // tp // 2
    return [pltpu.VMEM((rows, cols), BF16), pltpu.VMEM((4, half, cols), BF16),
            pltpu.VMEM((2, 2, half, cols), BF16), pltpu.VMEM((rows, cols), BF16)]


def meet(ep_peers, tp_peers):
    barrier = pltpu.get_barrier_semaphore()
    for peer in ep_peers:
        pl.semaphore_signal(barrier, inc=1, device_id={"ep": peer}, device_id_type=MESH)
    for peer in tp_peers:
        pl.semaphore_signal(barrier, inc=1, device_id={"tp": peer}, device_id_type=MESH)
    pl.semaphore_wait(barrier, len(ep_peers) + len(tp_peers))


def ring_ids():
    ep = lax.axis_size("ep")
    me = lax.axis_index("ep")
    core = lax.rem(me, 2)
    partner = me + 1 - 2 * core
    return ep, me, core, partner, lax.rem(me + 2, ep), lax.rem(me + ep - 2, ep), lax.rem(me + 4, ep)


def front_kernel(x_ref, ids_ref, pos_ref, freq_ref, gains_ref, wr_ref, kc_hbm, vc_hbm, wq_hbm, wk_hbm, wv_hbm, wo_hbm,
                 h_ref, knew_ref, vnew_ref, meta_ref, mall_hbm,
                 mall, meta, a_s, q_s, o_s, k_s, v_s, pcol, kc, vc, wq, wk, wv, wo, own, part, relay, got, full,
                 send_sems, recv_sems, load_sems, out_sems):
    tokens, dim = x_ref.shape
    head = wk.shape[1]
    heads = wq.shape[1] // head
    slots = kc.shape[1]
    ep, me, core, partner, right, left, far = ring_ids()
    tp, mt = lax.axis_size("tp"), lax.axis_index("tp")
    loads = [pltpu.make_async_copy(s, d, load_sems.at[i]) for i, (s, d) in enumerate(
        [(wq_hbm, wq), (wk_hbm, wk), (wv_hbm, wv), (kc_hbm, kc), (vc_hbm, vc), (wo_hbm, wo)])]
    for load in loads:
        load.start()
    peers = [lax.rem(me + i, ep) for i in range(1, ep)]
    barrier = pltpu.get_barrier_semaphore()
    for peer in peers:
        pl.semaphore_signal(barrier, inc=1, device_id={"ep": peer}, device_id_type=MESH)
    for peer in (lax.rem(mt + 1, tp), lax.rem(mt + tp - 1, tp)):
        pl.semaphore_signal(barrier, inc=1, device_id={"tp": peer}, device_id_type=MESH)

    wide = x_ref[...].astype(F32)
    inv = lax.rsqrt(jnp.mean(wide * wide, axis=-1, keepdims=True) + NORM_EPS)
    mall[me] = (wide * inv * gains_ref[2:3, :]).astype(BF16)
    a_s[...] = (wide * inv * gains_ref[0:1, :]).astype(BF16)

    pl.semaphore_wait(barrier, len(peers) + 2)
    links = Links(send_sems, recv_sems)
    hrow = tokens // 2

    def half(i, h):
        return mall.at[i, pl.ds(h * hrow, hrow)]

    links.send(0, half(me, 0), half(me, 0), {"ep": right})
    links.send(1, half(me, 1), half(me, 1), {"ep": left})
    links.send(2, half(me, 1), half(me, 1), {"ep": right})
    links.send(3, half(me, 0), half(me, 0), {"ep": left})
    links.send(4, mall.at[me], mall.at[me], {"ep": partner})
    outs = []

    def put(i):
        copy = pltpu.make_async_copy(mall.at[i], mall_hbm.at[i], out_sems.at[len(outs)])
        copy.start()
        outs.append(copy)

    put(me)

    m_own = mall[me]
    logits = mm(m_own, wr_ref[...])
    probs = jnp.exp(logits - jnp.max(logits, axis=-1, keepdims=True))
    probs = probs / jnp.sum(probs, axis=-1, keepdims=True)
    experts = logits.shape[1]
    ids = ids_ref[...].astype(F32)
    lane = iota((tokens, experts), 1).astype(F32)
    picked = []
    for k in (0, 1):
        id_col = jnp.transpose(jnp.broadcast_to(ids[k:k + 1, :], (experts, tokens)))
        picked.append(jnp.sum(jnp.where(id_col == lane, probs, 0.0), axis=-1, keepdims=True))
    both = picked[0] + picked[1]
    wt_rows = [jnp.transpose(jnp.broadcast_to(p / both, (tokens, 128)))[0:8, :] for p in picked]
    sub = iota((8, tokens), 0)
    block = jnp.where(sub == 0, jnp.broadcast_to(ids[0:1, :], (8, tokens)),
                      jnp.where(sub == 1, jnp.broadcast_to(ids[1:2, :], (8, tokens)),
                                jnp.where(sub == 2, wt_rows[0], wt_rows[1])))
    meta[me] = block
    for n, peer in enumerate(peers):
        links.send(20 + n, meta.at[me], meta.at[me], {"ep": peer})

    def pos_body(g, carry):
        row = iota((8, head), 0)
        acc = jnp.zeros((8, head), jnp.int32)
        for j in range(8):
            acc = jnp.where(row == j, pos_ref[g * 8 + j], acc)
        pcol[pl.ds(pl.multiple_of(g * 8, 8), 8), :] = acc
        return carry

    lax.fori_loop(0, tokens // 8, pos_body, 0)
    angles = pcol[...].astype(F32) * freq_ref[...]
    cosine = jnp.cos(angles)
    sine = jnp.where(iota((tokens, head), 1) < head // 2, -jnp.sin(angles), jnp.sin(angles))

    def rope(v):
        return v * cosine + pltpu.roll(v, head // 2, 1) * sine

    for load in loads[:3]:
        load.wait()
    normed = a_s[...]
    k_s[...] = rope(mm(normed, wk[...])).astype(BF16).astype(F32)
    v_s[...] = mm(normed, wv[...]).astype(BF16).astype(F32)
    knew_ref[...] = k_s[...].astype(BF16)
    vnew_ref[...] = v_s[...].astype(BF16)
    for i in range(heads // 2):
        q2 = mm(normed, wq[:, i * 2 * head:(i + 1) * 2 * head])
        for j in (0, 1):
            q_s[2 * i + j] = rope(q2[:, j * head:(j + 1) * head]).astype(BF16).astype(F32)

    loads[3].wait()
    loads[4].wait()

    def attend(g, carry):
        base = pl.multiple_of(g * 8, 8)
        slot = iota((slots, head), 0)
        keys, vals = [], []
        for j in range(8):
            hit = slot == pos_ref[g * 8 + j]
            keys.append(jnp.where(hit, k_s[pl.ds(base + j, 1), :], kc[base + j].astype(F32)).astype(BF16))
            vals.append(jnp.where(hit, v_s[pl.ds(base + j, 1), :], vc[base + j].astype(F32)).astype(BF16))
        keys = jnp.concatenate(keys, axis=0)
        vals = jnp.concatenate(vals, axis=0)
        q8 = q_s[:, pl.ds(base, 8), :].reshape(heads * 8, head).astype(BF16)
        scores = nt_dot(q8, keys) * (head ** -0.5)
        col = iota((8, 8 * slots), 1)
        mask = jnp.zeros((8, 8 * slots), jnp.bool_)
        row_pos = jnp.concatenate([pcol[pl.ds(base, 8), :]] * (8 * slots // head), axis=1)
        mask = (col // slots == iota((8, 8 * slots), 0)) & (lax.rem(col, slots) <= row_pos)
        mask = jnp.broadcast_to(mask[None], (heads, 8, 8 * slots)).reshape(heads * 8, 8 * slots)
        scores = jnp.where(mask, scores, -1e30)
        e = jnp.exp(scores - jnp.max(scores, axis=-1, keepdims=True))
        p = (e / jnp.sum(e, axis=-1, keepdims=True)).astype(BF16)
        o8 = mm(p, vals)
        o_s[:, pl.ds(base, 8), :] = o8.reshape(heads, 8, head)
        return carry

    lax.fori_loop(0, tokens // 8, attend, 0)
    mix = jnp.concatenate([o_s[i].astype(BF16) for i in range(heads)], axis=1)
    loads[5].wait()
    for i in range(dim // 512):
        cols = slice(i * 512, (i + 1) * 512)
        piece = mm(mix, wo[:, cols])
        own[:, cols] = piece
        part[:, cols] = piece.astype(BF16)
    tp_sum = RowSum(links, 5, part, relay, got, full, "tp")
    tp_sum.start()

    links.recv(0)
    links.send(17, half(left, 0), half(left, 0), {"ep": right})
    links.send(27, half(left, 0), half(left, 0), {"ep": partner})
    links.recv(1)
    links.send(18, half(right, 1), half(right, 1), {"ep": left})
    links.send(28, half(right, 1), half(right, 1), {"ep": partner})
    tp_sum.pass_on()
    links.recv(4)
    put(partner)
    tp_sum.finish_sum(own, x_ref)
    links.recv(2)
    links.send(29, half(left, 1), half(left, 1), {"ep": partner})
    put(left)
    links.recv(3)
    links.send(30, half(right, 0), half(right, 0), {"ep": partner})
    put(right)
    tp_sum.forward()
    tp_sum.finish()
    h_ref[...] = full[...]
    links.recv(*range(20, 20 + len(peers)))
    meta_ref[...] = meta[...]
    links.recv(17)
    links.send(31, half(far, 0), half(far, 0), {"ep": partner})
    links.recv(18)
    links.send(32, half(far, 1), half(far, 1), {"ep": partner})
    put(far)

    def twin(i):
        return i + 1 - 2 * lax.rem(i, 2)

    links.recv(27, 29)
    links.recv(28, 30)
    put(twin(left))
    put(twin(right))
    links.recv(31, 32)
    put(twin(far))
    links.drain()
    for copy in outs:
        copy.wait()


def front(x, ids_t, pos, freq, gains, w_router, kc, vc, w_q, w_k, w_v, w_o, ep, tp):
    tokens, dim = x.shape
    head = w_k.shape[1]
    heads = w_q.shape[1] // head
    slots = kc.shape[1]
    shape = jax.ShapeDtypeStruct
    return pl.pallas_call(
        front_kernel,
        name="front",
        out_shape=(shape((tokens, dim), BF16), shape((tokens, head), BF16), shape((tokens, head), BF16),
                   shape((ep, 8, tokens), F32), shape((ep, tokens, dim), BF16)),
        in_specs=[VMEM, VMEM, SMEM, VMEM, VMEM, VMEM] + [ANY] * 6,
        out_specs=(VMEM, VMEM, VMEM, VMEM, ANY),
        scratch_shapes=[
            pltpu.VMEM((ep, tokens, dim), BF16), pltpu.VMEM((ep, 8, tokens), F32), pltpu.VMEM((tokens, dim), BF16),
            pltpu.VMEM((heads, tokens, head), F32), pltpu.VMEM((heads, tokens, head), F32),
            pltpu.VMEM((tokens, head), F32), pltpu.VMEM((tokens, head), F32), pltpu.VMEM((tokens, head), jnp.int32),
            pltpu.VMEM(kc.shape, BF16), pltpu.VMEM(vc.shape, BF16), pltpu.VMEM(w_q.shape, BF16),
            pltpu.VMEM(w_k.shape, BF16), pltpu.VMEM(w_v.shape, BF16), pltpu.VMEM(w_o.shape, BF16),
            pltpu.VMEM((tokens, dim), F32), *row_sum_scratch(tokens, dim, tp),
            pltpu.SemaphoreType.DMA((33,)), pltpu.SemaphoreType.DMA((33,)),
            pltpu.SemaphoreType.DMA((6,)), pltpu.SemaphoreType.DMA((8,))],
        compiler_params=pltpu.CompilerParams(collective_id=0, has_side_effects=True, vmem_limit_bytes=VMEM_LIMIT),
    )(x, ids_t, pos, freq, gains, w_router, kc, vc, w_q, w_k, w_v, w_o)


def expert_kernel(meta_ref, mall_hbm, eg_hbm, eu_hbm, ed_hbm, out_hbm,
                  rows, sorted_in, sorted_out, pos_row, pos_col, wt_row, wt_slot, plan, plan_s, eg, eu, ed, out,
                  rows_sem, plan_sem, w_sems, out_sems):
    count = eg.shape[0]
    ep, _, tokens = meta_ref.shape
    total_rows, dim = rows.shape
    cap = out.shape[0]
    me = lax.axis_index("ep")
    rows_copy = pltpu.make_async_copy(mall_hbm, rows, rows_sem)
    rows_copy.start()

    def weights(e):
        return [pltpu.make_async_copy(src.at[e], dst.at[e], w_sems.at[i, e])
                for i, (src, dst) in enumerate([(eg_hbm, eg), (eu_hbm, eu), (ed_hbm, ed)])]

    for e in range(count):
        for copy in weights(e):
            copy.start()
    sorted_out[...] = jnp.zeros_like(sorted_out)

    first = (me * count).astype(F32)
    before = (iota((tokens, tokens), 0) < iota((tokens, tokens), 1)).astype(F32).astype(BF16)
    expert = iota((count, tokens), 0).astype(F32)
    hots, ranks, local = [], [], []
    seen = jnp.zeros((count, 1), F32)
    for s in range(ep):
        block = meta_ref[s]
        one, two = block[0:1, :] - first, block[1:2, :] - first
        in_one = (one >= 0) & (one < count)
        in_two = (two >= 0) & (two < count)
        mine = jnp.where(in_one, one, jnp.where(in_two, two, -1.0))
        wt_row[s:s + 1, :] = jnp.where(in_one, block[2:3, :], jnp.where(in_two, block[3:4, :], 0.0))
        hot = (expert == mine).astype(F32)
        hots.append(hot)
        local.append(mine)
        ranks.append(mm(hot.astype(BF16), before) + seen)
        seen = seen + jnp.sum(hot, axis=1, keepdims=True)
    padded = jnp.floor((seen + (ALIGN - 1)) * (1.0 / ALIGN)) * ALIGN
    padded = jnp.broadcast_to(padded, (count, tokens))
    earlier = (iota((count, count), 1) < iota((count, count), 0)).astype(F32).astype(BF16)
    start = mm(earlier, padded.astype(BF16))
    for s in range(ep):
        at = jnp.sum(hots[s] * (start + ranks[s]), axis=0, keepdims=True)
        at = jnp.where(local[s] >= 0, at, -1.0)
        pos_row[s:s + 1, :] = at
        pos_col[pl.ds(s * tokens, tokens), :] = jnp.transpose(jnp.broadcast_to(at, (tokens, tokens)))
    plan[0:count, :] = jnp.broadcast_to(seen, (count, tokens)).astype(jnp.int32)
    plan[count:2 * count, :] = start.astype(jnp.int32)
    plan[2 * count:3 * count, :] = (start + padded).astype(jnp.int32)
    plan_copy = pltpu.make_async_copy(plan, plan_s, plan_sem)
    plan_copy.start()
    plan_copy.wait()
    used = plan_s[3 * count - 1, 0]
    chunks = (used + (CHUNK - 1)) // CHUNK
    rows_copy.wait()

    def gather(c, carry):
        base = pl.multiple_of(c * CHUNK, CHUNK)
        slot = (iota((CHUNK, tokens), 0) + base).astype(F32)
        picks = []
        wt = jnp.zeros((CHUNK, tokens), F32)
        for s in range(ep):
            hot = slot == pos_row[s:s + 1, :]
            wt = wt + jnp.where(hot, wt_row[s:s + 1, :], 0.0)
            picks.append(hot.astype(F32).astype(BF16))
        pick = jnp.concatenate(picks, axis=1)
        wt_slot[pl.ds(base, CHUNK), :] = jnp.broadcast_to(jnp.sum(wt, axis=1, keepdims=True), (CHUNK, tokens))
        for i in range(dim // 512):
            cols = slice(i * 512, (i + 1) * 512)
            sorted_in[pl.ds(base, CHUNK), cols] = mm(pick, rows[:, cols]).astype(BF16)
        return carry

    lax.fori_loop(0, chunks, gather, 0)

    def run_expert(e, carry):
        for copy in weights(e):
            copy.wait()
        passes = (plan_s[e, 0] + (WIN - 1)) // WIN
        begin = plan_s[count + e, 0]

        def one_pass(p, inner):
            at = pl.ds(pl.multiple_of(begin + p * WIN, ALIGN), WIN)
            x = sorted_in[at, :]
            gate = nt_dot(eg[e], x)
            up = nt_dot(eu[e], x)
            act = jnp.transpose(jax.nn.silu(gate) * up).astype(BF16)
            wt = wt_slot[at, :][:, 0:1]
            for i in range(dim // 512):
                cols = slice(i * 512, (i + 1) * 512)
                sorted_out[at, cols] = (mm(act, ed[e, :, cols]) * wt).astype(BF16)
            return inner

        lax.fori_loop(0, passes, one_pass, 0)
        return carry

    lax.fori_loop(0, count, run_expert, 0)

    block = total_rows // 2
    lane = iota((block, tokens), 1).astype(F32)
    for k in range(1, cap // CHUNK + 1):
        @pl.when(jnp.maximum(chunks, 1) == k)
        def _():
            for b in range(2):
                at = pl.ds(b * block, block)
                where = pos_col[at, :]
                pick = jnp.concatenate([(where == lane + float(j * tokens)).astype(F32).astype(BF16)
                                        for j in range(k * CHUNK // tokens)], axis=1)

                def cols_body(i, carry):
                    cols = pl.ds(pl.multiple_of(i * 512, 512), 512)
                    rows[at, cols] = mm(pick, sorted_out[0:k * CHUNK, cols]).astype(BF16)
                    return carry

                lax.fori_loop(0, dim // 512, cols_body, 0)
                pltpu.make_async_copy(rows.at[at], out_hbm.at[at], out_sems.at[b]).start()
    for b in range(2):
        at = pl.ds(b * block, block)
        pltpu.make_async_copy(rows.at[at], out_hbm.at[at], out_sems.at[b]).wait()


def experts(meta, mall, eg_t, eu_t, ed):
    ep, _, tokens = meta.shape
    dim = mall.shape[1]
    count = eg_t.shape[0]
    most = ep * tokens // 2 + count * (ALIGN - 1)
    cap = (most + CHUNK - 1) // CHUNK * CHUNK
    total = ep * tokens
    return pl.pallas_call(
        expert_kernel,
        name="experts",
        out_shape=jax.ShapeDtypeStruct((total, dim), BF16),
        in_specs=[VMEM] + [ANY] * 4,
        out_specs=ANY,
        scratch_shapes=[
            pltpu.VMEM((total, dim), BF16), pltpu.VMEM((cap + WIN, dim), BF16), pltpu.VMEM((cap + WIN, dim), BF16),
            pltpu.VMEM((ep, tokens), F32), pltpu.VMEM((total, tokens), F32), pltpu.VMEM((ep, tokens), F32),
            pltpu.VMEM((cap + WIN, tokens), F32), pltpu.VMEM((3 * count, tokens), jnp.int32),
            pltpu.SMEM((3 * count, tokens), jnp.int32),
            pltpu.VMEM(eg_t.shape, BF16), pltpu.VMEM(eu_t.shape, BF16), pltpu.VMEM(ed.shape, BF16),
            pltpu.VMEM((cap, 128), BF16),
            pltpu.SemaphoreType.DMA, pltpu.SemaphoreType.DMA, pltpu.SemaphoreType.DMA((3, count)),
            pltpu.SemaphoreType.DMA((2,))],
        compiler_params=pltpu.CompilerParams(vmem_limit_bytes=VMEM_LIMIT),
    )(meta, mall, eg_t, eu_t, ed)


def back_kernel(h_ref, gains_ref, moe_hbm, wg_hbm, wu_hbm, wd_hbm, out_ref,
                keep, give, take, ring, relay_x, got_x, swap, own, c_s, wg, wu, wd, part, relay, got, full,
                send_sems, recv_sems, load_sems):
    tokens, dim = h_ref.shape
    ep, me, core, partner, right, left, far = ring_ids()
    tp, mt = lax.axis_size("tp"), lax.axis_index("tp")
    halfd = dim // 2
    quart = halfd // 2
    pair = 2 * tokens
    mine = pl.ds(pl.multiple_of(core * halfd, halfd), halfd)
    other = pl.ds(pl.multiple_of((1 - core) * halfd, halfd), halfd)
    chips = [far // 2, right // 2, left // 2, me // 2]

    def rows_of(chip):
        return pl.ds(pl.multiple_of(chip * pair, pair), pair)

    give_loads = [pltpu.make_async_copy(moe_hbm.at[rows_of(chip), other], give.at[i], load_sems.at[i])
                  for i, chip in enumerate(chips)]
    keep_loads = [pltpu.make_async_copy(moe_hbm.at[rows_of(chip), mine], keep.at[i], load_sems.at[4 + i])
                  for i, chip in enumerate(chips)]
    w_loads = [pltpu.make_async_copy(s, d, load_sems.at[8 + i])
               for i, (s, d) in enumerate([(wg_hbm, wg), (wu_hbm, wu), (wd_hbm, wd)])]
    for load in give_loads + keep_loads + w_loads:
        load.start()
    meet([partner, right, left], [lax.rem(mt + 1, tp), lax.rem(mt + tp - 1, tp)])
    links = Links(send_sems, recv_sems)
    for i in range(4):
        give_loads[i].wait()
        links.send(i, give.at[i], take.at[i], {"ep": partner})

    def add_pair(i):
        keep_loads[i].wait()
        links.recv(i)
        ring[i] = (keep[i].astype(F32) + take[i].astype(F32)).astype(BF16)

    lo, hi = pl.ds(0, quart), pl.ds(quart, quart)
    to_right, to_left = {"ep": right}, {"ep": left}
    add_pair(0)
    links.send(4, ring.at[0, :, lo], relay_x.at[0], to_right)
    links.send(5, ring.at[0, :, hi], relay_x.at[1], to_left)
    add_pair(1)
    links.send(6, ring.at[1, :, hi], got_x.at[0, 1], to_right)
    add_pair(2)
    links.send(7, ring.at[2, :, lo], got_x.at[1, 0], to_left)
    add_pair(3)

    wide = h_ref[...].astype(F32)
    inv = lax.rsqrt(jnp.mean(wide * wide, axis=-1, keepdims=True) + NORM_EPS)
    c_s[...] = (wide * inv * gains_ref[1:2, :]).astype(BF16)
    w_loads[0].wait()
    w_loads[1].wait()
    acts = []
    for i in range(wg.shape[1] // 512):
        cols = slice(i * 512, (i + 1) * 512)
        gate = mm(c_s[...], wg[:, cols])
        up = mm(c_s[...], wu[:, cols])
        acts.append((jax.nn.silu(gate) * up).astype(BF16))
    act = jnp.concatenate(acts, axis=1)
    w_loads[2].wait()
    for i in range(dim // 512):
        cols = slice(i * 512, (i + 1) * 512)
        own[:, cols] = mm(act, wd[:, cols])

    links.recv(4)
    relay_x[2] = (ring[1, :, 0:quart].astype(F32) + relay_x[0].astype(F32)).astype(BF16)
    links.send(8, relay_x.at[2], got_x.at[0, 0], to_right)
    links.recv(5)
    relay_x[3] = (ring[2, :, quart:halfd].astype(F32) + relay_x[1].astype(F32)).astype(BF16)
    links.send(9, relay_x.at[3], got_x.at[1, 1], to_left)
    links.recv(6, 7, 8, 9)
    mine_rows = pl.ds(pl.multiple_of(core * tokens, tokens), tokens)
    give_rows = pl.ds(pl.multiple_of((1 - core) * tokens, tokens), tokens)

    def arrived(at):
        pieces = []
        for q in (0, 1):
            cols = slice(q * quart, (q + 1) * quart)
            pieces.append(ring[3, at, cols].astype(F32) + got_x[0, q, at, :].astype(F32)
                          + got_x[1, q, at, :].astype(F32))
        return jnp.concatenate(pieces, axis=1)

    swap[0] = arrived(give_rows).astype(BF16)
    links.send(10, swap.at[0], swap.at[1], {"ep": partner})
    own[:, mine] += arrived(mine_rows)
    part[:, mine] = own[:, mine].astype(BF16)
    links.recv(10)
    own[:, other] += swap[1].astype(F32)
    part[:, other] = own[:, other].astype(BF16)
    tp_sum = RowSum(links, 11, part, relay, got, full, "tp")
    tp_sum.start()
    tp_sum.pass_on()
    tp_sum.finish_sum(own, h_ref)
    tp_sum.forward()
    tp_sum.finish()
    out_ref[...] = full[...]
    links.drain()


def back(h, gains, moe, w_gate, w_up, w_down, tp):
    tokens, dim = h.shape
    pair, halfd, quart = 2 * tokens, dim // 2, dim // 4
    chips = moe.shape[0] // pair
    return pl.pallas_call(
        back_kernel,
        name="back",
        out_shape=jax.ShapeDtypeStruct((tokens, dim), BF16),
        in_specs=[VMEM, VMEM] + [ANY] * 4,
        out_specs=VMEM,
        scratch_shapes=[
            pltpu.VMEM((chips, pair, halfd), BF16), pltpu.VMEM((chips, pair, halfd), BF16),
            pltpu.VMEM((chips, pair, halfd), BF16), pltpu.VMEM((chips, pair, halfd), BF16),
            pltpu.VMEM((4, pair, quart), BF16), pltpu.VMEM((2, 2, pair, quart), BF16),
            pltpu.VMEM((2, tokens, halfd), BF16), pltpu.VMEM((tokens, dim), F32), pltpu.VMEM((tokens, dim), BF16),
            pltpu.VMEM(w_gate.shape, BF16), pltpu.VMEM(w_up.shape, BF16), pltpu.VMEM(w_down.shape, BF16),
            *row_sum_scratch(tokens, dim, tp),
            pltpu.SemaphoreType.DMA((23,)), pltpu.SemaphoreType.DMA((23,)), pltpu.SemaphoreType.DMA((11,))],
        compiler_params=pltpu.CompilerParams(collective_id=1, has_side_effects=True, vmem_limit_bytes=VMEM_LIMIT),
    )(h, gains, moe, w_gate, w_up, w_down)


def solution(mesh):
    ep, tp = mesh.shape['ep'], mesh.shape['tp']
    row_spec = P(('dp', 'ep'), None)
    cache_spec = P(('dp', 'ep'), None, 'tp', None)
    col_split = P(None, 'tp')
    row_split = P('tp', None)
    in_specs = (row_spec, P(('dp', 'ep')), row_spec, cache_spec, cache_spec, P(None), P(None), P(None), col_split, col_split, col_split, row_split, col_split, col_split, row_split, P(None, None), P('ep', None, 'tp'), P('ep', None, 'tp'), P('ep', 'tp', None))
    out_specs = (row_spec, cache_spec, cache_spec)

    def local_layer(hidden_in, positions, expert_ids, k_cache, v_cache, norm_in, norm_res, norm_post, w_q, w_k, w_v, w_o, w_gate, w_up, w_down, w_router, e_gate, e_up, e_down):
        tokens, dim = hidden_in.shape
        slots, head = k_cache.shape[1], k_cache.shape[3]
        freq = (1.0 / (ROPE_BASE ** (jnp.arange(0, head, 2, dtype=F32) / head)))[None, :]
        freq = jnp.concatenate([freq, freq], axis=1)
        gains = jnp.stack([norm_in, norm_res, norm_post]).astype(F32)
        h, k_new, v_new, meta, mall = front(
            hidden_in, expert_ids.T, positions, freq, gains, w_router,
            k_cache.reshape(tokens, slots, head), v_cache.reshape(tokens, slots, head), w_q, w_k, w_v, w_o, ep, tp)
        moe = experts(meta, mall.reshape(ep * tokens, dim), jnp.swapaxes(e_gate, 1, 2), jnp.swapaxes(e_up, 1, 2), e_down)
        slot_hit = (jnp.arange(slots)[None, :] == positions[:, None])[:, :, None, None]
        k_out = jnp.where(slot_hit, k_new[:, None, None, :], k_cache)
        v_out = jnp.where(slot_hit, v_new[:, None, None, :], v_cache)
        return back(h, gains, moe, w_gate, w_up, w_down, tp), k_out, v_out

    return jax.shard_map(local_layer, mesh=mesh, in_specs=in_specs, out_specs=out_specs, check_vma=False)
```

```python
import functools

import jax
import jax.numpy as jnp
import numpy as np
from jax import lax
from jax.experimental import pallas as pl
from jax.experimental.pallas import tpu as pltpu
from jax.sharding import PartitionSpec as P

NORM_EPS = 1e-5
ROPE_BASE = 10000.0
MESH = pl.DeviceIdType.MESH
F32 = jnp.float32
BF16 = jnp.bfloat16
WIN = 32
ALIGN = 16
AHEAD = 6
COLS = 512
CHUNK = 256
VMEM_LIMIT = 60 * 1024 * 1024

ANY = pl.BlockSpec(memory_space=pl.ANY)
VMEM = pl.BlockSpec(memory_space=pltpu.VMEM)
SMEM = pl.BlockSpec(memory_space=pltpu.SMEM)


def nt_dot(a, b):
    return lax.dot_general(a, b, (((1,), (1,)), ((), ())), preferred_element_type=F32)


def mm(a, b):
    return jnp.dot(a, b, preferred_element_type=F32)


def span(i, width):
    return slice(i * width, (i + 1) * width)


def total(v, axis):
    return jnp.sum(v, axis=axis, keepdims=True)


def exp_rows(v):
    return jnp.exp(v - jnp.max(v, axis=-1, keepdims=True))


def rms(wide):
    return lax.rsqrt(jnp.mean(wide * wide, axis=-1, keepdims=True) + NORM_EPS)


def iota(shape, dim):
    return lax.broadcasted_iota(jnp.int32, shape, dim)


def gain_row(ref):
    return ref[...].astype(F32).reshape(1, ref.shape[0])


class Links:
    def __init__(self, send_sems, recv_sems):
        self.send_sems, self.recv_sems, self.started = send_sems, recv_sems, {}

    def send(self, i, src, dst, device):
        copy = pltpu.make_async_remote_copy(
            src_ref=src, dst_ref=dst, send_sem=self.send_sems.at[i], recv_sem=self.recv_sems.at[i],
            device_id=device, device_id_type=MESH)
        copy.start()
        self.started[i] = copy

    def recv(self, *ids):
        for i in ids:
            self.started[i].wait_recv()

    def drain(self):
        for copy in self.started.values():
            copy.wait_send()


class RowSum:
    def __init__(self, links, base, axis, full, part=None, relay=None, got=None):
        self.links, self.base, self.part, self.relay, self.got, self.full = links, base, part, relay, got, full
        self.size = lax.axis_size(axis)
        self.me = lax.axis_index(axis)
        self.right = lax.rem(self.me + 1, self.size)
        self.left = lax.rem(self.me + self.size - 1, self.size)
        self.far = lax.rem(self.me + 2, self.size)
        self.to_right, self.to_left = {axis: self.right}, {axis: self.left}
        self.block = full.shape[0] // self.size
        self.half = self.block // 2

    def rows(self, rank, half):
        if half is None:
            return pl.ds(pl.multiple_of(rank * self.block, self.block), self.block)
        return pl.ds(pl.multiple_of(rank * self.block + half * self.half, self.half), self.half)

    def send(self, i, src, dst, device):
        self.links.send(self.base + i, src, dst, device)

    def recv(self, *ids):
        self.links.recv(*[self.base + i for i in ids])

    def start(self):
        part = self.part
        self.send(0, part.at[self.rows(self.far, 0)], self.relay.at[0], self.to_right)
        self.send(1, part.at[self.rows(self.far, 1)], self.relay.at[1], self.to_left)
        self.send(2, part.at[self.rows(self.right, 1)], self.got.at[0, 1], self.to_right)
        self.send(3, part.at[self.rows(self.left, 0)], self.got.at[1, 0], self.to_left)

    def pass_on(self):
        part, relay = self.part, self.relay
        self.recv(0)
        relay[2] = (part[self.rows(self.right, 0), :].astype(F32) + relay[0].astype(F32)).astype(BF16)
        self.send(4, relay.at[2], self.got.at[0, 0], self.to_right)
        self.recv(1)
        relay[3] = (part[self.rows(self.left, 1), :].astype(F32) + relay[1].astype(F32)).astype(BF16)
        self.send(5, relay.at[3], self.got.at[1, 1], self.to_left)

    def collect(self, own, rest):
        full = self.full
        self.recv(2, 3, 4, 5)
        for half in (0, 1):
            at = self.rows(self.me, half)
            acc = own[at, :] + self.got[0, half].astype(F32) + self.got[1, half].astype(F32)
            full[at, :] = (rest[at, :].astype(F32) + acc).astype(BF16)

    def spread(self):
        full = self.full
        self.send(6, full.at[self.rows(self.me, 0)], full.at[self.rows(self.me, 0)], self.to_right)
        self.send(7, full.at[self.rows(self.me, 1)], full.at[self.rows(self.me, 1)], self.to_left)
        self.send(8, full.at[self.rows(self.me, 1)], full.at[self.rows(self.me, 1)], self.to_right)
        self.send(9, full.at[self.rows(self.me, 0)], full.at[self.rows(self.me, 0)], self.to_left)

    def forward(self):
        full = self.full
        self.recv(6)
        self.send(10, full.at[self.rows(self.left, 0)], full.at[self.rows(self.left, 0)], self.to_right)
        self.recv(7)
        self.send(11, full.at[self.rows(self.right, 1)], full.at[self.rows(self.right, 1)], self.to_left)

    def finish(self):
        self.recv(8, 9, 10, 11)


def row_sum_scratch(rows, cols, tp):
    half = rows // tp // 2
    return [pltpu.VMEM((rows, cols), BF16), pltpu.VMEM((4, half, cols), BF16),
            pltpu.VMEM((2, 2, half, cols), BF16), pltpu.VMEM((rows, cols), BF16)]


def meet(ep_peers, tp_peers):
    barrier = pltpu.get_barrier_semaphore()
    for peer in ep_peers:
        pl.semaphore_signal(barrier, inc=1, device_id={"ep": peer}, device_id_type=MESH)
    for peer in tp_peers:
        pl.semaphore_signal(barrier, inc=1, device_id={"tp": peer}, device_id_type=MESH)
    pl.semaphore_wait(barrier, len(ep_peers) + len(tp_peers))


def ring_ids():
    ep = lax.axis_size("ep")
    me = lax.axis_index("ep")
    core = lax.rem(me, 2)
    partner = me + 1 - 2 * core
    return ep, me, core, partner, lax.rem(me + 2, ep), lax.rem(me + ep - 2, ep), lax.rem(me + 4, ep)


def front_kernel(x_ref, ids_ref, pos_ref, gin_ref, gpost_ref, wr_ref, kc_hbm, vc_hbm, wq_hbm, wk_hbm, wv_hbm, wo_hbm,
                 hsum_ref, knew_ref, vnew_ref, meta_ref, mall_hbm,
                 mall, meta, a_s, q_s, o_s, k_s, v_s, pcol, kc, vc, wq, wk, wv, wo, own, part, relay, got, full,
                 send_sems, recv_sems, load_sems, out_sems):
    tokens, dim = x_ref.shape
    head = wk.shape[1]
    heads = wq.shape[1] // head
    slots = kc.shape[1]
    ep, me, core, partner, right, left, far = ring_ids()
    tp, mt = lax.axis_size("tp"), lax.axis_index("tp")
    loads = [pltpu.make_async_copy(s, d, load_sems.at[i]) for i, (s, d) in enumerate(
        [(wq_hbm, wq), (wk_hbm, wk), (wv_hbm, wv), (kc_hbm, kc), (vc_hbm, vc), (wo_hbm, wo)])]
    for load in loads:
        load.start()
    peers = [lax.rem(me + i, ep) for i in range(1, ep)]
    barrier = pltpu.get_barrier_semaphore()
    for peer in peers:
        pl.semaphore_signal(barrier, inc=1, device_id={"ep": peer}, device_id_type=MESH)
    for peer in (lax.rem(mt + 1, tp), lax.rem(mt + tp - 1, tp)):
        pl.semaphore_signal(barrier, inc=1, device_id={"tp": peer}, device_id_type=MESH)

    wide = x_ref[...].astype(F32)
    inv = rms(wide)
    mall[me] = (wide * inv * gain_row(gpost_ref)).astype(BF16)
    a_s[...] = (wide * inv * gain_row(gin_ref)).astype(BF16)

    pl.semaphore_wait(barrier, len(peers) + 2)
    links = Links(send_sems, recv_sems)
    hrow = tokens // 2

    def half(i, h):
        return mall.at[i, pl.ds(h * hrow, hrow)]

    links.send(0, half(me, 0), half(me, 0), {"ep": right})
    links.send(1, half(me, 1), half(me, 1), {"ep": left})
    links.send(2, half(me, 1), half(me, 1), {"ep": right})
    links.send(3, half(me, 0), half(me, 0), {"ep": left})
    links.send(4, mall.at[me], mall.at[me], {"ep": partner})
    outs = []

    def put(i):
        copy = pltpu.make_async_copy(mall.at[i], mall_hbm.at[i], out_sems.at[len(outs)])
        copy.start()
        outs.append(copy)

    put(me)

    m_own = mall[me]
    logits = mm(m_own, wr_ref[...])
    probs = exp_rows(logits)
    probs = probs / total(probs, 1)
    experts = logits.shape[1]
    ids = ids_ref[...].astype(F32)
    lane = iota((tokens, experts), 1).astype(F32)
    picked = []
    for k in (0, 1):
        id_col = jnp.transpose(jnp.broadcast_to(ids[k:k + 1, :], (experts, tokens)))
        picked.append(total(jnp.where(id_col == lane, probs, 0.0), 1))
    both = picked[0] + picked[1]
    wt_rows = [jnp.transpose(jnp.broadcast_to(p / both, (tokens, 128)))[0:8, :] for p in picked]
    sub = iota((8, tokens), 0)
    block = jnp.where(sub == 0, jnp.broadcast_to(ids[0:1, :], (8, tokens)),
                      jnp.where(sub == 1, jnp.broadcast_to(ids[1:2, :], (8, tokens)),
                                jnp.where(sub == 2, wt_rows[0], wt_rows[1])))
    meta[me] = block
    for n, peer in enumerate(peers):
        links.send(20 + n, meta.at[me], meta.at[me], {"ep": peer})

    def pos_body(g, carry):
        row = iota((8, head), 0)
        acc = jnp.zeros((8, head), jnp.int32)
        for j in range(8):
            acc = jnp.where(row == j, pos_ref[g * 8 + j], acc)
        pcol[pl.ds(pl.multiple_of(g * 8, 8), 8), :] = acc
        return carry

    lax.fori_loop(0, tokens // 8, pos_body, 0)
    spot = iota((tokens, head), 1)
    power = lax.rem(spot, head // 2).astype(F32) * (-np.log(ROPE_BASE) / (head // 2))
    angles = pcol[...].astype(F32) * jnp.exp(power)
    cosine = jnp.cos(angles)
    sine = jnp.sin(angles)
    sine = jnp.where(spot < head // 2, -sine, sine)

    def rope(v):
        return v * cosine + pltpu.roll(v, head // 2, 1) * sine

    for load in loads[:3]:
        load.wait()
    normed = a_s[...]
    k_s[...] = rope(mm(normed, wk[...])).astype(BF16).astype(F32)
    v_s[...] = mm(normed, wv[...]).astype(BF16).astype(F32)
    knew_ref[...] = k_s[...].astype(BF16)
    vnew_ref[...] = v_s[...].astype(BF16)
    for i in range(heads // 2):
        q2 = mm(normed, wq[:, span(i, 2 * head)])
        for j in (0, 1):
            q_s[2 * i + j] = rope(q2[:, span(j, head)]).astype(BF16).astype(F32)

    loads[3].wait()
    loads[4].wait()

    def attend(g, carry):
        base = pl.multiple_of(g * 8, 8)
        slot = iota((slots, head), 0)
        keys, vals = [], []
        for j in range(8):
            hit = slot == pos_ref[g * 8 + j]
            keys.append(jnp.where(hit, k_s[pl.ds(base + j, 1), :], kc[base + j].astype(F32)).astype(BF16))
            vals.append(jnp.where(hit, v_s[pl.ds(base + j, 1), :], vc[base + j].astype(F32)).astype(BF16))
        keys = jnp.concatenate(keys, axis=0)
        vals = jnp.concatenate(vals, axis=0)
        q8 = q_s[:, pl.ds(base, 8), :].reshape(heads * 8, head).astype(BF16)
        scores = nt_dot(q8, keys) * (head ** -0.5)
        col = iota((8, 8 * slots), 1)
        row_pos = jnp.concatenate([pcol[pl.ds(base, 8), :]] * (8 * slots // head), axis=1)
        mask = (col // slots == iota((8, 8 * slots), 0)) & (lax.rem(col, slots) <= row_pos)
        mask = jnp.broadcast_to(mask[None], (heads, 8, 8 * slots)).reshape(heads * 8, 8 * slots)
        scores = jnp.where(mask, scores, -1e30)
        e = exp_rows(scores)
        p = (e / total(e, 1)).astype(BF16)
        o8 = mm(p, vals)
        o_s[:, pl.ds(base, 8), :] = o8.reshape(heads, 8, head)
        return carry

    lax.fori_loop(0, tokens // 8, attend, 0)
    mix = jnp.concatenate([o_s[i].astype(BF16) for i in range(heads)], axis=1)
    loads[5].wait()
    for i in range(dim // COLS):
        cols = span(i, COLS)
        piece = mm(mix, wo[:, cols])
        own[:, cols] = piece
        part[:, cols] = piece.astype(BF16)
    tp_sum = RowSum(links, 5, "tp", full, part, relay, got)
    tp_sum.start()

    def twin(i):
        return i + 1 - 2 * lax.rem(i, 2)

    moves = [(0, 17, left, 0, right), (1, 18, right, 1, left)]
    for n, (came, to, block, h, device) in enumerate(moves):
        links.recv(came)
        links.send(to, half(block, h), half(block, h), {"ep": device})
        links.send(27 + n, half(block, h), half(block, h), {"ep": partner})
    tp_sum.pass_on()
    links.recv(4)
    put(partner)
    tp_sum.collect(own, x_ref)
    hsum_ref[...] = full[tp_sum.rows(tp_sum.me, None), :]
    for n, (came, block, h) in enumerate([(2, left, 1), (3, right, 0)]):
        links.recv(came)
        links.send(29 + n, half(block, h), half(block, h), {"ep": partner})
        put(block)
    links.recv(*range(20, 20 + len(peers)))
    meta_ref[...] = meta[...]
    links.recv(27, 29)
    put(twin(left))
    links.recv(28, 30)
    put(twin(right))
    for n, came in enumerate([17, 18]):
        links.recv(came)
        links.send(31 + n, half(far, n), half(far, n), {"ep": partner})
    put(far)
    links.recv(31, 32)
    put(twin(far))
    links.drain()
    for copy in outs:
        copy.wait()


def front(x, ids_t, pos, g_in, g_post, w_router, kc, vc, w_q, w_k, w_v, w_o, ep, tp):
    tokens, dim = x.shape
    head = w_k.shape[1]
    heads = w_q.shape[1] // head
    slots = kc.shape[1]
    shape = jax.ShapeDtypeStruct
    return pl.pallas_call(
        front_kernel,
        name="front",
        out_shape=(shape((tokens // tp, dim), BF16), shape((tokens, head), BF16), shape((tokens, head), BF16),
                   shape((ep, 8, tokens), F32), shape((ep, tokens, dim), BF16)),
        in_specs=[VMEM, VMEM, SMEM, VMEM, VMEM, VMEM] + [ANY] * 6,
        out_specs=(VMEM, VMEM, VMEM, VMEM, ANY),
        scratch_shapes=[
            pltpu.VMEM((ep, tokens, dim), BF16), pltpu.VMEM((ep, 8, tokens), F32), pltpu.VMEM((tokens, dim), BF16),
            pltpu.VMEM((heads, tokens, head), F32), pltpu.VMEM((heads, tokens, head), F32),
            pltpu.VMEM((tokens, head), F32), pltpu.VMEM((tokens, head), F32), pltpu.VMEM((tokens, head), jnp.int32),
            pltpu.VMEM(kc.shape, BF16), pltpu.VMEM(vc.shape, BF16), pltpu.VMEM(w_q.shape, BF16),
            pltpu.VMEM(w_k.shape, BF16), pltpu.VMEM(w_v.shape, BF16), pltpu.VMEM(w_o.shape, BF16),
            pltpu.VMEM((tokens, dim), F32), *row_sum_scratch(tokens, dim, tp),
            pltpu.SemaphoreType.DMA((33,)), pltpu.SemaphoreType.DMA((33,)),
            pltpu.SemaphoreType.DMA((6,)), pltpu.SemaphoreType.DMA((8,))],
        compiler_params=pltpu.CompilerParams(collective_id=0, has_side_effects=True, vmem_limit_bytes=VMEM_LIMIT),
    )(x, ids_t, pos, g_in, g_post, w_router, kc, vc, w_q, w_k, w_v, w_o)


def expert_kernel(meta_ref, pos_ref, knew_ref, vnew_ref, kc_hbm, vc_hbm, mall_hbm, eg_hbm, eu_hbm, ed_hbm,
                  out_hbm, ko_hbm, vo_hbm,
                  kc, vc, k_s, v_s, rows, sorted_in, sorted_out, pos_row, pos_col, wt_row, wt_slot, plan, plan_s, eg, eu, ed, out,
                  rows_sem, plan_sem, cache_sems, w_sems, out_sems):
    count = eg.shape[0]
    ep, _, tokens = meta_ref.shape
    total_rows, dim = rows.shape
    cap = out.shape[0]
    me = lax.axis_index("ep")
    rows_copy = pltpu.make_async_copy(mall_hbm, rows, rows_sem)
    rows_copy.start()

    def weights(e):
        return [pltpu.make_async_copy(src.at[e], dst.at[e], w_sems.at[i, e])
                for i, (src, dst) in enumerate([(eg_hbm, eg), (eu_hbm, eu), (ed_hbm, ed)])]

    sorted_out[...] = jnp.zeros_like(sorted_out)

    first = (me * count).astype(F32)
    before = (iota((tokens, tokens), 0) < iota((tokens, tokens), 1)).astype(F32).astype(BF16)
    expert = iota((count, tokens), 0).astype(F32)
    hots, ranks, local = [], [], []
    seen = jnp.zeros((count, 1), F32)
    for s in range(ep):
        block = meta_ref[s]
        one, two = block[0:1, :] - first, block[1:2, :] - first
        in_one = (one >= 0) & (one < count)
        in_two = (two >= 0) & (two < count)
        mine = jnp.where(in_one, one, jnp.where(in_two, two, -1.0))
        wt_row[s:s + 1, :] = jnp.where(in_one, block[2:3, :], jnp.where(in_two, block[3:4, :], 0.0))
        hot = (expert == mine).astype(F32)
        hots.append(hot)
        local.append(mine)
        ranks.append(mm(hot.astype(BF16), before) + seen)
        seen = seen + total(hot, 1)
    padded = jnp.floor((seen + (ALIGN - 1)) * (1.0 / ALIGN)) * ALIGN
    padded = jnp.broadcast_to(padded, (count, tokens))
    earlier = (iota((count, count), 1) < iota((count, count), 0)).astype(F32).astype(BF16)
    start = mm(earlier, padded.astype(BF16))
    for s in range(ep):
        at = total(hots[s] * (start + ranks[s]), 0)
        at = jnp.where(local[s] >= 0, at, -1.0)
        pos_row[s:s + 1, :] = at
        pos_col[pl.ds(s * tokens, tokens), :] = jnp.transpose(jnp.broadcast_to(at, (tokens, tokens)))
    plan[0:count, :] = jnp.broadcast_to(seen, (count, tokens)).astype(jnp.int32)
    plan[count:2 * count, :] = start.astype(jnp.int32)
    plan[2 * count:3 * count, :] = (start + padded).astype(jnp.int32)
    plan_copy = pltpu.make_async_copy(plan, plan_s, plan_sem)
    plan_copy.start()
    plan_copy.wait()
    used = plan_s[3 * count - 1, 0]
    chunks = (used + (CHUNK - 1)) // CHUNK
    rows_copy.wait()
    for e in range(AHEAD):
        for copy in weights(e):
            copy.start()
    caches = [(kc_hbm, kc, ko_hbm), (vc_hbm, vc, vo_hbm)]
    cache_in = [pltpu.make_async_copy(src, buf, cache_sems.at[0, i]) for i, (src, buf, _) in enumerate(caches)]
    cache_out = [pltpu.make_async_copy(buf, dst, cache_sems.at[1, i]) for i, (_, buf, dst) in enumerate(caches)]
    for copy in cache_in:
        copy.start()

    def gather(c, carry):
        base = pl.multiple_of(c * CHUNK, CHUNK)
        slot = (iota((CHUNK, tokens), 0) + base).astype(F32)
        picks = []
        wt = jnp.zeros((CHUNK, tokens), F32)
        for s in range(ep):
            hot = slot == pos_row[s:s + 1, :]
            wt = wt + jnp.where(hot, wt_row[s:s + 1, :], 0.0)
            picks.append(hot.astype(F32).astype(BF16))
        pick = jnp.concatenate(picks, axis=1)
        wt_slot[pl.ds(base, CHUNK), :] = jnp.broadcast_to(total(wt, 1), (CHUNK, tokens))
        for i in range(dim // COLS):
            cols = span(i, COLS)
            sorted_in[pl.ds(base, CHUNK), cols] = mm(pick, rows[:, cols]).astype(BF16)
        return carry

    lax.fori_loop(0, chunks, gather, 0)

    def run_expert(e, carry):
        @pl.when(e + AHEAD < count)
        def _():
            for copy in weights(e + AHEAD):
                copy.start()

        for copy in weights(e):
            copy.wait()
        passes = (plan_s[e, 0] + (WIN - 1)) // WIN
        begin = plan_s[count + e, 0]

        def one_pass(p, inner):
            at = pl.ds(pl.multiple_of(begin + p * WIN, ALIGN), WIN)
            x = sorted_in[at, :]
            gate = nt_dot(eg[e], x)
            up = nt_dot(eu[e], x)
            act = jnp.transpose(jax.nn.silu(gate) * up).astype(BF16)
            wt = wt_slot[at, :][:, 0:1]
            for i in range(dim // COLS):
                cols = span(i, COLS)
                sorted_out[at, cols] = (mm(act, ed[e, :, cols]) * wt).astype(BF16)
            return inner

        lax.fori_loop(0, passes, one_pass, 0)
        return carry

    lax.fori_loop(0, count, run_expert, 0)

    k_s[...] = knew_ref[...].astype(F32)
    v_s[...] = vnew_ref[...].astype(F32)
    for copy in cache_in:
        copy.wait()
    head = kc.shape[2]

    def new_rows(g, carry):
        for j in range(8):
            b = g * 8 + j
            spot = pos_ref[b]
            base = pl.multiple_of(spot // ALIGN * ALIGN, ALIGN)
            hit = iota((ALIGN, head), 0) == spot - base
            for buf, new in ((kc, k_s), (vc, v_s)):
                tile = buf[b, pl.ds(base, ALIGN), :].astype(F32)
                buf[b, pl.ds(base, ALIGN), :] = jnp.where(hit, new[pl.ds(b, 1), :], tile).astype(BF16)
        return carry

    lax.fori_loop(0, tokens // 8, new_rows, 0)
    for copy in cache_out:
        copy.start()

    block = total_rows // 2
    lane = iota((block, tokens), 1).astype(F32)
    for k in range(1, cap // CHUNK + 1):
        @pl.when(jnp.maximum(chunks, 1) == k)
        def _():
            for b in range(2):
                at = pl.ds(b * block, block)
                where = pos_col[at, :]
                pick = jnp.concatenate([(where == lane + float(j * tokens)).astype(F32).astype(BF16)
                                        for j in range(k * CHUNK // tokens)], axis=1)

                def cols_body(i, carry):
                    cols = pl.ds(pl.multiple_of(i * COLS, COLS), COLS)
                    rows[at, cols] = mm(pick, sorted_out[0:k * CHUNK, cols]).astype(BF16)
                    return carry

                lax.fori_loop(0, dim // 512, cols_body, 0)
                pltpu.make_async_copy(rows.at[at], out_hbm.at[at], out_sems.at[b]).start()
    for b in range(2):
        at = pl.ds(b * block, block)
        pltpu.make_async_copy(rows.at[at], out_hbm.at[at], out_sems.at[b]).wait()
    for copy in cache_out:
        copy.wait()


def experts(meta, pos, k_new, v_new, kc, vc, mall, eg_t, eu_t, ed):
    ep, _, tokens = meta.shape
    dim = mall.shape[1]
    count = eg_t.shape[0]
    most = ep * tokens // 2 + count * (ALIGN - 1)
    cap = (most + CHUNK - 1) // CHUNK * CHUNK
    every = ep * tokens
    return pl.pallas_call(
        expert_kernel,
        name="experts",
        out_shape=(jax.ShapeDtypeStruct((every, dim), BF16), jax.ShapeDtypeStruct(kc.shape, BF16),
                   jax.ShapeDtypeStruct(vc.shape, BF16)),
        in_specs=[VMEM, SMEM, VMEM, VMEM] + [ANY] * 6,
        out_specs=(ANY, ANY, ANY),
        scratch_shapes=[
            pltpu.VMEM(kc.shape, BF16), pltpu.VMEM(vc.shape, BF16),
            pltpu.VMEM(k_new.shape, F32), pltpu.VMEM(v_new.shape, F32),
            pltpu.VMEM((every, dim), BF16), pltpu.VMEM((cap + WIN, dim), BF16), pltpu.VMEM((cap + WIN, dim), BF16),
            pltpu.VMEM((ep, tokens), F32), pltpu.VMEM((every, tokens), F32), pltpu.VMEM((ep, tokens), F32),
            pltpu.VMEM((cap + WIN, tokens), F32), pltpu.VMEM((3 * count, tokens), jnp.int32),
            pltpu.SMEM((3 * count, tokens), jnp.int32),
            pltpu.VMEM(eg_t.shape, BF16), pltpu.VMEM(eu_t.shape, BF16), pltpu.VMEM(ed.shape, BF16),
            pltpu.VMEM((cap, 128), BF16),
            pltpu.SemaphoreType.DMA, pltpu.SemaphoreType.DMA, pltpu.SemaphoreType.DMA((2, 2)),
            pltpu.SemaphoreType.DMA((3, count)),
            pltpu.SemaphoreType.DMA((2,))],
        compiler_params=pltpu.CompilerParams(vmem_limit_bytes=VMEM_LIMIT),
    )(meta, pos, k_new, v_new, kc, vc, mall, eg_t, eu_t, ed)


def back_kernel(hsum_ref, gres_ref, moe_hbm, wg_hbm, wu_hbm, wd_hbm, out_ref,
                keep, give, take, ring, relay_x, got_x, swap, own, c_s, wg, wu, wd, hid, part, relay, got, full,
                send_sems, recv_sems, load_sems):
    tokens, dim = hid.shape
    ep, me, core, partner, right, left, far = ring_ids()
    tp, mt = lax.axis_size("tp"), lax.axis_index("tp")
    halfd = dim // 2
    quart = halfd // 2
    pair = 2 * tokens
    mine = pl.ds(pl.multiple_of(core * halfd, halfd), halfd)
    other = pl.ds(pl.multiple_of((1 - core) * halfd, halfd), halfd)
    chips = [far // 2, right // 2, left // 2, me // 2]

    def rows_of(chip):
        return pl.ds(pl.multiple_of(chip * pair, pair), pair)

    give_loads = [pltpu.make_async_copy(moe_hbm.at[rows_of(chip), other], give.at[i], load_sems.at[i])
                  for i, chip in enumerate(chips)]
    keep_loads = [pltpu.make_async_copy(moe_hbm.at[rows_of(chip), mine], keep.at[i], load_sems.at[4 + i])
                  for i, chip in enumerate(chips)]
    w_loads = [pltpu.make_async_copy(s, d, load_sems.at[8 + i])
               for i, (s, d) in enumerate([(wg_hbm, wg), (wu_hbm, wu), (wd_hbm, wd)])]
    for load in give_loads + keep_loads + w_loads:
        load.start()
    meet([partner, right, left], [lax.rem(mt + 1, tp), lax.rem(mt + tp - 1, tp)])
    links = Links(send_sems, recv_sems)
    mid = RowSum(links, 17, "tp", hid)
    hid[mid.rows(mid.me, None), :] = hsum_ref[...]
    mid.spread()
    for i in range(4):
        give_loads[i].wait()
        links.send(i, give.at[i], take.at[i], {"ep": partner})

    def add_pair(i):
        keep_loads[i].wait()
        links.recv(i)
        ring[i] = (keep[i].astype(F32) + take[i].astype(F32)).astype(BF16)

    lo, hi = pl.ds(0, quart), pl.ds(quart, quart)
    to_right, to_left = {"ep": right}, {"ep": left}
    add_pair(0)
    links.send(4, ring.at[0, :, lo], relay_x.at[0], to_right)
    links.send(5, ring.at[0, :, hi], relay_x.at[1], to_left)
    add_pair(1)
    links.send(6, ring.at[1, :, hi], got_x.at[0, 1], to_right)
    add_pair(2)
    links.send(7, ring.at[2, :, lo], got_x.at[1, 0], to_left)
    add_pair(3)

    mid.forward()
    mid.finish()
    wide = hid[...].astype(F32)
    inv = rms(wide)
    c_s[...] = (wide * inv * gain_row(gres_ref)).astype(BF16)
    w_loads[0].wait()
    w_loads[1].wait()
    acts = []
    for i in range(wg.shape[1] // COLS):
        cols = span(i, COLS)
        gate = mm(c_s[...], wg[:, cols])
        up = mm(c_s[...], wu[:, cols])
        acts.append((jax.nn.silu(gate) * up).astype(BF16))
    act = jnp.concatenate(acts, axis=1)
    w_loads[2].wait()
    for i in range(dim // COLS):
        cols = span(i, COLS)
        own[:, cols] = mm(act, wd[:, cols])

    links.recv(4)
    relay_x[2] = (ring[1, :, 0:quart].astype(F32) + relay_x[0].astype(F32)).astype(BF16)
    links.send(8, relay_x.at[2], got_x.at[0, 0], to_right)
    links.recv(5)
    relay_x[3] = (ring[2, :, quart:halfd].astype(F32) + relay_x[1].astype(F32)).astype(BF16)
    links.send(9, relay_x.at[3], got_x.at[1, 1], to_left)
    links.recv(6, 7, 8, 9)
    mine_rows = pl.ds(pl.multiple_of(core * tokens, tokens), tokens)
    give_rows = pl.ds(pl.multiple_of((1 - core) * tokens, tokens), tokens)

    def arrived(at):
        pieces = []
        for q in (0, 1):
            cols = span(q, quart)
            pieces.append(ring[3, at, cols].astype(F32) + got_x[0, q, at, :].astype(F32)
                          + got_x[1, q, at, :].astype(F32))
        return jnp.concatenate(pieces, axis=1)

    swap[0] = arrived(give_rows).astype(BF16)
    links.send(10, swap.at[0], swap.at[1], {"ep": partner})
    own[:, mine] += arrived(mine_rows)
    part[:, mine] = own[:, mine].astype(BF16)
    links.recv(10)
    own[:, other] += swap[1].astype(F32)
    part[:, other] = own[:, other].astype(BF16)
    tp_sum = RowSum(links, 11, "tp", full, part, relay, got)
    tp_sum.start()
    tp_sum.pass_on()
    tp_sum.collect(own, hid)
    tp_sum.spread()
    tp_sum.forward()
    tp_sum.finish()
    out_ref[...] = full[...]
    links.drain()


def back(h_sum, g_res, moe, w_gate, w_up, w_down, tp):
    tokens, dim = h_sum.shape[0] * tp, h_sum.shape[1]
    pair, halfd, quart = 2 * tokens, dim // 2, dim // 4
    chips = moe.shape[0] // pair
    return pl.pallas_call(
        back_kernel,
        name="back",
        out_shape=jax.ShapeDtypeStruct((tokens, dim), BF16),
        in_specs=[VMEM, VMEM] + [ANY] * 4,
        out_specs=VMEM,
        scratch_shapes=[
            pltpu.VMEM((chips, pair, halfd), BF16), pltpu.VMEM((chips, pair, halfd), BF16),
            pltpu.VMEM((chips, pair, halfd), BF16), pltpu.VMEM((chips, pair, halfd), BF16),
            pltpu.VMEM((4, pair, quart), BF16), pltpu.VMEM((2, 2, pair, quart), BF16),
            pltpu.VMEM((2, tokens, halfd), BF16), pltpu.VMEM((tokens, dim), F32), pltpu.VMEM((tokens, dim), BF16),
            pltpu.VMEM(w_gate.shape, BF16), pltpu.VMEM(w_up.shape, BF16), pltpu.VMEM(w_down.shape, BF16),
            pltpu.VMEM((tokens, dim), BF16), *row_sum_scratch(tokens, dim, tp),
            pltpu.SemaphoreType.DMA((29,)), pltpu.SemaphoreType.DMA((29,)), pltpu.SemaphoreType.DMA((11,))],
        compiler_params=pltpu.CompilerParams(collective_id=1, has_side_effects=True, vmem_limit_bytes=VMEM_LIMIT),
    )(h_sum, g_res, moe, w_gate, w_up, w_down)


def solution(mesh):
    ep, tp = mesh.shape['ep'], mesh.shape['tp']
    row_spec = P(('dp', 'ep'), None)
    cache_spec = P(('dp', 'ep'), None, 'tp', None)
    col_split = P(None, 'tp')
    row_split = P('tp', None)
    in_specs = (row_spec, P(('dp', 'ep')), row_spec, cache_spec, cache_spec, P(None), P(None), P(None), col_split, col_split, col_split, row_split, col_split, col_split, row_split, P(None, None), P('ep', None, 'tp'), P('ep', None, 'tp'), P('ep', 'tp', None))
    out_specs = (row_spec, cache_spec, cache_spec)

    def local_layer(hidden_in, positions, expert_ids, k_cache, v_cache, norm_in, norm_res, norm_post, w_q, w_k, w_v, w_o, w_gate, w_up, w_down, w_router, e_gate, e_up, e_down):
        tokens, dim = hidden_in.shape
        slots, head = k_cache.shape[1], k_cache.shape[3]
        kc, vc = (cache.reshape(tokens, slots, head) for cache in (k_cache, v_cache))
        h_sum, k_new, v_new, meta, mall = front(
            hidden_in, expert_ids.T, positions, norm_in, norm_post, w_router, kc, vc, w_q, w_k, w_v, w_o, ep, tp)
        moe, k_out, v_out = experts(
            meta, positions, k_new, v_new, kc, vc, mall.reshape(ep * tokens, dim),
            jnp.swapaxes(e_gate, 1, 2), jnp.swapaxes(e_up, 1, 2), e_down)
        hidden_out = back(h_sum, norm_res, moe, w_gate, w_up, w_down, tp)
        return hidden_out, k_out.reshape(k_cache.shape), v_out.reshape(v_cache.shape)

    return jax.shard_map(local_layer, mesh=mesh, in_specs=in_specs, out_specs=out_specs, check_vma=False)
```

```python
import functools

import jax
import jax.numpy as jnp
import numpy as np
from jax import lax
from jax.experimental import pallas as pl
from jax.experimental.pallas import tpu as pltpu
from jax.sharding import PartitionSpec as P

NORM_EPS = 1e-5
ROPE_BASE = 10000.0
MESH = pl.DeviceIdType.MESH
F32 = jnp.float32
BF16 = jnp.bfloat16
WIN = 32
ALIGN = 16
COLS = 512
VMEM_LIMIT = 67000000

ANY = pl.BlockSpec(memory_space=pl.ANY)
VMEM = pl.BlockSpec(memory_space=pltpu.VMEM)
SMEM = pl.BlockSpec(memory_space=pltpu.SMEM)


def nt_dot(a, b):
    return lax.dot_general(a, b, (((1,), (1,)), ((), ())), preferred_element_type=F32)


def mm(a, b):
    return jnp.dot(a, b, preferred_element_type=F32)


def span(i, width):
    return slice(i * width, (i + 1) * width)


def total(v, axis):
    return jnp.sum(v, axis=axis, keepdims=True)


def exp_rows(v):
    return jnp.exp(v - jnp.max(v, axis=-1, keepdims=True))


def rms(wide):
    return lax.rsqrt(jnp.mean(wide * wide, axis=-1, keepdims=True) + NORM_EPS)


def iota(shape, dim):
    return lax.broadcasted_iota(jnp.int32, shape, dim)


def gain_row(ref):
    return ref[...].astype(F32).reshape(1, ref.shape[0])


class Links:
    def __init__(self, send_sems, recv_sems):
        self.send_sems, self.recv_sems, self.started, self.unsent = send_sems, recv_sems, {}, []

    def copy(self, i):
        src, dst, device = self.started[i]
        return pltpu.make_async_remote_copy(
            src_ref=src(), dst_ref=dst(), send_sem=self.send_sems.at[i], recv_sem=self.recv_sems.at[i],
            device_id=device, device_id_type=MESH)

    def send(self, i, src, device, dst=None):
        self.started[i] = (src, dst or src, device)
        self.copy(i).start()
        self.unsent.append(i)

    def recv(self, *ids):
        for i in ids:
            self.copy(i).wait_recv()

    def drain(self):
        for i in self.unsent:
            self.copy(i).wait_send()
        self.unsent = []


def at(ref, *index):
    return lambda: ref.at[index]


class RowSum:
    def __init__(self, links, base, axis, full, part=None, relay=None, got=None):
        self.links, self.base, self.part, self.relay, self.got, self.full = links, base, part, relay, got, full
        self.size = lax.axis_size(axis)
        self.me = lax.axis_index(axis)
        self.right = lax.rem(self.me + 1, self.size)
        self.left = lax.rem(self.me + self.size - 1, self.size)
        self.far = lax.rem(self.me + 2, self.size)
        self.to_right, self.to_left = {axis: self.right}, {axis: self.left}
        self.block = full.shape[0] // self.size
        self.half = self.block // 2

    def rows(self, rank, half):
        if half is None:
            return pl.ds(pl.multiple_of(rank * self.block, self.block), self.block)
        return pl.ds(pl.multiple_of(rank * self.block + half * self.half, self.half), self.half)

    def send(self, i, device, src, dst=None):
        buf, *rows = src
        self.links.send(self.base + i, (lambda: buf.at[self.rows(*rows)]) if rows else (lambda: buf), device, dst)

    def recv(self, *ids):
        self.links.recv(*[self.base + i for i in ids])

    def start(self):
        part, relay, got = self.part, self.relay, self.got
        self.send(0, self.to_right, (part, self.far, 0), at(relay, 0))
        self.send(1, self.to_left, (part, self.far, 1), at(relay, 1))
        self.send(2, self.to_right, (part, self.right, 1), at(got, 0, 1))
        self.send(3, self.to_left, (part, self.left, 0), at(got, 1, 0))

    def pass_on(self):
        part, relay = self.part, self.relay
        for n, (dest, device) in enumerate([(self.right, self.to_right), (self.left, self.to_left)]):
            self.recv(n)
            relay[2 + n] = (part[self.rows(dest, n), :].astype(F32) + relay[n].astype(F32)).astype(BF16)
            self.send(4 + n, device, (relay.at[2 + n],), at(self.got, n, n))

    def collect(self, own, rest):
        self.recv(2, 3, 4, 5)
        for half in range(2):
            here = self.rows(self.me, half)
            acc = own[here, :] + self.got[0, half].astype(F32) + self.got[1, half].astype(F32)
            self.full[here, :] = (rest[here, :].astype(F32) + acc).astype(BF16)

    def spread(self):
        for n, device in enumerate([self.to_right, self.to_left]):
            self.send(6 + n, device, (self.full, self.me, n))
        for n, device in enumerate([self.to_right, self.to_left]):
            self.send(8 + n, device, (self.full, self.me, 1 - n))

    def forward(self):
        for n, (block, device) in enumerate([(self.left, self.to_right), (self.right, self.to_left)]):
            self.recv(6 + n)
            self.send(10 + n, device, (self.full, block, n))

    def finish(self):
        self.recv(8, 9, 10, 11)


def row_sum_scratch(rows, cols, tp):
    half = rows // tp // 2
    return [pltpu.VMEM((rows, cols), BF16), pltpu.VMEM((4, half, cols), BF16),
            pltpu.VMEM((2, 2, half, cols), BF16), pltpu.VMEM((rows, cols), BF16)]


def ring_ids():
    ep = lax.axis_size("ep")
    me = lax.axis_index("ep")
    core = lax.rem(me, 2)
    partner = me + 1 - 2 * core
    return ep, me, core, partner, lax.rem(me + 2, ep), lax.rem(me + ep - 2, ep), lax.rem(me + 4, ep)


ROWS, ATT, FAR, META, TWIN, GIVE, RING, SWAP, LAST = 0, 5, 17, 20, 28, 34, 38, 44, 45
COPIES = 57


def layer_kernel(x_ref, ids_ref, pos_ref, gin_ref, gpost_ref, gres_ref, wr_ref, kc_hbm, vc_hbm, wq_hbm, wk_hbm, wv_hbm,
                 wo_hbm, eg_hbm, eu_hbm, ed_hbm, wg_hbm, wu_hbm, wd_hbm, out_ref, knew_ref, vnew_ref,
                 mall, meta, a_s, own, pos_row, pos_col, plan, plan_s, take, ring, relay_x, got_x, swap,
                 part, relay, got, hid, part_b, relay_b, got_b, full_b, send_sems, recv_sems, load_sems, plan_sem, w_sems):
    tokens, dim = x_ref.shape
    head = wk_hbm.shape[1]
    heads = wq_hbm.shape[1] // head
    slots = kc_hbm.shape[1]
    count, width = ed_hbm.shape[0], ed_hbm.shape[1]
    ep, me, core, partner, right, left, far = ring_ids()
    tp, mt = lax.axis_size("tp"), lax.axis_index("tp")
    to_right, to_left, to_partner = {"ep": right}, {"ep": left}, {"ep": partner}
    peers = [lax.rem(me + i, ep) for i in range(1, ep)]
    barrier = pltpu.get_barrier_semaphore()
    for peer in peers:
        pl.semaphore_signal(barrier, inc=1, device_id={"ep": peer}, device_id_type=MESH)
    for peer in (lax.rem(mt + 1, tp), lax.rem(mt + tp - 1, tp)):
        pl.semaphore_signal(barrier, inc=1, device_id={"tp": peer}, device_id_type=MESH)
    links = Links(send_sems, recv_sems)
    att_sum = RowSum(links, ATT, "tp", hid, part, relay, got)
    hrow = tokens // 2

    def half(i, h):
        return at(mall, i, pl.ds(h * hrow, hrow))

    def twin(i):
        return i + 1 - 2 * lax.rem(i, 2)

    def attention(kc, vc, wq, wk, wv, wo, q_s, o_s, k_s, v_s, pcol):
        loads = [pltpu.make_async_copy(src, dst, load_sems.at[i]) for i, (src, dst) in enumerate(
            [(wq_hbm, wq), (wk_hbm, wk), (wv_hbm, wv), (kc_hbm, kc), (vc_hbm, vc), (wo_hbm, wo)])]
        for load in loads:
            load.start()
        wide = x_ref[...].astype(F32)
        inv = rms(wide)
        mall[me] = (wide * inv * gain_row(gpost_ref)).astype(BF16)
        a_s[...] = (wide * inv * gain_row(gin_ref)).astype(BF16)
        pl.semaphore_wait(barrier, len(peers) + 2)
        first = [(0, right), (1, left), (1, right), (0, left)]
        for n, (h, device) in enumerate(first):
            links.send(ROWS + n, half(me, h), {"ep": device})
        links.send(ROWS + len(first), at(mall, me), to_partner)

        logits = mm(mall[me], wr_ref[...])
        probs = exp_rows(logits)
        probs = probs / total(probs, 1)
        experts = logits.shape[1]
        ids = ids_ref[...].astype(F32)
        lane = iota((tokens, experts), 1).astype(F32)
        id_rows = [ids[k:k + 1, :] for k in range(2)]
        picked = [total(jnp.where(jnp.transpose(jnp.broadcast_to(row, (experts, tokens))) == lane, probs, 0.0), 1)
                  for row in id_rows]
        both = picked[0] + picked[1]
        sub = iota((8, tokens), 0)
        block = jnp.zeros((8, tokens), F32)
        wts = [jnp.transpose(jnp.broadcast_to(p / both, (tokens, tokens)))[0:8, :] for p in picked]
        for n, row in enumerate(id_rows + wts):
            block = jnp.where(sub == n, row, block)
        meta[me] = block
        for n, peer in enumerate(peers):
            links.send(META + n, at(meta, me), {"ep": peer})

        def pos_body(g, carry):
            row = iota((8, head), 0)
            acc = jnp.zeros((8, head), jnp.int32)
            for j in range(8):
                acc = jnp.where(row == j, pos_ref[g * 8 + j], acc)
            pcol[pl.ds(pl.multiple_of(g * 8, 8), 8), :] = acc
            return carry

        lax.fori_loop(0, tokens // 8, pos_body, 0)
        spot = iota((tokens, head), 1)
        power = lax.rem(spot, head // 2).astype(F32) * (-np.log(ROPE_BASE) / (head // 2))
        angles = pcol[...].astype(F32) * jnp.exp(power)
        cosine = jnp.cos(angles)
        sine = jnp.sin(angles)
        sine = jnp.where(spot < head // 2, -sine, sine)

        def rope(v):
            return (v * cosine + pltpu.roll(v, head // 2, 1) * sine).astype(BF16).astype(F32)

        for load in loads[:3]:
            load.wait()
        normed = a_s[...]
        k_s[...] = rope(mm(normed, wk[...]))
        v_s[...] = mm(normed, wv[...]).astype(BF16).astype(F32)
        knew_ref[...] = k_s[...].astype(BF16)
        vnew_ref[...] = v_s[...].astype(BF16)
        for i in range(heads // 2):
            q2 = mm(normed, wq[:, span(i, 2 * head)])
            for j in range(2):
                q_s[2 * i + j] = rope(q2[:, span(j, head)])
        for load in loads[3:5]:
            load.wait()

        def attend(g, carry):
            base = pl.multiple_of(g * 8, 8)
            slot = iota((slots, head), 0)
            pairs = []
            for new, old in ((k_s, kc), (v_s, vc)):
                pieces = [jnp.where(slot == pos_ref[g * 8 + j], new[pl.ds(base + j, 1), :], old[base + j].astype(F32))
                          for j in range(8)]
                pairs.append(jnp.concatenate([piece.astype(BF16) for piece in pieces], axis=0))
            keys, vals = pairs
            q8 = q_s[:, pl.ds(base, 8), :].reshape(heads * 8, head).astype(BF16)
            scores = nt_dot(q8, keys) * (head ** -0.5)
            each = (8, 8 * slots)
            col = iota(each, 1)
            row_pos = jnp.concatenate([pcol[pl.ds(base, 8), :]] * (8 * slots // head), axis=1)
            mask = (col // slots == iota(each, 0)) & (lax.rem(col, slots) <= row_pos)
            mask = jnp.broadcast_to(mask[None], (heads, *each)).reshape(heads * 8, 8 * slots)
            e = exp_rows(jnp.where(mask, scores, -1e30))
            o8 = mm((e / total(e, 1)).astype(BF16), vals)
            o_s[:, pl.ds(base, 8), :] = o8.reshape(heads, 8, head)
            return carry

        lax.fori_loop(0, tokens // 8, attend, 0)
        mix = jnp.concatenate([o_s[i].astype(BF16) for i in range(heads)], axis=1)
        loads[5].wait()
        for i in range(dim // COLS):
            cols = span(i, COLS)
            piece = mm(mix, wo[:, cols])
            own[:, cols] = piece
            part[:, cols] = piece.astype(BF16)
        att_sum.start()

    kv = pltpu.VMEM((tokens, head), F32)
    each_head = pltpu.VMEM((heads, tokens, head), F32)
    pl.run_scoped(
        attention, *[pltpu.VMEM(ref.shape, BF16) for ref in (kc_hbm, vc_hbm, wq_hbm, wk_hbm, wv_hbm, wo_hbm)],
        each_head, each_head, kv, kv, pltpu.VMEM((tokens, head), jnp.int32))

    chips = [far // 2, right // 2, left // 2, me // 2]
    halfd = dim // 2
    quart = halfd // 2
    mine = pl.ds(pl.multiple_of(core * halfd, halfd), halfd)
    other = pl.ds(pl.multiple_of((1 - core) * halfd, halfd), halfd)
    lo, hi, full = pl.ds(0, quart), pl.ds(quart, quart), slice(None)

    def chip_rows(chip):
        return pl.ds(chip * 2, 2)

    def add_pair(i):
        links.recv(GIVE + i)
        for j in range(2):
            ring[i, j] = (mall[chips[i] * 2 + j, :, mine].astype(F32) + take[i, j].astype(F32)).astype(BF16)

    def moe(srt, wt_slot, eg, eu, ed):
        loads = []
        for i, (src, dst) in enumerate([(eg_hbm, eg), (eu_hbm, eu), (ed_hbm, ed)]):
            load = pltpu.make_async_copy(src, dst, w_sems.at[i])
            load.start()
            loads.append(load)
        cap = srt.shape[0]
        rows = min(cap, COLS)

        for n, (block, h, device) in enumerate([(left, 0, right), (right, 1, left)]):
            links.recv(ROWS + n)
            links.send(FAR + n, half(block, h), {"ep": device})
            links.send(TWIN + n, half(block, h), to_partner)

        links.recv(*range(META, META + len(peers)))
        begin = (me * count).astype(F32)
        before = (iota((tokens, tokens), 0) < iota((tokens, tokens), 1)).astype(F32).astype(BF16)
        expert = iota((count, tokens), 0).astype(F32)
        hots, ranks, local, wts = [], [], [], []
        seen = jnp.zeros((count, 1), F32)
        for s in range(ep):
            block = meta[s]
            one, two = block[0:1, :] - begin, block[1:2, :] - begin
            in_one = (one >= 0) & (one < count)
            in_two = (two >= 0) & (two < count)
            took = jnp.where(in_one, one, jnp.where(in_two, two, -1.0))
            wts.append(jnp.where(in_one, block[2:3, :], jnp.where(in_two, block[3:4, :], 0.0)))
            hot = (expert == took).astype(F32)
            hots.append(hot)
            local.append(took)
            ranks.append(mm(hot.astype(BF16), before) + seen)
            seen = seen + total(hot, 1)
        tiles = jnp.broadcast_to(jnp.floor((seen + (WIN - 1)) * (1.0 / WIN)), (count, tokens))
        earlier = (iota((count, count), 1) < iota((count, count), 0)).astype(F32).astype(BF16)
        start = mm(earlier, tiles.astype(BF16))
        ended = (start + tiles <= iota((count, tokens), 1).astype(F32)).astype(F32)
        plan[...] = jnp.broadcast_to(jnp.minimum(total(ended, 0), count - 1.0), plan.shape).astype(jnp.int32)
        plan_copy = pltpu.make_async_copy(plan, plan_s, plan_sem)
        plan_copy.start()
        for s in range(ep):
            place = total(hots[s] * (start * WIN + ranks[s]), 0)
            place = jnp.where(local[s] >= 0, place, -1.0)
            pos_row[s] = jnp.broadcast_to(place, (8, tokens))
            pos_col[s] = jnp.transpose(jnp.broadcast_to(place, (tokens, tokens)))
        plan_copy.wait()

        for c in range(cap // rows):
            slot = (iota((rows, tokens), 0) + c * rows).astype(F32)
            wt = jnp.zeros((rows, tokens), F32)
            for s in range(ep):
                wt = wt + jnp.where(slot == pos_row[s, 0:1, :], wts[s], 0.0)
            wt_slot[span(c, rows), :] = jnp.broadcast_to(total(wt, 1), (rows, tokens))

        def gather(one, fresh):
            two = twin(one)

            def body(c, carry):
                here = pl.ds(pl.multiple_of(c * rows, rows), rows)
                slot = (iota((rows, tokens), 0) + c * rows).astype(F32)
                pick = jnp.concatenate([(slot == pos_row[s, 0:1, :]).astype(F32).astype(BF16) for s in (one, two)], axis=1)
                for i in range(dim // COLS):
                    cols = span(i, COLS)
                    got_rows = mm(pick, jnp.concatenate([mall[one, :, cols], mall[two, :, cols]], axis=0))
                    if not fresh:
                        got_rows = got_rows + srt[here, cols].astype(F32)
                    srt[here, cols] = got_rows.astype(BF16)
                return carry

            lax.fori_loop(0, cap // rows, body, 0)

        links.recv(ROWS + 4)
        gather(me, True)
        att_sum.pass_on()
        att_sum.collect(own, x_ref)
        att_sum.spread()
        for n, (block, h) in enumerate([(left, 1), (right, 0)]):
            links.recv(ROWS + 2 + n)
            links.send(TWIN + 2 + n, half(block, h), to_partner)
        att_sum.forward()
        for n, block in enumerate([left, right]):
            links.recv(TWIN + n, TWIN + 2 + n)
            gather(block, False)
        for n in range(2):
            links.recv(FAR + n)
            links.send(TWIN + 4 + n, half(far, n), to_partner)
        att_sum.finish()
        links.recv(TWIN + 4, TWIN + 5)
        gather(far, False)
        for load in loads:
            load.wait()

        def tile(i, carry):
            e = jnp.minimum(jnp.maximum(plan_s[0, i], 0), count - 1)
            here = pl.ds(pl.multiple_of(i * WIN, WIN), WIN)
            x = srt[here, :]
            act = jnp.transpose(jax.nn.silu(nt_dot(eg[e], x)) * nt_dot(eu[e], x)).astype(BF16)
            wt = wt_slot[here, :][:, 0:1]
            for i in range(dim // COLS):
                cols = span(i, COLS)
                srt[here, cols] = (mm(act, ed[e, :, cols]) * wt).astype(BF16)
            return carry

        lax.fori_loop(0, cap // WIN, tile, 0)
        links.drain()

        lane = iota((2 * tokens, tokens), 1).astype(F32)

        def scatter(i):
            where = pos_col[chip_rows(chips[i])].reshape(2 * tokens, tokens)
            pick = jnp.concatenate([(where == lane + j * tokens).astype(F32).astype(BF16)
                                    for j in range(cap // tokens)], axis=1)
            for n in range(dim // COLS):
                cols = span(n, COLS)
                mall[chip_rows(chips[i]), :, cols] = mm(pick, srt[:, cols]).astype(BF16).reshape(2, tokens, COLS)
            links.send(GIVE + i, lambda: mall.at[chip_rows(chips[i]), :, other], to_partner, at(take, i))

        scatter(0)
        scatter(1)
        add_pair(0)
        links.send(RING, at(ring, 0, full, full, lo), to_right, at(relay_x, 0))
        links.send(RING + 1, at(ring, 0, full, full, hi), to_left, at(relay_x, 1))
        scatter(2)
        add_pair(1)
        links.send(RING + 2, at(ring, 1, full, full, hi), to_right, at(got_x, 0, 1))
        scatter(3)
        add_pair(2)
        links.send(RING + 3, at(ring, 2, full, full, lo), to_left, at(got_x, 1, 0))
        add_pair(3)

    cap = ep * tokens // 2 + count * WIN
    pl.run_scoped(
        moe, pltpu.VMEM((cap, dim), BF16), pltpu.VMEM((cap, tokens), F32),
        *[pltpu.VMEM(ref.shape, BF16) for ref in (eg_hbm, eu_hbm, ed_hbm)])

    def dense(wg, wu, wd):
        loads = [pltpu.make_async_copy(src, dst, load_sems.at[i])
                 for i, (src, dst) in enumerate([(wg_hbm, wg), (wu_hbm, wu), (wd_hbm, wd)])]
        for load in loads:
            load.start()
        wide = hid[...].astype(F32)
        a_s[...] = (wide * rms(wide) * gain_row(gres_ref)).astype(BF16)
        for load in loads[:2]:
            load.wait()
        acts = []
        for i in range(wg.shape[1] // COLS):
            cols = span(i, COLS)
            acts.append((jax.nn.silu(mm(a_s[...], wg[:, cols])) * mm(a_s[...], wu[:, cols])).astype(BF16))
        act = jnp.concatenate(acts, axis=1)
        loads[2].wait()
        for i in range(dim // COLS):
            cols = span(i, COLS)
            own[:, cols] = mm(act, wd[:, cols])

    pl.run_scoped(dense, *[pltpu.VMEM(ref.shape, BF16) for ref in (wg_hbm, wu_hbm, wd_hbm)])

    for n, (dest, cols, device, side) in enumerate([(1, span(0, quart), to_right, 0), (2, span(1, quart), to_left, 1)]):
        links.recv(RING + n)
        relay_x[2 + n] = (ring[dest, :, :, cols].astype(F32) + relay_x[n].astype(F32)).astype(BF16)
        links.send(RING + 4 + n, at(relay_x, 2 + n), device, at(got_x, side, n))
    links.recv(*range(RING + 2, SWAP))

    def arrived(j):
        return jnp.concatenate(
            [ring[3, j, :, span(q, quart)].astype(F32) + got_x[0, q, j].astype(F32) + got_x[1, q, j].astype(F32)
             for q in range(2)], axis=1)

    swap[0] = arrived(1 - core).astype(BF16)
    links.send(SWAP, at(swap, 0), to_partner, at(swap, 1))
    last = RowSum(links, LAST, "tp", full_b, part_b, relay_b, got_b)
    own[:, mine] += arrived(core)
    part_b[:, mine] = own[:, mine].astype(BF16)
    links.recv(SWAP)
    own[:, other] += swap[1].astype(F32)
    part_b[:, other] = own[:, other].astype(BF16)
    last.start()
    last.pass_on()
    last.collect(own, hid)
    last.spread()
    last.forward()
    last.finish()
    out_ref[...] = full_b[...]
    links.drain()


def layer(x, ids_t, pos, g_in, g_post, g_res, w_router, kc, vc, w_q, w_k, w_v, w_o, eg_t, eu_t, ed, w_gate, w_up, w_down, ep, tp):
    tokens, dim = x.shape
    head = w_k.shape[1]
    chips, halfd, quart = ep // 2, dim // 2, dim // 4
    shape = jax.ShapeDtypeStruct
    return pl.pallas_call(
        layer_kernel,
        name="layer",
        out_shape=(shape((tokens, dim), BF16), shape((tokens, head), BF16), shape((tokens, head), BF16)),
        in_specs=[VMEM, VMEM, SMEM] + [VMEM] * 4 + [ANY] * 12,
        out_specs=(VMEM, VMEM, VMEM),
        scratch_shapes=[
            pltpu.VMEM((ep, tokens, dim), BF16), pltpu.VMEM((ep, 8, tokens), F32), pltpu.VMEM((tokens, dim), BF16),
            pltpu.VMEM((tokens, dim), F32), pltpu.VMEM((ep, 8, tokens), F32), pltpu.VMEM((ep, tokens, tokens), F32),
            pltpu.VMEM((8, tokens), jnp.int32), pltpu.SMEM((8, tokens), jnp.int32),
            pltpu.VMEM((chips, 2, tokens, halfd), BF16), pltpu.VMEM((chips, 2, tokens, halfd), BF16),
            pltpu.VMEM((4, 2, tokens, quart), BF16), pltpu.VMEM((2, 2, 2, tokens, quart), BF16),
            pltpu.VMEM((2, tokens, halfd), BF16), *row_sum_scratch(tokens, dim, tp), *row_sum_scratch(tokens, dim, tp),
            pltpu.SemaphoreType.DMA((COPIES,)), pltpu.SemaphoreType.DMA((COPIES,)), pltpu.SemaphoreType.DMA((6,)),
            pltpu.SemaphoreType.DMA, pltpu.SemaphoreType.DMA((3,))],
        compiler_params=pltpu.CompilerParams(collective_id=0, has_side_effects=True, vmem_limit_bytes=VMEM_LIMIT),
    )(x, ids_t, pos, g_in, g_post, g_res, w_router, kc, vc, w_q, w_k, w_v, w_o, eg_t, eu_t, ed, w_gate, w_up, w_down)


def cache_kernel(pos_ref, knew_ref, vnew_ref, hid_ref, kc_hbm, vc_hbm, out_ref, ko_hbm, vo_hbm, kc, vc, k_s, v_s, sems):
    tokens, _, head = kc.shape
    caches = [(kc_hbm, kc, ko_hbm), (vc_hbm, vc, vo_hbm)]
    cache_in = [pltpu.make_async_copy(src, buf, sems.at[0, i]) for i, (src, buf, _) in enumerate(caches)]
    cache_out = [pltpu.make_async_copy(buf, dst, sems.at[1, i]) for i, (_, buf, dst) in enumerate(caches)]
    for copy in cache_in:
        copy.start()
    out_ref[...] = hid_ref[...]
    k_s[...] = knew_ref[...].astype(F32)
    v_s[...] = vnew_ref[...].astype(F32)
    for buf, new, came, goes in zip((kc, vc), (k_s, v_s), cache_in, cache_out):
        came.wait()

        def new_rows(g, carry):
            for j in range(8):
                b = g * 8 + j
                spot = pos_ref[b]
                base = pl.multiple_of(spot // ALIGN * ALIGN, ALIGN)
                hit = iota((ALIGN, head), 0) == spot - base
                tile = buf[b, pl.ds(base, ALIGN), :].astype(F32)
                buf[b, pl.ds(base, ALIGN), :] = jnp.where(hit, new[pl.ds(b, 1), :], tile).astype(BF16)
            return carry

        lax.fori_loop(0, tokens // 8, new_rows, 0)
        goes.start()
    for copy in cache_out:
        copy.wait()


def caches(pos, k_new, v_new, hid, kc, vc):
    shape = jax.ShapeDtypeStruct
    return pl.pallas_call(
        cache_kernel,
        name="caches",
        out_shape=(shape(hid.shape, BF16), shape(kc.shape, BF16), shape(vc.shape, BF16)),
        in_specs=[SMEM, VMEM, VMEM, VMEM, ANY, ANY],
        out_specs=(VMEM, ANY, ANY),
        scratch_shapes=[pltpu.VMEM(kc.shape, BF16), pltpu.VMEM(vc.shape, BF16), pltpu.VMEM(k_new.shape, F32),
                        pltpu.VMEM(v_new.shape, F32), pltpu.SemaphoreType.DMA((2, 2))],
    )(pos, k_new, v_new, hid, kc, vc)


def solution(mesh):
    ep, tp = mesh.shape['ep'], mesh.shape['tp']
    row_spec = P(('dp', 'ep'), None)
    cache_spec = P(('dp', 'ep'), None, 'tp', None)
    col_split = P(None, 'tp')
    row_split = P('tp', None)
    in_specs = (row_spec, P(('dp', 'ep')), row_spec, cache_spec, cache_spec, P(None), P(None), P(None), col_split, col_split, col_split, row_split, col_split, col_split, row_split, P(None, None), P('ep', None, 'tp'), P('ep', None, 'tp'), P('ep', 'tp', None))
    out_specs = (row_spec, cache_spec, cache_spec)

    def local_layer(hidden_in, positions, expert_ids, k_cache, v_cache, norm_in, norm_res, norm_post, w_q, w_k, w_v, w_o, w_gate, w_up, w_down, w_router, e_gate, e_up, e_down):
        tokens, dim = hidden_in.shape
        slots, head = k_cache.shape[1], k_cache.shape[3]
        kc, vc = (cache.reshape(tokens, slots, head) for cache in (k_cache, v_cache))
        hid, k_new, v_new = layer(
            hidden_in, expert_ids.T, positions, norm_in, norm_post, norm_res, w_router, kc, vc, w_q, w_k, w_v, w_o,
            jnp.swapaxes(e_gate, 1, 2), jnp.swapaxes(e_up, 1, 2), e_down, w_gate, w_up, w_down, ep, tp)
        hidden_out, k_out, v_out = caches(positions, k_new, v_new, hid, kc, vc)
        return hidden_out, k_out.reshape(k_cache.shape), v_out.reshape(v_cache.shape)

    return jax.shard_map(local_layer, mesh=mesh, in_specs=in_specs, out_specs=out_specs, check_vma=False)
```

```python
import functools

import jax
import jax.numpy as jnp
import numpy as np
from jax import lax
from jax.experimental import pallas as pl
from jax.experimental.pallas import tpu as pltpu
from jax.sharding import PartitionSpec as P

NORM_EPS = 1e-5
ROPE_BASE = 10000.0
MESH = pl.DeviceIdType.MESH
F32 = jnp.float32
BF16 = jnp.bfloat16
WIN = 64
ALIGN = 16
AHEAD = 8
COLS = 512
PARTS = 4
VMEM_LIMIT = 67000000

ANY = pl.BlockSpec(memory_space=pl.ANY)
VMEM = pl.BlockSpec(memory_space=pltpu.VMEM)
SMEM = pl.BlockSpec(memory_space=pltpu.SMEM)


def nt_dot(a, b):
    return lax.dot_general(a, b, (((1,), (1,)), ((), ())), preferred_element_type=F32)


def mm(a, b):
    return jnp.dot(a, b, preferred_element_type=F32)


def span(i, width):
    return slice(i * width, (i + 1) * width)


def total(v, axis):
    return jnp.sum(v, axis=axis, keepdims=True)


def exp_rows(v):
    return jnp.exp(v - jnp.max(v, axis=-1, keepdims=True))


def rms(wide):
    return lax.rsqrt(jnp.mean(wide * wide, axis=-1, keepdims=True) + NORM_EPS)


def iota(shape, dim):
    return lax.broadcasted_iota(jnp.int32, shape, dim)


def gain_row(ref):
    return ref[...].astype(F32).reshape(1, ref.shape[0])


class Links:
    def __init__(self, send_sems, recv_sems):
        self.send_sems, self.recv_sems, self.started, self.unsent = send_sems, recv_sems, {}, []

    def copy(self, i):
        src, dst, device = self.started[i]
        return pltpu.make_async_remote_copy(
            src_ref=src(), dst_ref=dst(), send_sem=self.send_sems.at[i], recv_sem=self.recv_sems.at[i],
            device_id=device, device_id_type=MESH)

    def send(self, i, src, device, dst=None):
        self.started[i] = (src, dst or src, device)
        self.copy(i).start()
        self.unsent.append(i)

    def recv(self, *ids):
        for i in ids:
            self.copy(i).wait_recv()

    def drain(self):
        for i in self.unsent:
            self.copy(i).wait_send()
        self.unsent = []


def pieces_of(src, dst, sems, i, parts):
    size = src.shape[0] // parts
    copies = [pltpu.make_async_copy(src.at[pl.ds(n * size, size)], dst.at[pl.ds(n * size, size)], sems.at[i, n])
              for n in range(parts)]
    for copy in copies:
        copy.start()
    return copies


def finish(copies):
    for copy in copies:
        copy.wait()


def at(ref, *index):
    return lambda: ref.at[index]


class RowSum:
    def __init__(self, links, base, axis, full, part=None, relay=None, got=None):
        self.links, self.base, self.part, self.relay, self.got, self.full = links, base, part, relay, got, full
        self.size = lax.axis_size(axis)
        self.me = lax.axis_index(axis)
        self.right = lax.rem(self.me + 1, self.size)
        self.left = lax.rem(self.me + self.size - 1, self.size)
        self.far = lax.rem(self.me + 2, self.size)
        self.to_right, self.to_left = {axis: self.right}, {axis: self.left}
        self.block = full.shape[0] // self.size
        self.half = self.block // 2

    def rows(self, rank, half):
        if half is None:
            return pl.ds(pl.multiple_of(rank * self.block, self.block), self.block)
        return pl.ds(pl.multiple_of(rank * self.block + half * self.half, self.half), self.half)

    def send(self, i, device, src, dst=None):
        buf, *rows = src
        self.links.send(self.base + i, (lambda: buf.at[self.rows(*rows)]) if rows else (lambda: buf), device, dst)

    def recv(self, *ids):
        self.links.recv(*[self.base + i for i in ids])

    def start(self):
        part, relay, got = self.part, self.relay, self.got
        self.send(0, self.to_right, (part, self.far, 0), at(relay, 0))
        self.send(1, self.to_left, (part, self.far, 1), at(relay, 1))
        self.send(2, self.to_right, (part, self.right, 1), at(got, 0, 1))
        self.send(3, self.to_left, (part, self.left, 0), at(got, 1, 0))

    def pass_on(self):
        part, relay = self.part, self.relay
        for n, (dest, device) in enumerate([(self.right, self.to_right), (self.left, self.to_left)]):
            self.recv(n)
            relay[2 + n] = (part[self.rows(dest, n), :].astype(F32) + relay[n].astype(F32)).astype(BF16)
            self.send(4 + n, device, (relay.at[2 + n],), at(self.got, n, n))

    def collect(self, own, rest):
        self.recv(2, 3, 4, 5)
        for half in range(2):
            here = self.rows(self.me, half)
            acc = own[here, :] + self.got[0, half].astype(F32) + self.got[1, half].astype(F32)
            self.full[here, :] = (rest[here, :].astype(F32) + acc).astype(BF16)

    def spread(self):
        for n, device in enumerate([self.to_right, self.to_left]):
            self.send(6 + n, device, (self.full, self.me, n))
        for n, device in enumerate([self.to_right, self.to_left]):
            self.send(8 + n, device, (self.full, self.me, 1 - n))

    def forward(self):
        for n, (block, device) in enumerate([(self.left, self.to_right), (self.right, self.to_left)]):
            self.recv(6 + n)
            self.send(10 + n, device, (self.full, block, n))

    def finish(self):
        self.recv(8, 9, 10, 11)


def row_sum_scratch(rows, cols, tp):
    half = rows // tp // 2
    return [pltpu.VMEM((rows, cols), BF16), pltpu.VMEM((4, half, cols), BF16),
            pltpu.VMEM((2, 2, half, cols), BF16), pltpu.VMEM((rows, cols), BF16)]


def ring_ids():
    ep = lax.axis_size("ep")
    me = lax.axis_index("ep")
    core = lax.rem(me, 2)
    partner = me + 1 - 2 * core
    return ep, me, core, partner, lax.rem(me + 2, ep), lax.rem(me + ep - 2, ep), lax.rem(me + 4, ep)


ROWS, ATT, FAR, META, TWIN, FRONT_COPIES = 0, 5, 17, 20, 28, 34
GIVE, RING, SWAP, LAST, MID, BACK_COPIES = 0, 4, 10, 11, 23, 35


def front_kernel(x_ref, ids_ref, pos_ref, gin_ref, gpost_ref, wr_ref, kc_hbm, vc_hbm, wq_hbm, wk_hbm, wv_hbm, wo_hbm,
                 hsum_ref, knew_ref, vnew_ref, place_ref, plan_ref, wt_slot, srt,
                 mall, meta, a_s, own, pos_row, part, relay, got, hid, send_sems, recv_sems, load_sems):
    tokens, dim = x_ref.shape
    head = wk_hbm.shape[1]
    heads = wq_hbm.shape[1] // head
    slots = kc_hbm.shape[1]
    count = plan_ref.shape[0] // 2
    ep, me, core, partner, right, left, far = ring_ids()
    tp, mt = lax.axis_size("tp"), lax.axis_index("tp")
    to_right, to_left, to_partner = {"ep": right}, {"ep": left}, {"ep": partner}
    peers = [lax.rem(me + i, ep) for i in range(1, ep)]
    barrier = pltpu.get_barrier_semaphore()
    for peer in peers:
        pl.semaphore_signal(barrier, inc=1, device_id={"ep": peer}, device_id_type=MESH)
    for peer in (lax.rem(mt + 1, tp), lax.rem(mt + tp - 1, tp)):
        pl.semaphore_signal(barrier, inc=1, device_id={"tp": peer}, device_id_type=MESH)
    links = Links(send_sems, recv_sems)
    att_sum = RowSum(links, ATT, "tp", hid, part, relay, got)
    hrow = tokens // 2

    def half(i, h):
        return at(mall, i, pl.ds(h * hrow, hrow))

    def twin(i):
        return i + 1 - 2 * lax.rem(i, 2)

    def attention(kc, vc, wq, wk, wv, wo, q_s, o_s, k_s, v_s, pcol):
        loads = [pieces_of(src, dst, load_sems, i, PARTS) for i, (src, dst) in enumerate(
            [(wq_hbm, wq), (wk_hbm, wk), (wv_hbm, wv), (kc_hbm, kc), (vc_hbm, vc), (wo_hbm, wo)])]
        wide = x_ref[...].astype(F32)
        inv = rms(wide)
        mall[me] = (wide * inv * gain_row(gpost_ref)).astype(BF16)
        a_s[...] = (wide * inv * gain_row(gin_ref)).astype(BF16)
        pl.semaphore_wait(barrier, len(peers) + 2)
        first = [(0, right), (1, left), (1, right), (0, left)]
        for n, (h, device) in enumerate(first):
            links.send(ROWS + n, half(me, h), {"ep": device})
        links.send(ROWS + len(first), at(mall, me), to_partner)

        logits = mm(mall[me], wr_ref[...])
        probs = exp_rows(logits)
        probs = probs / total(probs, 1)
        experts = logits.shape[1]
        ids = ids_ref[...].astype(F32)
        lane = iota((tokens, experts), 1).astype(F32)
        id_rows = [ids[k:k + 1, :] for k in range(2)]
        picked = [total(jnp.where(jnp.transpose(jnp.broadcast_to(row, (experts, tokens))) == lane, probs, 0.0), 1)
                  for row in id_rows]
        both = picked[0] + picked[1]
        sub = iota((8, tokens), 0)
        block = jnp.zeros((8, tokens), F32)
        wts = [jnp.transpose(jnp.broadcast_to(p / both, (tokens, tokens)))[0:8, :] for p in picked]
        for n, row in enumerate(id_rows + wts):
            block = jnp.where(sub == n, row, block)
        meta[me] = block
        for n, peer in enumerate(peers):
            links.send(META + n, at(meta, me), {"ep": peer})

        def pos_body(g, carry):
            row = iota((8, head), 0)
            acc = jnp.zeros((8, head), jnp.int32)
            for j in range(8):
                acc = jnp.where(row == j, pos_ref[g * 8 + j], acc)
            pcol[pl.ds(pl.multiple_of(g * 8, 8), 8), :] = acc
            return carry

        lax.fori_loop(0, tokens // 8, pos_body, 0)
        spot = iota((tokens, head), 1)
        power = lax.rem(spot, head // 2).astype(F32) * (-np.log(ROPE_BASE) / (head // 2))
        angles = pcol[...].astype(F32) * jnp.exp(power)
        cosine = jnp.cos(angles)
        sine = jnp.sin(angles)
        sine = jnp.where(spot < head // 2, -sine, sine)

        def rope(v):
            return (v * cosine + pltpu.roll(v, head // 2, 1) * sine).astype(BF16).astype(F32)

        for load in loads[:3]:
            finish(load)
        normed = a_s[...]
        k_s[...] = rope(mm(normed, wk[...]))
        v_s[...] = mm(normed, wv[...]).astype(BF16).astype(F32)
        knew_ref[...] = k_s[...].astype(BF16)
        vnew_ref[...] = v_s[...].astype(BF16)
        for i in range(heads // 2):
            q2 = mm(normed, wq[:, span(i, 2 * head)])
            for j in range(2):
                q_s[2 * i + j] = rope(q2[:, span(j, head)])
        for load in loads[3:5]:
            finish(load)

        def attend(g, carry):
            base = pl.multiple_of(g * 8, 8)
            slot = iota((slots, head), 0)
            pairs = []
            for new, old in ((k_s, kc), (v_s, vc)):
                pieces = [jnp.where(slot == pos_ref[g * 8 + j], new[pl.ds(base + j, 1), :], old[base + j].astype(F32))
                          for j in range(8)]
                pairs.append(jnp.concatenate([piece.astype(BF16) for piece in pieces], axis=0))
            keys, vals = pairs
            q8 = q_s[:, pl.ds(base, 8), :].reshape(heads * 8, head).astype(BF16)
            scores = nt_dot(q8, keys) * (head ** -0.5)
            each = (8, 8 * slots)
            col = iota(each, 1)
            row_pos = jnp.concatenate([pcol[pl.ds(base, 8), :]] * (8 * slots // head), axis=1)
            mask = (col // slots == iota(each, 0)) & (lax.rem(col, slots) <= row_pos)
            mask = jnp.broadcast_to(mask[None], (heads, *each)).reshape(heads * 8, 8 * slots)
            e = exp_rows(jnp.where(mask, scores, -1e30))
            o8 = mm((e / total(e, 1)).astype(BF16), vals)
            o_s[:, pl.ds(base, 8), :] = o8.reshape(heads, 8, head)
            return carry

        lax.fori_loop(0, tokens // 8, attend, 0)
        mix = jnp.concatenate([o_s[i].astype(BF16) for i in range(heads)], axis=1)
        finish(loads[5])
        for i in range(dim // COLS):
            cols = span(i, COLS)
            piece = mm(mix, wo[:, cols])
            own[:, cols] = piece
            part[:, cols] = piece.astype(BF16)
        att_sum.start()

    kv = pltpu.VMEM((tokens, head), F32)
    each_head = pltpu.VMEM((heads, tokens, head), F32)
    pl.run_scoped(
        attention, *[pltpu.VMEM(ref.shape, BF16) for ref in (kc_hbm, vc_hbm, wq_hbm, wk_hbm, wv_hbm, wo_hbm)],
        each_head, each_head, kv, kv, pltpu.VMEM((tokens, head), jnp.int32))

    cap = srt.shape[0]
    rows = cap // 2

    for n, (block, h, device) in enumerate([(left, 0, right), (right, 1, left)]):
        links.recv(ROWS + n)
        links.send(FAR + n, half(block, h), {"ep": device})
        links.send(TWIN + n, half(block, h), to_partner)

    links.recv(*range(META, META + len(peers)))
    begin = (me * count).astype(F32)
    before = (iota((tokens, tokens), 0) < iota((tokens, tokens), 1)).astype(F32).astype(BF16)
    expert = iota((count, tokens), 0).astype(F32)
    hots, ranks, local, wts = [], [], [], []
    seen = jnp.zeros((count, 1), F32)
    for s in range(ep):
        block = meta[s]
        one, two = block[0:1, :] - begin, block[1:2, :] - begin
        in_one = (one >= 0) & (one < count)
        in_two = (two >= 0) & (two < count)
        took = jnp.where(in_one, one, jnp.where(in_two, two, -1.0))
        wts.append(jnp.where(in_one, block[2:3, :], jnp.where(in_two, block[3:4, :], 0.0)))
        hot = (expert == took).astype(F32)
        hots.append(hot)
        local.append(took)
        ranks.append(mm(hot.astype(BF16), before) + seen)
        seen = seen + total(hot, 1)
    padded = jnp.broadcast_to(jnp.floor((seen + (ALIGN - 1)) * (1.0 / ALIGN)) * ALIGN, (count, tokens))
    earlier = (iota((count, count), 1) < iota((count, count), 0)).astype(F32).astype(BF16)
    start = mm(earlier, padded.astype(BF16))
    plan_ref[0:count, :] = jnp.broadcast_to(seen, (count, tokens)).astype(jnp.int32)
    plan_ref[count:, :] = start.astype(jnp.int32)
    for s in range(ep):
        place = total(hots[s] * (start + ranks[s]), 0)
        place = jnp.where(local[s] >= 0, place, -1.0)
        pos_row[s] = jnp.broadcast_to(place, (8, tokens))
        place_ref[s:s + 1, :] = place

    wt_slot[cap:, :] = jnp.zeros((WIN, tokens), F32)
    for c in range(cap // rows):
        slot = (iota((rows, tokens), 0) + c * rows).astype(F32)
        wt = jnp.zeros((rows, tokens), F32)
        for s in range(ep):
            wt = wt + jnp.where(slot == pos_row[s, 0:1, :], wts[s], 0.0)
        wt_slot[span(c, rows), :] = jnp.broadcast_to(total(wt, 1), (rows, tokens))

    def gather(one, fresh):
        two = twin(one)

        def body(c, carry):
            here = pl.ds(pl.multiple_of(c * rows, rows), rows)
            slot = (iota((rows, tokens), 0) + c * rows).astype(F32)
            pick = jnp.concatenate([(slot == pos_row[s, 0:1, :]).astype(F32).astype(BF16) for s in (one, two)], axis=1)
            for i in range(dim // COLS):
                cols = span(i, COLS)
                got_rows = mm(pick, jnp.concatenate([mall[one, :, cols], mall[two, :, cols]], axis=0))
                if not fresh:
                    got_rows = got_rows + srt[here, cols].astype(F32)
                srt[here, cols] = got_rows.astype(BF16)
            return carry

        lax.fori_loop(0, cap // rows, body, 0)

    links.recv(ROWS + 4)
    gather(me, True)
    att_sum.pass_on()
    for n, (block, h) in enumerate([(left, 1), (right, 0)]):
        links.recv(ROWS + 2 + n)
        links.send(TWIN + 2 + n, half(block, h), to_partner)
    att_sum.collect(own, x_ref)
    hsum_ref[...] = hid[att_sum.rows(mt, None), :]
    for n, block in enumerate([left, right]):
        links.recv(TWIN + n, TWIN + 2 + n)
        gather(block, False)
    for n in range(2):
        links.recv(FAR + n)
        links.send(TWIN + 4 + n, half(far, n), to_partner)
    links.recv(TWIN + 4, TWIN + 5)
    gather(far, False)
    links.drain()


def sorted_rows(ep, tokens, count):
    most = ep * tokens // 2 + count * (ALIGN - 1)
    return -(-most // (2 * tokens)) * 2 * tokens


def front(x, ids_t, pos, g_in, g_post, w_router, kc, vc, w_q, w_k, w_v, w_o, count, ep, tp):
    tokens, dim = x.shape
    head = w_k.shape[1]
    cap = sorted_rows(ep, tokens, count)
    shape = jax.ShapeDtypeStruct
    return pl.pallas_call(
        front_kernel,
        name="front",
        out_shape=(shape((tokens // tp, dim), BF16), shape((tokens, head), BF16), shape((tokens, head), BF16),
                   shape((ep, tokens), F32), shape((2 * count, tokens), jnp.int32), shape((cap + WIN, tokens), F32),
                   shape((cap, dim), BF16)),
        in_specs=[VMEM, VMEM, SMEM] + [VMEM] * 3 + [ANY] * 6,
        out_specs=(VMEM,) * 7,
        scratch_shapes=[
            pltpu.VMEM((ep, tokens, dim), BF16), pltpu.VMEM((ep, 8, tokens), F32), pltpu.VMEM((tokens, dim), BF16),
            pltpu.VMEM((tokens, dim), F32), pltpu.VMEM((ep, 8, tokens), F32), *row_sum_scratch(tokens, dim, tp),
            pltpu.SemaphoreType.DMA((FRONT_COPIES,)), pltpu.SemaphoreType.DMA((FRONT_COPIES,)),
            pltpu.SemaphoreType.DMA((6, PARTS))],
        compiler_params=pltpu.CompilerParams(collective_id=0, has_side_effects=True, vmem_limit_bytes=VMEM_LIMIT),
    )(x, ids_t, pos, g_in, g_post, w_router, kc, vc, w_q, w_k, w_v, w_o)


def expert_kernel(plan_ref, pos_ref, wt_slot, knew_ref, vnew_ref, kc_hbm, vc_hbm, srt_hbm, eg_hbm, eu_hbm, ed_hbm,
                  out_hbm, ko_hbm, vo_hbm, kc, vc, k_s, v_s, rows, out, eg, eu, ed, rows_sem, cache_sems, w_sems):
    count = eg.shape[0]
    tokens, _, head = kc.shape
    cap, dim = srt_hbm.shape

    def weights(e):
        return [pltpu.make_async_copy(src.at[e], dst.at[e], w_sems.at[i, e])
                for i, (src, dst) in enumerate([(eg_hbm, eg), (eu_hbm, eu), (ed_hbm, ed)])]

    news = ((k_s, kc, kc_hbm, ko_hbm), (v_s, vc, vc_hbm, vo_hbm))
    rows_copy = pltpu.make_async_copy(srt_hbm, rows.at[pl.ds(0, cap)], rows_sem.at[0])
    rows_copy.start()
    came = [pieces_of(src, buf, cache_sems, i, PARTS) for i, (_, buf, src, _) in enumerate(news)]
    for e in range(AHEAD):
        for copy in weights(e):
            copy.start()
    k_s[...] = knew_ref[...].astype(F32)
    v_s[...] = vnew_ref[...].astype(F32)
    out[...] = jnp.zeros_like(out)
    step = tokens // PARTS
    goes = []
    for n in range(PARTS):
        for i, (new, buf, _, dst) in enumerate(news):
            came[i][n].wait()

            def new_rows(g, carry):
                for j in range(8):
                    b = n * step + g * 8 + j
                    spot = pos_ref[b]
                    base = pl.multiple_of(spot // ALIGN * ALIGN, ALIGN)
                    hit = iota((ALIGN, head), 0) == spot - base
                    tile = buf[b, pl.ds(base, ALIGN), :].astype(F32)
                    buf[b, pl.ds(base, ALIGN), :] = jnp.where(hit, new[pl.ds(b, 1), :], tile).astype(BF16)
                return carry

            lax.fori_loop(0, step // 8, new_rows, 0)
            part = pl.ds(n * step, step)
            goes.append(pltpu.make_async_copy(buf.at[part], dst.at[part], cache_sems.at[2 + i, n]))
            goes[-1].start()
    rows_copy.wait()

    def run_expert(e, carry):
        @pl.when(e + AHEAD < count)
        def _():
            for copy in weights(e + AHEAD):
                copy.start()

        for copy in weights(e):
            copy.wait()
        passes = (plan_ref[e, 0] + (WIN - 1)) // WIN
        begin = plan_ref[count + e, 0]

        def one_pass(p, inner):
            here = pl.ds(pl.multiple_of(begin + p * WIN, ALIGN), WIN)
            x = rows[here, :]
            act = jnp.transpose(jax.nn.silu(nt_dot(eg[e], x)) * nt_dot(eu[e], x)).astype(BF16)
            wt = wt_slot[here, :][:, 0:1]
            for i in range(dim // COLS):
                cols = span(i, COLS)
                out[here, cols] = (mm(act, ed[e, :, cols]) * wt).astype(BF16)
            return inner

        lax.fori_loop(0, passes, one_pass, 0)
        return carry

    lax.fori_loop(0, count, run_expert, 0)
    out_copy = pltpu.make_async_copy(out.at[pl.ds(0, cap)], out_hbm, rows_sem.at[1])
    out_copy.start()
    out_copy.wait()
    finish(goes)


def experts(plan, pos, wt_slot, k_new, v_new, kc, vc, srt, eg_t, eu_t, ed):
    shape = jax.ShapeDtypeStruct
    count = ed.shape[0]
    room = (srt.shape[0] + WIN, srt.shape[1])
    return pl.pallas_call(
        expert_kernel,
        name="experts",
        out_shape=(shape(srt.shape, BF16), shape(kc.shape, BF16), shape(vc.shape, BF16)),
        in_specs=[SMEM, SMEM, VMEM, VMEM, VMEM] + [ANY] * 6,
        out_specs=(ANY, ANY, ANY),
        scratch_shapes=[
            pltpu.VMEM(kc.shape, BF16), pltpu.VMEM(vc.shape, BF16), pltpu.VMEM(k_new.shape, F32),
            pltpu.VMEM(v_new.shape, F32), pltpu.VMEM(room, BF16), pltpu.VMEM(room, BF16),
            *[pltpu.VMEM(w.shape, BF16) for w in (eg_t, eu_t, ed)],
            pltpu.SemaphoreType.DMA((2,)), pltpu.SemaphoreType.DMA((4, PARTS)), pltpu.SemaphoreType.DMA((3, count))],
        compiler_params=pltpu.CompilerParams(vmem_limit_bytes=VMEM_LIMIT),
    )(plan, pos, wt_slot, k_new, v_new, kc, vc, srt, eg_t, eu_t, ed)


def back_kernel(hsum_ref, gres_ref, place_ref, srt_hbm, wg_hbm, wu_hbm, wd_hbm, out_ref,
                srt, mall, pos_col, wg, wu, wd, a_s, own, take, ring, relay_x, got_x, swap, hid,
                part_b, relay_b, got_b, full_b, send_sems, recv_sems, load_sems):
    ep, tokens, dim = mall.shape
    cap = srt.shape[0]
    ep, me, core, partner, right, left, far = ring_ids()
    tp, mt = lax.axis_size("tp"), lax.axis_index("tp")
    to_right, to_left, to_partner = {"ep": right}, {"ep": left}, {"ep": partner}
    rows_in = pieces_of(srt_hbm, srt, load_sems, 3, 1)
    loads = [pieces_of(src, dst, load_sems, i, PARTS) for i, (src, dst) in enumerate(
        [(wg_hbm, wg), (wu_hbm, wu), (wd_hbm, wd)])]
    barrier = pltpu.get_barrier_semaphore()
    peers = [{"ep": i} for i in (partner, right, left)] + [{"tp": lax.rem(mt + i, tp)} for i in (1, tp - 1)]
    for peer in peers:
        pl.semaphore_signal(barrier, inc=1, device_id=peer, device_id_type=MESH)
    for s in range(ep):
        pos_col[s] = jnp.transpose(jnp.broadcast_to(place_ref[s:s + 1, :], (tokens, tokens)))
    pl.semaphore_wait(barrier, len(peers))
    links = Links(send_sems, recv_sems)
    mid = RowSum(links, MID, "tp", hid)
    hid[mid.rows(mt, None), :] = hsum_ref[...]
    mid.spread()
    chips = [far // 2, right // 2, left // 2, me // 2]
    halfd = dim // 2
    quart = halfd // 2
    mine = pl.ds(pl.multiple_of(core * halfd, halfd), halfd)
    other = pl.ds(pl.multiple_of((1 - core) * halfd, halfd), halfd)
    lo, hi, full = pl.ds(0, quart), pl.ds(quart, quart), slice(None)

    def chip_rows(chip):
        return pl.ds(chip * 2, 2)

    def add_pair(i):
        links.recv(GIVE + i)
        for j in range(2):
            ring[i, j] = (mall[chips[i] * 2 + j, :, mine].astype(F32) + take[i, j].astype(F32)).astype(BF16)

    lane = iota((2 * tokens, tokens), 1).astype(F32)

    def scatter(i):
        where = pos_col[chip_rows(chips[i])].reshape(2 * tokens, tokens)
        pick = jnp.concatenate([(where == lane + j * tokens).astype(F32).astype(BF16)
                                for j in range(cap // tokens)], axis=1)
        for n in range(dim // COLS):
            cols = span(n, COLS)
            mall[chip_rows(chips[i]), :, cols] = mm(pick, srt[:, cols]).astype(BF16).reshape(2, tokens, COLS)
        links.send(GIVE + i, lambda: mall.at[chip_rows(chips[i]), :, other], to_partner, at(take, i))

    finish(rows_in[0:1])
    scatter(0)
    scatter(1)
    add_pair(0)
    links.send(RING, at(ring, 0, full, full, lo), to_right, at(relay_x, 0))
    links.send(RING + 1, at(ring, 0, full, full, hi), to_left, at(relay_x, 1))
    scatter(2)
    add_pair(1)
    links.send(RING + 2, at(ring, 1, full, full, hi), to_right, at(got_x, 0, 1))
    scatter(3)
    add_pair(2)
    links.send(RING + 3, at(ring, 2, full, full, lo), to_left, at(got_x, 1, 0))
    add_pair(3)
    mid.forward()
    mid.finish()
    wide = hid[...].astype(F32)
    a_s[...] = (wide * rms(wide) * gain_row(gres_ref)).astype(BF16)
    for load in loads[:2]:
        finish(load)
    acts = []
    for i in range(wg.shape[1] // COLS):
        cols = span(i, COLS)
        acts.append((jax.nn.silu(mm(a_s[...], wg[:, cols])) * mm(a_s[...], wu[:, cols])).astype(BF16))
    act = jnp.concatenate(acts, axis=1)
    finish(loads[2])
    for i in range(dim // COLS):
        cols = span(i, COLS)
        own[:, cols] = mm(act, wd[:, cols])

    for n, (dest, cols, device, side) in enumerate([(1, span(0, quart), to_right, 0), (2, span(1, quart), to_left, 1)]):
        links.recv(RING + n)
        relay_x[2 + n] = (ring[dest, :, :, cols].astype(F32) + relay_x[n].astype(F32)).astype(BF16)
        links.send(RING + 4 + n, at(relay_x, 2 + n), device, at(got_x, side, n))
    links.recv(*range(RING + 2, SWAP))

    def arrived(j):
        return jnp.concatenate(
            [ring[3, j, :, span(q, quart)].astype(F32) + got_x[0, q, j].astype(F32) + got_x[1, q, j].astype(F32)
             for q in range(2)], axis=1)

    swap[0] = arrived(1 - core).astype(BF16)
    links.send(SWAP, at(swap, 0), to_partner, at(swap, 1))
    last = RowSum(links, LAST, "tp", full_b, part_b, relay_b, got_b)
    own[:, mine] += arrived(core)
    part_b[:, mine] = own[:, mine].astype(BF16)
    links.recv(SWAP)
    own[:, other] += swap[1].astype(F32)
    part_b[:, other] = own[:, other].astype(BF16)
    last.start()
    last.pass_on()
    last.collect(own, hid)
    last.spread()
    last.forward()
    last.finish()
    out_ref[...] = full_b[...]
    links.drain()


def back(h_sum, g_res, place, srt, w_gate, w_up, w_down, tp):
    tokens, dim = h_sum.shape[0] * tp, h_sum.shape[1]
    ep = place.shape[0]
    chips, halfd, quart = ep // 2, dim // 2, dim // 4
    return pl.pallas_call(
        back_kernel,
        name="back",
        out_shape=jax.ShapeDtypeStruct((tokens, dim), BF16),
        in_specs=[VMEM, VMEM, VMEM] + [ANY] * 4,
        out_specs=VMEM,
        scratch_shapes=[
            pltpu.VMEM(srt.shape, BF16), pltpu.VMEM((ep, tokens, dim), BF16), pltpu.VMEM((ep, tokens, tokens), F32),
            *[pltpu.VMEM(w.shape, BF16) for w in (w_gate, w_up, w_down)],
            pltpu.VMEM((tokens, dim), BF16), pltpu.VMEM((tokens, dim), F32),
            pltpu.VMEM((chips, 2, tokens, halfd), BF16), pltpu.VMEM((chips, 2, tokens, halfd), BF16),
            pltpu.VMEM((4, 2, tokens, quart), BF16), pltpu.VMEM((2, 2, 2, tokens, quart), BF16),
            pltpu.VMEM((2, tokens, halfd), BF16), pltpu.VMEM((tokens, dim), BF16), *row_sum_scratch(tokens, dim, tp),
            pltpu.SemaphoreType.DMA((BACK_COPIES,)), pltpu.SemaphoreType.DMA((BACK_COPIES,)),
            pltpu.SemaphoreType.DMA((4, PARTS))],
        compiler_params=pltpu.CompilerParams(collective_id=1, has_side_effects=True, vmem_limit_bytes=VMEM_LIMIT),
    )(h_sum, g_res, place, srt, w_gate, w_up, w_down)


def solution(mesh):
    ep, tp = mesh.shape['ep'], mesh.shape['tp']
    row_spec = P(('dp', 'ep'), None)
    cache_spec = P(('dp', 'ep'), None, 'tp', None)
    col_split = P(None, 'tp')
    row_split = P('tp', None)
    in_specs = (row_spec, P(('dp', 'ep')), row_spec, cache_spec, cache_spec, P(None), P(None), P(None), col_split, col_split, col_split, row_split, col_split, col_split, row_split, P(None, None), P('ep', None, 'tp'), P('ep', None, 'tp'), P('ep', 'tp', None))
    out_specs = (row_spec, cache_spec, cache_spec)

    def local_layer(hidden_in, positions, expert_ids, k_cache, v_cache, norm_in, norm_res, norm_post, w_q, w_k, w_v, w_o, w_gate, w_up, w_down, w_router, e_gate, e_up, e_down):
        tokens, dim = hidden_in.shape
        slots, head = k_cache.shape[1], k_cache.shape[3]
        kc, vc = (cache.reshape(tokens, slots, head) for cache in (k_cache, v_cache))
        h_sum, k_new, v_new, place, plan, wt_slot, srt = front(
            hidden_in, expert_ids.T, positions, norm_in, norm_post, w_router, kc, vc, w_q, w_k, w_v, w_o,
            e_down.shape[0], ep, tp)
        out, k_out, v_out = experts(
            plan, positions, wt_slot, k_new, v_new, kc, vc, srt, jnp.swapaxes(e_gate, 1, 2), jnp.swapaxes(e_up, 1, 2), e_down)
        hidden_out = back(h_sum, norm_res, place, out, w_gate, w_up, w_down, tp)
        return hidden_out, k_out.reshape(k_cache.shape), v_out.reshape(v_cache.shape)

    return jax.shard_map(local_layer, mesh=mesh, in_specs=in_specs, out_specs=out_specs, check_vma=False)
```

```python
import functools

import jax
import jax.numpy as jnp
import numpy as np
from jax import lax
from jax.experimental import pallas as pl
from jax.experimental.pallas import tpu as pltpu
from jax.sharding import PartitionSpec as P

NORM_EPS = 1e-5
ROPE_BASE = 10000.0
MESH = pl.DeviceIdType.MESH
F32 = jnp.float32
BF16 = jnp.bfloat16
WIN = 64
ALIGN = 16
AHEAD = 6
COLS = 512
PARTS = 4
VMEM_LIMIT = 67000000

ANY = pl.BlockSpec(memory_space=pl.ANY)
VMEM = pl.BlockSpec(memory_space=pltpu.VMEM)
SMEM = pl.BlockSpec(memory_space=pltpu.SMEM)


def nt_dot(a, b):
    return lax.dot_general(a, b, (((1,), (1,)), ((), ())), preferred_element_type=F32)


def mm(a, b):
    return jnp.dot(a, b, preferred_element_type=F32)


def span(i, width):
    return slice(i * width, (i + 1) * width)


def total(v, axis):
    return jnp.sum(v, axis=axis, keepdims=True)


def exp_rows(v):
    return jnp.exp(v - jnp.max(v, axis=-1, keepdims=True))


def rms(wide):
    return lax.rsqrt(jnp.mean(wide * wide, axis=-1, keepdims=True) + NORM_EPS)


def iota(shape, dim):
    return lax.broadcasted_iota(jnp.int32, shape, dim)


def gain_row(ref):
    return ref[...].astype(F32).reshape(1, ref.shape[0])


class Links:
    def __init__(self, send_sems, recv_sems):
        self.send_sems, self.recv_sems, self.started, self.unsent = send_sems, recv_sems, {}, []

    def copy(self, i):
        src, dst, device = self.started[i]
        return pltpu.make_async_remote_copy(
            src_ref=src(), dst_ref=dst(), send_sem=self.send_sems.at[i], recv_sem=self.recv_sems.at[i],
            device_id=device, device_id_type=MESH)

    def send(self, i, src, device, dst=None):
        self.started[i] = (src, dst or src, device)
        self.copy(i).start()
        self.unsent.append(i)

    def recv(self, *ids):
        for i in ids:
            self.copy(i).wait_recv()

    def drain(self):
        for i in self.unsent:
            self.copy(i).wait_send()
        self.unsent = []


def pieces_of(src, dst, sems, i, parts):
    size = src.shape[0] // parts
    copies = [pltpu.make_async_copy(src.at[pl.ds(n * size, size)], dst.at[pl.ds(n * size, size)], sems.at[i, n])
              for n in range(parts)]
    for copy in copies:
        copy.start()
    return copies


def finish(copies):
    for copy in copies:
        copy.wait()


def at(ref, *index):
    return lambda: ref.at[index]


class RowSum:
    def __init__(self, links, base, axis, full, part=None, relay=None, got=None):
        self.links, self.base, self.part, self.relay, self.got, self.full = links, base, part, relay, got, full
        self.size = lax.axis_size(axis)
        self.me = lax.axis_index(axis)
        self.right = lax.rem(self.me + 1, self.size)
        self.left = lax.rem(self.me + self.size - 1, self.size)
        self.far = lax.rem(self.me + 2, self.size)
        self.to_right, self.to_left = {axis: self.right}, {axis: self.left}
        self.block = full.shape[0] // self.size
        self.half = self.block // 2

    def rows(self, rank, half):
        if half is None:
            return pl.ds(pl.multiple_of(rank * self.block, self.block), self.block)
        return pl.ds(pl.multiple_of(rank * self.block + half * self.half, self.half), self.half)

    def send(self, i, device, src, dst=None):
        buf, *rows = src
        self.links.send(self.base + i, (lambda: buf.at[self.rows(*rows)]) if rows else (lambda: buf), device, dst)

    def recv(self, *ids):
        self.links.recv(*[self.base + i for i in ids])

    def start(self):
        part, relay, got = self.part, self.relay, self.got
        self.send(0, self.to_right, (part, self.far, 0), at(relay, 0))
        self.send(1, self.to_left, (part, self.far, 1), at(relay, 1))
        self.send(2, self.to_right, (part, self.right, 1), at(got, 0, 1))
        self.send(3, self.to_left, (part, self.left, 0), at(got, 1, 0))

    def pass_on(self):
        part, relay = self.part, self.relay
        for n, (dest, device) in enumerate([(self.right, self.to_right), (self.left, self.to_left)]):
            self.recv(n)
            relay[2 + n] = (part[self.rows(dest, n), :].astype(F32) + relay[n].astype(F32)).astype(BF16)
            self.send(4 + n, device, (relay.at[2 + n],), at(self.got, n, n))

    def collect(self, own, rest):
        self.recv(2, 3, 4, 5)
        for half in range(2):
            here = self.rows(self.me, half)
            acc = own[here, :] + self.got[0, half].astype(F32) + self.got[1, half].astype(F32)
            self.full[here, :] = (rest[here, :].astype(F32) + acc).astype(BF16)

    def spread(self):
        for n, device in enumerate([self.to_right, self.to_left]):
            self.send(6 + n, device, (self.full, self.me, n))
        for n, device in enumerate([self.to_right, self.to_left]):
            self.send(8 + n, device, (self.full, self.me, 1 - n))

    def forward(self):
        for n, (block, device) in enumerate([(self.left, self.to_right), (self.right, self.to_left)]):
            self.recv(6 + n)
            self.send(10 + n, device, (self.full, block, n))

    def finish(self):
        self.recv(8, 9, 10, 11)


def row_sum_scratch(rows, cols, tp):
    half = rows // tp // 2
    return [pltpu.VMEM((rows, cols), BF16), pltpu.VMEM((4, half, cols), BF16),
            pltpu.VMEM((2, 2, half, cols), BF16), pltpu.VMEM((rows, cols), BF16)]


def ring_ids():
    ep = lax.axis_size("ep")
    me = lax.axis_index("ep")
    core = lax.rem(me, 2)
    partner = me + 1 - 2 * core
    return ep, me, core, partner, lax.rem(me + 2, ep), lax.rem(me + ep - 2, ep), lax.rem(me + 4, ep)


ROWS, ATT, FAR, META, TWIN, FRONT_COPIES = 0, 5, 17, 20, 28, 34
GIVE, RING, SWAP, LAST, MID, BACK_COPIES = 0, 4, 10, 11, 23, 35


def front_kernel(x_ref, ids_ref, pos_ref, gin_ref, gpost_ref, wr_ref, kc_hbm, vc_hbm, wq_hbm, wk_hbm, wv_hbm, wo_hbm,
                 hsum_ref, knew_ref, vnew_ref, place_ref, plan_ref, wt_slot, srt,
                 mall, meta, a_s, own, pos_row, part, relay, got, hid, send_sems, recv_sems, load_sems):
    tokens, dim = x_ref.shape
    head = wk_hbm.shape[1]
    heads = wq_hbm.shape[1] // head
    slots = kc_hbm.shape[1]
    count = plan_ref.shape[0] // 2
    ep, me, core, partner, right, left, far = ring_ids()
    tp, mt = lax.axis_size("tp"), lax.axis_index("tp")
    to_right, to_left, to_partner = {"ep": right}, {"ep": left}, {"ep": partner}
    peers = [lax.rem(me + i, ep) for i in range(1, ep)]
    barrier = pltpu.get_barrier_semaphore()
    for peer in peers:
        pl.semaphore_signal(barrier, inc=1, device_id={"ep": peer}, device_id_type=MESH)
    for peer in (lax.rem(mt + 1, tp), lax.rem(mt + tp - 1, tp)):
        pl.semaphore_signal(barrier, inc=1, device_id={"tp": peer}, device_id_type=MESH)
    links = Links(send_sems, recv_sems)
    att_sum = RowSum(links, ATT, "tp", hid, part, relay, got)
    hrow = tokens // 2

    def half(i, h):
        return at(mall, i, pl.ds(h * hrow, hrow))

    def twin(i):
        return i + 1 - 2 * lax.rem(i, 2)

    def attention(kc, vc, wq, wk, wv, wo, q_s, o_s, k_s, v_s, pcol):
        loads = [pieces_of(src, dst, load_sems, i, PARTS) for i, (src, dst) in enumerate(
            [(wq_hbm, wq), (wk_hbm, wk), (wv_hbm, wv), (kc_hbm, kc), (vc_hbm, vc), (wo_hbm, wo)])]
        wide = x_ref[...].astype(F32)
        inv = rms(wide)
        mall[me] = (wide * inv * gain_row(gpost_ref)).astype(BF16)
        a_s[...] = (wide * inv * gain_row(gin_ref)).astype(BF16)
        pl.semaphore_wait(barrier, len(peers) + 2)
        first = [(0, right), (1, left), (1, right), (0, left)]
        for n, (h, device) in enumerate(first):
            links.send(ROWS + n, half(me, h), {"ep": device})
        links.send(ROWS + len(first), at(mall, me), to_partner)

        logits = mm(mall[me], wr_ref[...])
        probs = exp_rows(logits)
        probs = probs / total(probs, 1)
        experts = logits.shape[1]
        ids = ids_ref[...].astype(F32)
        lane = iota((tokens, experts), 1).astype(F32)
        id_rows = [ids[k:k + 1, :] for k in range(2)]
        picked = [total(jnp.where(jnp.transpose(jnp.broadcast_to(row, (experts, tokens))) == lane, probs, 0.0), 1)
                  for row in id_rows]
        both = picked[0] + picked[1]
        sub = iota((8, tokens), 0)
        block = jnp.zeros((8, tokens), F32)
        wts = [jnp.transpose(jnp.broadcast_to(p / both, (tokens, tokens)))[0:8, :] for p in picked]
        for n, row in enumerate(id_rows + wts):
            block = jnp.where(sub == n, row, block)
        meta[me] = block
        for n, peer in enumerate(peers):
            links.send(META + n, at(meta, me), {"ep": peer})

        def pos_body(g, carry):
            row = iota((8, head), 0)
            acc = jnp.zeros((8, head), jnp.int32)
            for j in range(8):
                acc = jnp.where(row == j, pos_ref[g * 8 + j], acc)
            pcol[pl.ds(pl.multiple_of(g * 8, 8), 8), :] = acc
            return carry

        lax.fori_loop(0, tokens // 8, pos_body, 0)
        spot = iota((tokens, head), 1)
        power = lax.rem(spot, head // 2).astype(F32) * (-np.log(ROPE_BASE) / (head // 2))
        angles = pcol[...].astype(F32) * jnp.exp(power)
        cosine = jnp.cos(angles)
        sine = jnp.sin(angles)
        sine = jnp.where(spot < head // 2, -sine, sine)

        def rope(v):
            return (v * cosine + pltpu.roll(v, head // 2, 1) * sine).astype(BF16).astype(F32)

        for load in loads[:3]:
            finish(load)
        normed = a_s[...]
        k_s[...] = rope(mm(normed, wk[...]))
        v_s[...] = mm(normed, wv[...]).astype(BF16).astype(F32)
        knew_ref[...] = k_s[...].astype(BF16)
        vnew_ref[...] = v_s[...].astype(BF16)
        for i in range(heads // 2):
            q2 = mm(normed, wq[:, span(i, 2 * head)])
            for j in range(2):
                q_s[2 * i + j] = rope(q2[:, span(j, head)])
        for load in loads[3:5]:
            finish(load)

        def attend(g, carry):
            base = pl.multiple_of(g * 8, 8)
            slot = iota((slots, head), 0)
            pairs = []
            for new, old in ((k_s, kc), (v_s, vc)):
                pieces = [jnp.where(slot == pos_ref[g * 8 + j], new[pl.ds(base + j, 1), :], old[base + j].astype(F32))
                          for j in range(8)]
                pairs.append(jnp.concatenate([piece.astype(BF16) for piece in pieces], axis=0))
            keys, vals = pairs
            q8 = q_s[:, pl.ds(base, 8), :].reshape(heads * 8, head).astype(BF16)
            scores = nt_dot(q8, keys) * (head ** -0.5)
            each = (8, 8 * slots)
            col = iota(each, 1)
            row_pos = jnp.concatenate([pcol[pl.ds(base, 8), :]] * (8 * slots // head), axis=1)
            mask = (col // slots == iota(each, 0)) & (lax.rem(col, slots) <= row_pos)
            mask = jnp.broadcast_to(mask[None], (heads, *each)).reshape(heads * 8, 8 * slots)
            e = exp_rows(jnp.where(mask, scores, -1e30))
            o8 = mm((e / total(e, 1)).astype(BF16), vals)
            o_s[:, pl.ds(base, 8), :] = o8.reshape(heads, 8, head)
            return carry

        lax.fori_loop(0, tokens // 8, attend, 0)
        mix = jnp.concatenate([o_s[i].astype(BF16) for i in range(heads)], axis=1)
        finish(loads[5])
        for i in range(dim // COLS):
            cols = span(i, COLS)
            piece = mm(mix, wo[:, cols])
            own[:, cols] = piece
            part[:, cols] = piece.astype(BF16)
        att_sum.start()

    kv = pltpu.VMEM((tokens, head), F32)
    each_head = pltpu.VMEM((heads, tokens, head), F32)
    pl.run_scoped(
        attention, *[pltpu.VMEM(ref.shape, BF16) for ref in (kc_hbm, vc_hbm, wq_hbm, wk_hbm, wv_hbm, wo_hbm)],
        each_head, each_head, kv, kv, pltpu.VMEM((tokens, head), jnp.int32))

    cap = srt.shape[0]
    rows = cap // 2

    for n, (block, h, device) in enumerate([(left, 0, right), (right, 1, left)]):
        links.recv(ROWS + n)
        links.send(FAR + n, half(block, h), {"ep": device})
        links.send(TWIN + n, half(block, h), to_partner)

    links.recv(*range(META, META + len(peers)))
    begin = (me * count).astype(F32)
    before = (iota((tokens, tokens), 0) < iota((tokens, tokens), 1)).astype(F32).astype(BF16)
    expert = iota((count, tokens), 0).astype(F32)
    hots, ranks, local, wts = [], [], [], []
    seen = jnp.zeros((count, 1), F32)
    for s in range(ep):
        block = meta[s]
        one, two = block[0:1, :] - begin, block[1:2, :] - begin
        in_one = (one >= 0) & (one < count)
        in_two = (two >= 0) & (two < count)
        took = jnp.where(in_one, one, jnp.where(in_two, two, -1.0))
        wts.append(jnp.where(in_one, block[2:3, :], jnp.where(in_two, block[3:4, :], 0.0)))
        hot = (expert == took).astype(F32)
        hots.append(hot)
        local.append(took)
        ranks.append(mm(hot.astype(BF16), before) + seen)
        seen = seen + total(hot, 1)
    padded = jnp.broadcast_to(jnp.floor((seen + (ALIGN - 1)) * (1.0 / ALIGN)) * ALIGN, (count, tokens))
    earlier = (iota((count, count), 1) < iota((count, count), 0)).astype(F32).astype(BF16)
    start = mm(earlier, padded.astype(BF16))
    plan_ref[0:count, :] = jnp.broadcast_to(seen, (count, tokens)).astype(jnp.int32)
    plan_ref[count:, :] = start.astype(jnp.int32)
    for s in range(ep):
        place = total(hots[s] * (start + ranks[s]), 0)
        place = jnp.where(local[s] >= 0, place, -1.0)
        pos_row[s] = jnp.broadcast_to(place, (8, tokens))
        place_ref[s:s + 1, :] = place

    wt_slot[cap:, :] = jnp.zeros((WIN, tokens), F32)
    for c in range(cap // rows):
        slot = (iota((rows, tokens), 0) + c * rows).astype(F32)
        wt = jnp.zeros((rows, tokens), F32)
        for s in range(ep):
            wt = wt + jnp.where(slot == pos_row[s, 0:1, :], wts[s], 0.0)
        wt_slot[span(c, rows), :] = jnp.broadcast_to(total(wt, 1), (rows, tokens))

    def gather(one, fresh):
        two = twin(one)

        def body(c, carry):
            here = pl.ds(pl.multiple_of(c * rows, rows), rows)
            slot = (iota((rows, tokens), 0) + c * rows).astype(F32)
            pick = jnp.concatenate([(slot == pos_row[s, 0:1, :]).astype(F32).astype(BF16) for s in (one, two)], axis=1)
            for i in range(dim // COLS):
                cols = span(i, COLS)
                got_rows = mm(pick, jnp.concatenate([mall[one, :, cols], mall[two, :, cols]], axis=0))
                if not fresh:
                    got_rows = got_rows + srt[here, cols].astype(F32)
                srt[here, cols] = got_rows.astype(BF16)
            return carry

        lax.fori_loop(0, cap // rows, body, 0)

    links.recv(ROWS + 4)
    gather(me, True)
    att_sum.pass_on()
    for n, (block, h) in enumerate([(left, 1), (right, 0)]):
        links.recv(ROWS + 2 + n)
        links.send(TWIN + 2 + n, half(block, h), to_partner)
    att_sum.collect(own, x_ref)
    hsum_ref[...] = hid[att_sum.rows(mt, None), :]
    for n, block in enumerate([left, right]):
        links.recv(TWIN + n, TWIN + 2 + n)
        gather(block, False)
    for n in range(2):
        links.recv(FAR + n)
        links.send(TWIN + 4 + n, half(far, n), to_partner)
    links.recv(TWIN + 4, TWIN + 5)
    gather(far, False)
    links.drain()


def sorted_rows(ep, tokens, count):
    most = ep * tokens // 2 + count * (ALIGN - 1)
    return -(-most // (2 * tokens)) * 2 * tokens


def front(x, ids_t, pos, g_in, g_post, w_router, kc, vc, w_q, w_k, w_v, w_o, count, ep, tp):
    tokens, dim = x.shape
    head = w_k.shape[1]
    cap = sorted_rows(ep, tokens, count)
    shape = jax.ShapeDtypeStruct
    return pl.pallas_call(
        front_kernel,
        name="front",
        out_shape=(shape((tokens // tp, dim), BF16), shape((tokens, head), BF16), shape((tokens, head), BF16),
                   shape((ep, tokens), F32), shape((2 * count, tokens), jnp.int32), shape((cap + WIN, tokens), F32),
                   shape((cap, dim), BF16)),
        in_specs=[VMEM, VMEM, SMEM] + [VMEM] * 3 + [ANY] * 6,
        out_specs=(VMEM,) * 7,
        scratch_shapes=[
            pltpu.VMEM((ep, tokens, dim), BF16), pltpu.VMEM((ep, 8, tokens), F32), pltpu.VMEM((tokens, dim), BF16),
            pltpu.VMEM((tokens, dim), F32), pltpu.VMEM((ep, 8, tokens), F32), *row_sum_scratch(tokens, dim, tp),
            pltpu.SemaphoreType.DMA((FRONT_COPIES,)), pltpu.SemaphoreType.DMA((FRONT_COPIES,)),
            pltpu.SemaphoreType.DMA((6, PARTS))],
        compiler_params=pltpu.CompilerParams(collective_id=0, has_side_effects=True, vmem_limit_bytes=VMEM_LIMIT),
    )(x, ids_t, pos, g_in, g_post, w_router, kc, vc, w_q, w_k, w_v, w_o)


def expert_kernel(plan_ref, pos_ref, wt_slot, knew_ref, vnew_ref, kc_hbm, vc_hbm, srt_hbm, eg_hbm, eu_hbm, ed_hbm,
                  out_hbm, ko_hbm, vo_hbm, kc, vc, k_s, v_s, rows, out, gate_s, up_s, eg, eu, ed, rows_sem, cache_sems, w_sems):
    count = eg.shape[0]
    tokens, _, head = kc.shape
    cap, dim = srt_hbm.shape
    step = tokens // count
    news = ((k_s, kc, kc_hbm, ko_hbm), (v_s, vc, vc_hbm, vo_hbm))

    def some(e):
        return pl.ds(e * step, step)

    def comes(e):
        copies = [pltpu.make_async_copy(src.at[e], dst.at[e], w_sems.at[i, e])
                  for i, (src, dst) in enumerate([(eg_hbm, eg), (eu_hbm, eu), (ed_hbm, ed)])]
        return copies + [pltpu.make_async_copy(src.at[some(e)], buf.at[some(e)], cache_sems.at[i, e])
                         for i, (_, buf, src, _) in enumerate(news)]

    def goes(e):
        return [pltpu.make_async_copy(buf.at[some(e)], dst.at[some(e)], cache_sems.at[2 + i, e])
                for i, (_, buf, _, dst) in enumerate(news)]

    rows_copy = pltpu.make_async_copy(srt_hbm, rows.at[pl.ds(0, cap)], rows_sem.at[0])
    rows_copy.start()
    for e in range(AHEAD):
        for copy in comes(e):
            copy.start()
    k_s[...] = knew_ref[...].astype(F32)
    v_s[...] = vnew_ref[...].astype(F32)
    out[...] = jnp.zeros_like(out)
    rows_copy.wait()

    def new_rows(e):
        for new, buf, _, _ in news:
            for j in range(step):
                b = e * step + j
                spot = pos_ref[b]
                base = pl.multiple_of(spot // ALIGN * ALIGN, ALIGN)
                hit = iota((ALIGN, head), 0) == spot - base
                tile = buf[b, pl.ds(base, ALIGN), :].astype(F32)
                buf[b, pl.ds(base, ALIGN), :] = jnp.where(hit, new[pl.ds(b, 1), :], tile).astype(BF16)

    def window(e, p):
        return pl.ds(pl.multiple_of(plan_ref[count + e, 0] + p * WIN, ALIGN), WIN)

    def widen(e, here):
        x = rows[here, :]
        return nt_dot(eg[e], x), nt_dot(eu[e], x)

    def narrow(e, here, gate, up):
        act = jnp.transpose(jax.nn.silu(gate) * up).astype(BF16)
        wt = wt_slot[here, :][:, 0:1]
        for i in range(dim // COLS):
            cols = span(i, COLS)
            out[here, cols] = (mm(act, ed[e, :, cols]) * wt).astype(BF16)

    def others(e):
        def one(p, carry):
            narrow(e, window(e, p), *widen(e, window(e, p)))
            return carry

        lax.fori_loop(1, (plan_ref[e, 0] + (WIN - 1)) // WIN, one, 0)

    def begin(e):
        gate, up = widen(e, window(e, 0))
        gate_s[...] = gate
        up_s[...] = up

    finish(comes(0))
    begin(0)
    new_rows(0)
    for copy in goes(0):
        copy.start()

    def run(e, carry):
        @pl.when(e + (AHEAD - 1) < count)
        def _():
            for copy in comes(e + (AHEAD - 1)):
                copy.start()

        finish(comes(e))
        narrow(e - 1, window(e - 1, 0), gate_s[...], up_s[...])
        begin(e)
        new_rows(e)
        for copy in goes(e):
            copy.start()
        others(e - 1)
        return carry

    lax.fori_loop(1, count, run, 0)
    last = count - 1
    narrow(last, window(last, 0), gate_s[...], up_s[...])
    others(last)
    out_copy = pltpu.make_async_copy(out.at[pl.ds(0, cap)], out_hbm, rows_sem.at[1])
    out_copy.start()
    out_copy.wait()
    for e in range(count):
        finish(goes(e))


def experts(plan, pos, wt_slot, k_new, v_new, kc, vc, srt, eg_t, eu_t, ed):
    shape = jax.ShapeDtypeStruct
    count = ed.shape[0]
    room = (srt.shape[0] + WIN, srt.shape[1])
    return pl.pallas_call(
        expert_kernel,
        name="experts",
        out_shape=(shape(srt.shape, BF16), shape(kc.shape, BF16), shape(vc.shape, BF16)),
        in_specs=[SMEM, SMEM, VMEM, VMEM, VMEM] + [ANY] * 6,
        out_specs=(ANY, ANY, ANY),
        scratch_shapes=[
            pltpu.VMEM(kc.shape, BF16), pltpu.VMEM(vc.shape, BF16), pltpu.VMEM(k_new.shape, F32),
            pltpu.VMEM(v_new.shape, F32), pltpu.VMEM(room, BF16), pltpu.VMEM(room, BF16),
            pltpu.VMEM((eg_t.shape[1], WIN), F32), pltpu.VMEM((eg_t.shape[1], WIN), F32),
            *[pltpu.VMEM(w.shape, BF16) for w in (eg_t, eu_t, ed)],
            pltpu.SemaphoreType.DMA((2,)), pltpu.SemaphoreType.DMA((4, count)), pltpu.SemaphoreType.DMA((3, count))],
        compiler_params=pltpu.CompilerParams(vmem_limit_bytes=VMEM_LIMIT),
    )(plan, pos, wt_slot, k_new, v_new, kc, vc, srt, eg_t, eu_t, ed)


def back_kernel(hsum_ref, gres_ref, place_ref, srt_hbm, wg_hbm, wu_hbm, wd_hbm, out_ref,
                srt, mall, pos_col, wg, wu, wd, a_s, own, take, ring, relay_x, got_x, swap, hid,
                part_b, relay_b, got_b, full_b, send_sems, recv_sems, load_sems):
    ep, tokens, dim = mall.shape
    cap = srt.shape[0]
    ep, me, core, partner, right, left, far = ring_ids()
    tp, mt = lax.axis_size("tp"), lax.axis_index("tp")
    to_right, to_left, to_partner = {"ep": right}, {"ep": left}, {"ep": partner}
    rows_in = pieces_of(srt_hbm, srt, load_sems, 3, 1)
    loads = [pieces_of(src, dst, load_sems, i, PARTS) for i, (src, dst) in enumerate(
        [(wg_hbm, wg), (wu_hbm, wu), (wd_hbm, wd)])]
    barrier = pltpu.get_barrier_semaphore()
    peers = [{"ep": i} for i in (partner, right, left)] + [{"tp": lax.rem(mt + i, tp)} for i in (1, tp - 1)]
    for peer in peers:
        pl.semaphore_signal(barrier, inc=1, device_id=peer, device_id_type=MESH)
    for s in range(ep):
        pos_col[s] = jnp.transpose(jnp.broadcast_to(place_ref[s:s + 1, :], (tokens, tokens)))
    pl.semaphore_wait(barrier, len(peers))
    links = Links(send_sems, recv_sems)
    mid = RowSum(links, MID, "tp", hid)
    hid[mid.rows(mt, None), :] = hsum_ref[...]
    mid.spread()
    chips = [far // 2, right // 2, left // 2, me // 2]
    halfd = dim // 2
    quart = halfd // 2
    mine = pl.ds(pl.multiple_of(core * halfd, halfd), halfd)
    other = pl.ds(pl.multiple_of((1 - core) * halfd, halfd), halfd)
    lo, hi, full = pl.ds(0, quart), pl.ds(quart, quart), slice(None)

    def chip_rows(chip):
        return pl.ds(chip * 2, 2)

    def add_pair(i):
        links.recv(GIVE + i)
        for j in range(2):
            ring[i, j] = (mall[chips[i] * 2 + j, :, mine].astype(F32) + take[i, j].astype(F32)).astype(BF16)

    lane = iota((2 * tokens, tokens), 1).astype(F32)

    def scatter(i):
        where = pos_col[chip_rows(chips[i])].reshape(2 * tokens, tokens)
        pick = jnp.concatenate([(where == lane + j * tokens).astype(F32).astype(BF16)
                                for j in range(cap // tokens)], axis=1)
        for n in range(dim // COLS):
            cols = span(n, COLS)
            mall[chip_rows(chips[i]), :, cols] = mm(pick, srt[:, cols]).astype(BF16).reshape(2, tokens, COLS)
        links.send(GIVE + i, lambda: mall.at[chip_rows(chips[i]), :, other], to_partner, at(take, i))

    finish(rows_in[0:1])
    scatter(0)
    scatter(1)
    add_pair(0)
    links.send(RING, at(ring, 0, full, full, lo), to_right, at(relay_x, 0))
    links.send(RING + 1, at(ring, 0, full, full, hi), to_left, at(relay_x, 1))
    scatter(2)
    add_pair(1)
    links.send(RING + 2, at(ring, 1, full, full, hi), to_right, at(got_x, 0, 1))
    scatter(3)
    add_pair(2)
    links.send(RING + 3, at(ring, 2, full, full, lo), to_left, at(got_x, 1, 0))
    add_pair(3)
    mid.forward()
    mid.finish()
    wide = hid[...].astype(F32)
    a_s[...] = (wide * rms(wide) * gain_row(gres_ref)).astype(BF16)
    for load in loads[:2]:
        finish(load)
    acts = []
    for i in range(wg.shape[1] // COLS):
        cols = span(i, COLS)
        acts.append((jax.nn.silu(mm(a_s[...], wg[:, cols])) * mm(a_s[...], wu[:, cols])).astype(BF16))
    act = jnp.concatenate(acts, axis=1)
    finish(loads[2])
    for i in range(dim // COLS):
        cols = span(i, COLS)
        own[:, cols] = mm(act, wd[:, cols])

    for n, (dest, cols, device, side) in enumerate([(1, span(0, quart), to_right, 0), (2, span(1, quart), to_left, 1)]):
        links.recv(RING + n)
        relay_x[2 + n] = (ring[dest, :, :, cols].astype(F32) + relay_x[n].astype(F32)).astype(BF16)
        links.send(RING + 4 + n, at(relay_x, 2 + n), device, at(got_x, side, n))
    links.recv(*range(RING + 2, SWAP))

    def arrived(j):
        return jnp.concatenate(
            [ring[3, j, :, span(q, quart)].astype(F32) + got_x[0, q, j].astype(F32) + got_x[1, q, j].astype(F32)
             for q in range(2)], axis=1)

    swap[0] = arrived(1 - core).astype(BF16)
    links.send(SWAP, at(swap, 0), to_partner, at(swap, 1))
    last = RowSum(links, LAST, "tp", full_b, part_b, relay_b, got_b)
    own[:, mine] += arrived(core)
    part_b[:, mine] = own[:, mine].astype(BF16)
    links.recv(SWAP)
    own[:, other] += swap[1].astype(F32)
    part_b[:, other] = own[:, other].astype(BF16)
    last.start()
    last.pass_on()
    last.collect(own, hid)
    last.spread()
    last.forward()
    last.finish()
    out_ref[...] = full_b[...]
    links.drain()


def back(h_sum, g_res, place, srt, w_gate, w_up, w_down, tp):
    tokens, dim = h_sum.shape[0] * tp, h_sum.shape[1]
    ep = place.shape[0]
    chips, halfd, quart = ep // 2, dim // 2, dim // 4
    return pl.pallas_call(
        back_kernel,
        name="back",
        out_shape=jax.ShapeDtypeStruct((tokens, dim), BF16),
        in_specs=[VMEM, VMEM, VMEM] + [ANY] * 4,
        out_specs=VMEM,
        scratch_shapes=[
            pltpu.VMEM(srt.shape, BF16), pltpu.VMEM((ep, tokens, dim), BF16), pltpu.VMEM((ep, tokens, tokens), F32),
            *[pltpu.VMEM(w.shape, BF16) for w in (w_gate, w_up, w_down)],
            pltpu.VMEM((tokens, dim), BF16), pltpu.VMEM((tokens, dim), F32),
            pltpu.VMEM((chips, 2, tokens, halfd), BF16), pltpu.VMEM((chips, 2, tokens, halfd), BF16),
            pltpu.VMEM((4, 2, tokens, quart), BF16), pltpu.VMEM((2, 2, 2, tokens, quart), BF16),
            pltpu.VMEM((2, tokens, halfd), BF16), pltpu.VMEM((tokens, dim), BF16), *row_sum_scratch(tokens, dim, tp),
            pltpu.SemaphoreType.DMA((BACK_COPIES,)), pltpu.SemaphoreType.DMA((BACK_COPIES,)),
            pltpu.SemaphoreType.DMA((4, PARTS))],
        compiler_params=pltpu.CompilerParams(collective_id=1, has_side_effects=True, vmem_limit_bytes=VMEM_LIMIT),
    )(h_sum, g_res, place, srt, w_gate, w_up, w_down)


def solution(mesh):
    ep, tp = mesh.shape['ep'], mesh.shape['tp']
    row_spec = P(('dp', 'ep'), None)
    cache_spec = P(('dp', 'ep'), None, 'tp', None)
    col_split = P(None, 'tp')
    row_split = P('tp', None)
    in_specs = (row_spec, P(('dp', 'ep')), row_spec, cache_spec, cache_spec, P(None), P(None), P(None), col_split, col_split, col_split, row_split, col_split, col_split, row_split, P(None, None), P('ep', None, 'tp'), P('ep', None, 'tp'), P('ep', 'tp', None))
    out_specs = (row_spec, cache_spec, cache_spec)

    def local_layer(hidden_in, positions, expert_ids, k_cache, v_cache, norm_in, norm_res, norm_post, w_q, w_k, w_v, w_o, w_gate, w_up, w_down, w_router, e_gate, e_up, e_down):
        tokens, dim = hidden_in.shape
        slots, head = k_cache.shape[1], k_cache.shape[3]
        kc, vc = (cache.reshape(tokens, slots, head) for cache in (k_cache, v_cache))
        h_sum, k_new, v_new, place, plan, wt_slot, srt = front(
            hidden_in, expert_ids.T, positions, norm_in, norm_post, w_router, kc, vc, w_q, w_k, w_v, w_o,
            e_down.shape[0], ep, tp)
        out, k_out, v_out = experts(
            plan, positions, wt_slot, k_new, v_new, kc, vc, srt, jnp.swapaxes(e_gate, 1, 2), jnp.swapaxes(e_up, 1, 2), e_down)
        hidden_out = back(h_sum, norm_res, place, out, w_gate, w_up, w_down, tp)
        return hidden_out, k_out.reshape(k_cache.shape), v_out.reshape(v_cache.shape)

    return jax.shard_map(local_layer, mesh=mesh, in_specs=in_specs, out_specs=out_specs, check_vma=False)
```

```python
import functools

import jax
import jax.numpy as jnp
import numpy as np
from jax import lax
from jax.experimental import pallas as pl
from jax.experimental.pallas import tpu as pltpu
from jax.sharding import PartitionSpec as P

NORM_EPS = 1e-5
ROPE_BASE = 10000.0
MESH = pl.DeviceIdType.MESH
F32 = jnp.float32
BF16 = jnp.bfloat16
WIN = 48
ALIGN = 16
AHEAD = 6
COLS = 512
PARTS = 4
VMEM_LIMIT = 67000000

ANY = pl.BlockSpec(memory_space=pl.ANY)
VMEM = pl.BlockSpec(memory_space=pltpu.VMEM)
SMEM = pl.BlockSpec(memory_space=pltpu.SMEM)


def nt_dot(a, b):
    return lax.dot_general(a, b, (((1,), (1,)), ((), ())), preferred_element_type=F32)


def mm(a, b):
    return jnp.dot(a, b, preferred_element_type=F32)


def span(i, width):
    return slice(i * width, (i + 1) * width)


def total(v, axis):
    return jnp.sum(v, axis=axis, keepdims=True)


def exp_rows(v):
    return jnp.exp(v - jnp.max(v, axis=-1, keepdims=True))


def rms(wide):
    return lax.rsqrt(jnp.mean(wide * wide, axis=-1, keepdims=True) + NORM_EPS)


def iota(shape, dim):
    return lax.broadcasted_iota(jnp.int32, shape, dim)


def gain_row(ref):
    return ref[...].astype(F32).reshape(1, ref.shape[0])


class Links:
    def __init__(self, send_sems, recv_sems):
        self.send_sems, self.recv_sems, self.started, self.unsent = send_sems, recv_sems, {}, []

    def copy(self, i):
        src, dst, device = self.started[i]
        return pltpu.make_async_remote_copy(
            src_ref=src(), dst_ref=dst(), send_sem=self.send_sems.at[i], recv_sem=self.recv_sems.at[i],
            device_id=device, device_id_type=MESH)

    def send(self, i, src, device, dst=None):
        self.started[i] = (src, dst or src, device)
        self.copy(i).start()
        self.unsent.append(i)

    def recv(self, *ids):
        for i in ids:
            self.copy(i).wait_recv()

    def drain(self):
        for i in self.unsent:
            self.copy(i).wait_send()
        self.unsent = []


def pieces_of(src, dst, sems, i, parts):
    size = src.shape[0] // parts
    copies = [pltpu.make_async_copy(src.at[pl.ds(n * size, size)], dst.at[pl.ds(n * size, size)], sems.at[i, n])
              for n in range(parts)]
    for copy in copies:
        copy.start()
    return copies


def finish(copies):
    for copy in copies:
        copy.wait()


def at(ref, *index):
    return lambda: ref.at[index]


class RowSum:
    def __init__(self, links, base, axis, full, part=None, relay=None, got=None):
        self.links, self.base, self.part, self.relay, self.got, self.full = links, base, part, relay, got, full
        self.size = lax.axis_size(axis)
        self.me = lax.axis_index(axis)
        self.right = lax.rem(self.me + 1, self.size)
        self.left = lax.rem(self.me + self.size - 1, self.size)
        self.far = lax.rem(self.me + 2, self.size)
        self.to_right, self.to_left = {axis: self.right}, {axis: self.left}
        self.block = full.shape[0] // self.size
        self.half = self.block // 2

    def rows(self, rank, half):
        if half is None:
            return pl.ds(pl.multiple_of(rank * self.block, self.block), self.block)
        return pl.ds(pl.multiple_of(rank * self.block + half * self.half, self.half), self.half)

    def send(self, i, device, src, dst=None):
        buf, *rows = src
        self.links.send(self.base + i, (lambda: buf.at[self.rows(*rows)]) if rows else (lambda: buf), device, dst)

    def recv(self, *ids):
        self.links.recv(*[self.base + i for i in ids])

    def start(self):
        part, relay, got = self.part, self.relay, self.got
        self.send(0, self.to_right, (part, self.far, 0), at(relay, 0))
        self.send(1, self.to_left, (part, self.far, 1), at(relay, 1))
        self.send(2, self.to_right, (part, self.right, 1), at(got, 0, 1))
        self.send(3, self.to_left, (part, self.left, 0), at(got, 1, 0))

    def pass_on(self):
        part, relay = self.part, self.relay
        for n, (dest, device) in enumerate([(self.right, self.to_right), (self.left, self.to_left)]):
            self.recv(n)
            relay[2 + n] = (part[self.rows(dest, n), :].astype(F32) + relay[n].astype(F32)).astype(BF16)
            self.send(4 + n, device, (relay.at[2 + n],), at(self.got, n, n))

    def collect(self, own, rest):
        self.recv(2, 3, 4, 5)
        for half in range(2):
            here = self.rows(self.me, half)
            acc = own(here) + self.got[0, half].astype(F32) + self.got[1, half].astype(F32)
            self.full[here, :] = (rest(here).astype(F32) + acc).astype(BF16)

    def spread(self):
        for n, device in enumerate([self.to_right, self.to_left]):
            self.send(6 + n, device, (self.full, self.me, n))
        for n, device in enumerate([self.to_right, self.to_left]):
            self.send(8 + n, device, (self.full, self.me, 1 - n))

    def forward(self):
        for n, (block, device) in enumerate([(self.left, self.to_right), (self.right, self.to_left)]):
            self.recv(6 + n)
            self.send(10 + n, device, (self.full, block, n))

    def finish(self):
        self.recv(8, 9, 10, 11)


def row_sum_scratch(rows, cols, tp):
    half = rows // tp // 2
    return [pltpu.VMEM((rows, cols), BF16), pltpu.VMEM((4, half, cols), BF16),
            pltpu.VMEM((2, 2, half, cols), BF16), pltpu.VMEM((rows, cols), BF16)]


def ring_ids():
    ep = lax.axis_size("ep")
    me = lax.axis_index("ep")
    core = lax.rem(me, 2)
    partner = me + 1 - 2 * core
    return ep, me, core, partner, lax.rem(me + 2, ep), lax.rem(me + ep - 2, ep), lax.rem(me + 4, ep)


ROWS, ATT, FAR, META, TWIN, FRONT_COPIES = 0, 5, 17, 20, 28, 34
GIVE, RING, SWAP, LAST, MID, BACK_COPIES = 0, 4, 16, 18, 42, 54
GROUPS = 2


def front_kernel(x_ref, ids_ref, pos_ref, gin_ref, gpost_ref, wr_ref, kc_hbm, vc_hbm, wq_hbm, wk_hbm, wv_hbm, wo_hbm,
                 hsum_ref, knew_ref, vnew_ref, place_ref, plan_ref, wt_slot, srt,
                 mall, meta, a_s, own, pos_row, part, relay, got, hid, send_sems, recv_sems, load_sems):
    tokens, dim = x_ref.shape
    head = wk_hbm.shape[1]
    heads = wq_hbm.shape[1] // head
    slots = kc_hbm.shape[1]
    count = plan_ref.shape[0] // 2
    ep, me, core, partner, right, left, far = ring_ids()
    tp, mt = lax.axis_size("tp"), lax.axis_index("tp")
    to_right, to_left, to_partner = {"ep": right}, {"ep": left}, {"ep": partner}
    peers = [lax.rem(me + i, ep) for i in range(1, ep)]
    barrier = pltpu.get_barrier_semaphore()
    for peer in peers:
        pl.semaphore_signal(barrier, inc=1, device_id={"ep": peer}, device_id_type=MESH)
    for peer in (lax.rem(mt + 1, tp), lax.rem(mt + tp - 1, tp)):
        pl.semaphore_signal(barrier, inc=1, device_id={"tp": peer}, device_id_type=MESH)
    links = Links(send_sems, recv_sems)
    att_sum = RowSum(links, ATT, "tp", hid, part, relay, got)
    hrow = tokens // 2

    def half(i, h):
        return at(mall, i, pl.ds(h * hrow, hrow))

    def twin(i):
        return i + 1 - 2 * lax.rem(i, 2)

    def attention(kc, vc, wq, wk, wv, wo, q_s, o_s, k_s, v_s, pcol):
        loads = [pieces_of(src, dst, load_sems, i, PARTS) for i, (src, dst) in enumerate(
            [(wq_hbm, wq), (wk_hbm, wk), (wv_hbm, wv), (kc_hbm, kc), (vc_hbm, vc), (wo_hbm, wo)])]
        wide = x_ref[...].astype(F32)
        inv = rms(wide)
        mall[me] = (wide * inv * gain_row(gpost_ref)).astype(BF16)
        a_s[...] = (wide * inv * gain_row(gin_ref)).astype(BF16)
        pl.semaphore_wait(barrier, len(peers) + 2)
        first = [(0, right), (1, left), (1, right), (0, left)]
        for n, (h, device) in enumerate(first):
            links.send(ROWS + n, half(me, h), {"ep": device})
        links.send(ROWS + len(first), at(mall, me), to_partner)

        logits = mm(mall[me], wr_ref[...])
        probs = exp_rows(logits)
        probs = probs / total(probs, 1)
        experts = logits.shape[1]
        ids = ids_ref[...].astype(F32)
        lane = iota((tokens, experts), 1).astype(F32)
        id_rows = [ids[k:k + 1, :] for k in range(2)]
        picked = [total(jnp.where(jnp.transpose(jnp.broadcast_to(row, (experts, tokens))) == lane, probs, 0.0), 1)
                  for row in id_rows]
        both = picked[0] + picked[1]
        sub = iota((8, tokens), 0)
        block = jnp.zeros((8, tokens), F32)
        wts = [jnp.transpose(jnp.broadcast_to(p / both, (tokens, tokens)))[0:8, :] for p in picked]
        for n, row in enumerate(id_rows + wts):
            block = jnp.where(sub == n, row, block)
        meta[me] = block
        for n, peer in enumerate(peers):
            links.send(META + n, at(meta, me), {"ep": peer})

        def pos_body(g, carry):
            row = iota((8, head), 0)
            acc = jnp.zeros((8, head), jnp.int32)
            for j in range(8):
                acc = jnp.where(row == j, pos_ref[g * 8 + j], acc)
            pcol[pl.ds(pl.multiple_of(g * 8, 8), 8), :] = acc
            return carry

        lax.fori_loop(0, tokens // 8, pos_body, 0)
        spot = iota((tokens, head), 1)
        power = lax.rem(spot, head // 2).astype(F32) * (-np.log(ROPE_BASE) / (head // 2))
        angles = pcol[...].astype(F32) * jnp.exp(power)
        cosine = jnp.cos(angles)
        sine = jnp.sin(angles)
        sine = jnp.where(spot < head // 2, -sine, sine)

        def rope(v):
            return (v * cosine + pltpu.roll(v, head // 2, 1) * sine).astype(BF16).astype(F32)

        for load in loads[:3]:
            finish(load)
        normed = a_s[...]
        k_s[...] = rope(mm(normed, wk[...]))
        v_s[...] = mm(normed, wv[...]).astype(BF16).astype(F32)
        knew_ref[...] = k_s[...].astype(BF16)
        vnew_ref[...] = v_s[...].astype(BF16)
        for i in range(heads // 2):
            q2 = mm(normed, wq[:, span(i, 2 * head)])
            for j in range(2):
                q_s[2 * i + j] = rope(q2[:, span(j, head)])
        for load in loads[3:5]:
            finish(load)

        def attend(g, carry):
            base = pl.multiple_of(g * 8, 8)
            slot = iota((slots, head), 0)
            pairs = []
            for new, old in ((k_s, kc), (v_s, vc)):
                pieces = [jnp.where(slot == pos_ref[g * 8 + j], new[pl.ds(base + j, 1), :], old[base + j].astype(F32))
                          for j in range(8)]
                pairs.append(jnp.concatenate([piece.astype(BF16) for piece in pieces], axis=0))
            keys, vals = pairs
            q8 = q_s[:, pl.ds(base, 8), :].reshape(heads * 8, head).astype(BF16)
            scores = nt_dot(q8, keys) * (head ** -0.5)
            each = (8, 8 * slots)
            col = iota(each, 1)
            row_pos = jnp.concatenate([pcol[pl.ds(base, 8), :]] * (8 * slots // head), axis=1)
            mask = (col // slots == iota(each, 0)) & (lax.rem(col, slots) <= row_pos)
            mask = jnp.broadcast_to(mask[None], (heads, *each)).reshape(heads * 8, 8 * slots)
            e = exp_rows(jnp.where(mask, scores, -1e30))
            o8 = mm((e / total(e, 1)).astype(BF16), vals)
            o_s[:, pl.ds(base, 8), :] = o8.reshape(heads, 8, head)
            return carry

        lax.fori_loop(0, tokens // 8, attend, 0)
        mix = jnp.concatenate([o_s[i].astype(BF16) for i in range(heads)], axis=1)
        finish(loads[5])
        for i in range(dim // COLS):
            cols = span(i, COLS)
            piece = mm(mix, wo[:, cols])
            own[:, cols] = piece
            part[:, cols] = piece.astype(BF16)
        att_sum.start()

    kv = pltpu.VMEM((tokens, head), F32)
    each_head = pltpu.VMEM((heads, tokens, head), F32)
    pl.run_scoped(
        attention, *[pltpu.VMEM(ref.shape, BF16) for ref in (kc_hbm, vc_hbm, wq_hbm, wk_hbm, wv_hbm, wo_hbm)],
        each_head, each_head, kv, kv, pltpu.VMEM((tokens, head), jnp.int32))

    cap = srt.shape[0]
    rows = cap // 2

    for n, (block, h, device) in enumerate([(left, 0, right), (right, 1, left)]):
        links.recv(ROWS + n)
        links.send(FAR + n, half(block, h), {"ep": device})
        links.send(TWIN + n, half(block, h), to_partner)

    links.recv(*range(META, META + len(peers)))
    begin = (me * count).astype(F32)
    before = (iota((tokens, tokens), 0) < iota((tokens, tokens), 1)).astype(F32).astype(BF16)
    expert = iota((count, tokens), 0).astype(F32)
    hots, ranks, local, wts = [], [], [], []
    seen = jnp.zeros((count, 1), F32)
    for s in range(ep):
        block = meta[s]
        one, two = block[0:1, :] - begin, block[1:2, :] - begin
        in_one = (one >= 0) & (one < count)
        in_two = (two >= 0) & (two < count)
        took = jnp.where(in_one, one, jnp.where(in_two, two, -1.0))
        wts.append(jnp.where(in_one, block[2:3, :], jnp.where(in_two, block[3:4, :], 0.0)))
        hot = (expert == took).astype(F32)
        hots.append(hot)
        local.append(took)
        ranks.append(mm(hot.astype(BF16), before) + seen)
        seen = seen + total(hot, 1)
    padded = jnp.broadcast_to(jnp.floor((seen + (ALIGN - 1)) * (1.0 / ALIGN)) * ALIGN, (count, tokens))
    earlier = (iota((count, count), 1) < iota((count, count), 0)).astype(F32).astype(BF16)
    start = mm(earlier, padded.astype(BF16))
    plan_ref[0:count, :] = jnp.broadcast_to(seen, (count, tokens)).astype(jnp.int32)
    plan_ref[count:, :] = start.astype(jnp.int32)
    for s in range(ep):
        place = total(hots[s] * (start + ranks[s]), 0)
        place = jnp.where(local[s] >= 0, place, -1.0)
        pos_row[s] = jnp.broadcast_to(place, (8, tokens))
        place_ref[s:s + 1, :] = place

    wt_slot[cap:, :] = jnp.zeros((WIN, tokens), F32)
    for c in range(cap // rows):
        slot = (iota((rows, tokens), 0) + c * rows).astype(F32)
        wt = jnp.zeros((rows, tokens), F32)
        for s in range(ep):
            wt = wt + jnp.where(slot == pos_row[s, 0:1, :], wts[s], 0.0)
        wt_slot[span(c, rows), :] = jnp.broadcast_to(total(wt, 1), (rows, tokens))

    def gather(one, fresh):
        two = twin(one)

        def body(c, carry):
            here = pl.ds(pl.multiple_of(c * rows, rows), rows)
            slot = (iota((rows, tokens), 0) + c * rows).astype(F32)
            pick = jnp.concatenate([(slot == pos_row[s, 0:1, :]).astype(F32).astype(BF16) for s in (one, two)], axis=1)
            for i in range(dim // COLS):
                cols = span(i, COLS)
                got_rows = mm(pick, jnp.concatenate([mall[one, :, cols], mall[two, :, cols]], axis=0))
                if not fresh:
                    got_rows = got_rows + srt[here, cols].astype(F32)
                srt[here, cols] = got_rows.astype(BF16)
            return carry

        lax.fori_loop(0, cap // rows, body, 0)

    links.recv(ROWS + 4)
    gather(me, True)
    att_sum.pass_on()
    for n, (block, h) in enumerate([(left, 1), (right, 0)]):
        links.recv(ROWS + 2 + n)
        links.send(TWIN + 2 + n, half(block, h), to_partner)
    att_sum.collect(lambda here: own[here, :], lambda here: x_ref[here, :])
    hsum_ref[...] = hid[att_sum.rows(mt, None), :]
    for n, block in enumerate([left, right]):
        links.recv(TWIN + n, TWIN + 2 + n)
        gather(block, False)
    for n in range(2):
        links.recv(FAR + n)
        links.send(TWIN + 4 + n, half(far, n), to_partner)
    links.recv(TWIN + 4, TWIN + 5)
    gather(far, False)
    links.drain()


def sorted_rows(ep, tokens, count):
    most = ep * tokens // 2 + count * (ALIGN - 1)
    return -(-most // (2 * tokens)) * 2 * tokens


def front(x, ids_t, pos, g_in, g_post, w_router, kc, vc, w_q, w_k, w_v, w_o, count, ep, tp):
    tokens, dim = x.shape
    head = w_k.shape[1]
    cap = sorted_rows(ep, tokens, count)
    shape = jax.ShapeDtypeStruct
    return pl.pallas_call(
        front_kernel,
        name="front",
        out_shape=(shape((tokens // tp, dim), BF16), shape((tokens, head), BF16), shape((tokens, head), BF16),
                   shape((ep, tokens), F32), shape((2 * count, tokens), jnp.int32), shape((cap + WIN, tokens), F32),
                   shape((cap, dim), BF16)),
        in_specs=[VMEM, VMEM, SMEM] + [VMEM] * 3 + [ANY] * 6,
        out_specs=(VMEM,) * 7,
        scratch_shapes=[
            pltpu.VMEM((ep, tokens, dim), BF16), pltpu.VMEM((ep, 8, tokens), F32), pltpu.VMEM((tokens, dim), BF16),
            pltpu.VMEM((tokens, dim), F32), pltpu.VMEM((ep, 8, tokens), F32), *row_sum_scratch(tokens, dim, tp),
            pltpu.SemaphoreType.DMA((FRONT_COPIES,)), pltpu.SemaphoreType.DMA((FRONT_COPIES,)),
            pltpu.SemaphoreType.DMA((6, PARTS))],
        compiler_params=pltpu.CompilerParams(collective_id=0, has_side_effects=True, vmem_limit_bytes=VMEM_LIMIT),
    )(x, ids_t, pos, g_in, g_post, w_router, kc, vc, w_q, w_k, w_v, w_o)


def expert_kernel(plan_ref, pos_ref, wt_slot, knew_ref, vnew_ref, kc_hbm, vc_hbm, srt_hbm, eg_hbm, eu_hbm, ed_hbm,
                  out_hbm, ko_hbm, vo_hbm, kc, vc, k_s, v_s, rows, out, gate_s, up_s, eg, eu, ed, rows_sem, cache_sems, w_sems):
    count = eg.shape[0]
    tokens, _, head = kc.shape
    cap, dim = srt_hbm.shape
    step = tokens // count
    news = ((k_s, kc, kc_hbm, ko_hbm), (v_s, vc, vc_hbm, vo_hbm))

    def some(e):
        return pl.ds(e * step, step)

    def comes(e):
        copies = [pltpu.make_async_copy(src.at[e], dst.at[e], w_sems.at[i, e])
                  for i, (src, dst) in enumerate([(eg_hbm, eg), (eu_hbm, eu), (ed_hbm, ed)])]
        return copies + [pltpu.make_async_copy(src.at[some(e)], buf.at[some(e)], cache_sems.at[i, e])
                         for i, (_, buf, src, _) in enumerate(news)]

    def goes(e):
        return [pltpu.make_async_copy(buf.at[some(e)], dst.at[some(e)], cache_sems.at[2 + i, e])
                for i, (_, buf, _, dst) in enumerate(news)]

    rows_copy = pltpu.make_async_copy(srt_hbm, rows.at[pl.ds(0, cap)], rows_sem.at[0])
    rows_copy.start()
    for e in range(AHEAD):
        for copy in comes(e):
            copy.start()
    k_s[...] = knew_ref[...].astype(F32)
    v_s[...] = vnew_ref[...].astype(F32)
    out[...] = jnp.zeros_like(out)
    rows_copy.wait()

    def new_rows(e):
        for new, buf, _, _ in news:
            for j in range(step):
                b = e * step + j
                spot = pos_ref[b]
                base = pl.multiple_of(spot // ALIGN * ALIGN, ALIGN)
                hit = iota((ALIGN, head), 0) == spot - base
                tile = buf[b, pl.ds(base, ALIGN), :].astype(F32)
                buf[b, pl.ds(base, ALIGN), :] = jnp.where(hit, new[pl.ds(b, 1), :], tile).astype(BF16)

    def window(e, p):
        return pl.ds(pl.multiple_of(plan_ref[count + e, 0] + p * WIN, ALIGN), WIN)

    def widen(e, here):
        x = rows[here, :]
        return nt_dot(eg[e], x), nt_dot(eu[e], x)

    def narrow(e, here, gate, up):
        act = jnp.transpose(jax.nn.silu(gate) * up).astype(BF16)
        wt = wt_slot[here, :][:, 0:1]
        for i in range(dim // COLS):
            cols = span(i, COLS)
            out[here, cols] = (mm(act, ed[e, :, cols]) * wt).astype(BF16)

    def others(e):
        def one(p, carry):
            narrow(e, window(e, p), *widen(e, window(e, p)))
            return carry

        lax.fori_loop(1, (plan_ref[e, 0] + (WIN - 1)) // WIN, one, 0)

    def begin(e):
        gate, up = widen(e, window(e, 0))
        gate_s[...] = gate
        up_s[...] = up

    finish(comes(0))
    begin(0)
    new_rows(0)
    for copy in goes(0):
        copy.start()

    def run(e, carry):
        @pl.when(e + (AHEAD - 1) < count)
        def _():
            for copy in comes(e + (AHEAD - 1)):
                copy.start()

        finish(comes(e))
        narrow(e - 1, window(e - 1, 0), gate_s[...], up_s[...])
        begin(e)
        new_rows(e)
        for copy in goes(e):
            copy.start()
        others(e - 1)
        return carry

    lax.fori_loop(1, count, run, 0)
    last = count - 1
    narrow(last, window(last, 0), gate_s[...], up_s[...])
    others(last)
    out_copy = pltpu.make_async_copy(out.at[pl.ds(0, cap)], out_hbm, rows_sem.at[1])
    out_copy.start()
    out_copy.wait()
    for e in range(count):
        finish(goes(e))


def experts(plan, pos, wt_slot, k_new, v_new, kc, vc, srt, eg_t, eu_t, ed):
    shape = jax.ShapeDtypeStruct
    count = ed.shape[0]
    room = (srt.shape[0] + WIN, srt.shape[1])
    return pl.pallas_call(
        expert_kernel,
        name="experts",
        out_shape=(shape(srt.shape, BF16), shape(kc.shape, BF16), shape(vc.shape, BF16)),
        in_specs=[SMEM, SMEM, VMEM, VMEM, VMEM] + [ANY] * 6,
        out_specs=(ANY, ANY, ANY),
        scratch_shapes=[
            pltpu.VMEM(kc.shape, BF16), pltpu.VMEM(vc.shape, BF16), pltpu.VMEM(k_new.shape, F32),
            pltpu.VMEM(v_new.shape, F32), pltpu.VMEM(room, BF16), pltpu.VMEM(room, BF16),
            pltpu.VMEM((eg_t.shape[1], WIN), F32), pltpu.VMEM((eg_t.shape[1], WIN), F32),
            *[pltpu.VMEM(w.shape, BF16) for w in (eg_t, eu_t, ed)],
            pltpu.SemaphoreType.DMA((2,)), pltpu.SemaphoreType.DMA((4, count)), pltpu.SemaphoreType.DMA((3, count))],
        compiler_params=pltpu.CompilerParams(vmem_limit_bytes=VMEM_LIMIT),
    )(plan, pos, wt_slot, k_new, v_new, kc, vc, srt, eg_t, eu_t, ed)


def back_kernel(hsum_ref, gres_ref, place_ref, srt_hbm, wg_hbm, wu_hbm, wd_hbm, out_ref,
                srt, mall, pos_col, wg, wu, wd, a_s, own, take, ring, relay_x, got_x, swap, hid,
                part_a, relay_a, got_a, full_a, part_b, relay_b, got_b, full_b, send_sems, recv_sems, load_sems):
    ep, tokens, dim = mall.shape
    cap = srt.shape[0]
    ep, me, core, partner, right, left, far = ring_ids()
    tp, mt = lax.axis_size("tp"), lax.axis_index("tp")
    to_right, to_left, to_partner = {"ep": right}, {"ep": left}, {"ep": partner}
    rows_in = pieces_of(srt_hbm, srt, load_sems, 3, 1)
    loads = [pieces_of(src, dst, load_sems, i, PARTS) for i, (src, dst) in enumerate(
        [(wg_hbm, wg), (wu_hbm, wu), (wd_hbm, wd)])]
    barrier = pltpu.get_barrier_semaphore()
    peers = [{"ep": i} for i in (partner, right, left)] + [{"tp": lax.rem(mt + i, tp)} for i in (1, tp - 1)]
    for peer in peers:
        pl.semaphore_signal(barrier, inc=1, device_id=peer, device_id_type=MESH)
    for s in range(ep):
        pos_col[s] = jnp.transpose(jnp.broadcast_to(place_ref[s:s + 1, :], (tokens, tokens)))
    pl.semaphore_wait(barrier, len(peers))
    links = Links(send_sems, recv_sems)
    mid = RowSum(links, MID, "tp", hid)
    hid[mid.rows(mt, None), :] = hsum_ref[...]
    mid.spread()
    chips = [far // 2, right // 2, left // 2, me // 2]
    halfd = dim // 2
    width = halfd // GROUPS
    piece = width // 2
    mine = pl.ds(pl.multiple_of(core * halfd, halfd), halfd)
    other = pl.ds(pl.multiple_of((1 - core) * halfd, halfd), halfd)
    full = slice(None)

    def part_of(g, q):
        return pl.ds(g * width + q * piece, piece)

    def chip_rows(chip):
        return pl.ds(chip * 2, 2)

    def add_pair(i):
        links.recv(GIVE + i)
        for j in range(2):
            ring[i, j] = (mall[chips[i] * 2 + j, :, mine].astype(F32) + take[i, j].astype(F32)).astype(BF16)

    lane = iota((2 * tokens, tokens), 1).astype(F32)

    def scatter(i):
        where = pos_col[chip_rows(chips[i])].reshape(2 * tokens, tokens)
        pick = jnp.concatenate([(where == lane + j * tokens).astype(F32).astype(BF16)
                                for j in range(cap // tokens)], axis=1)
        for n in range(dim // COLS):
            cols = span(n, COLS)
            mall[chip_rows(chips[i]), :, cols] = mm(pick, srt[:, cols]).astype(BF16).reshape(2, tokens, COLS)
        links.send(GIVE + i, lambda: mall.at[chip_rows(chips[i]), :, other], to_partner, at(take, i))

    finish(rows_in[0:1])
    scatter(0)
    scatter(1)
    add_pair(0)
    for g in range(GROUPS):
        for q, device in enumerate([to_right, to_left]):
            links.send(RING + 6 * g + q, at(ring, 0, full, full, part_of(g, q)), device, at(relay_x, g, q))

    def direct(g, side):
        q = 1 - side
        links.send(RING + 6 * g + 2 + side, at(ring, 1 + side, full, full, part_of(g, q)), (to_right, to_left)[side],
                   at(got_x, g, side, q))

    scatter(2)
    add_pair(1)
    direct(0, 0)
    scatter(3)
    add_pair(2)
    direct(0, 1)
    add_pair(3)
    mid.forward()
    mid.finish()
    wide = hid[...].astype(F32)
    a_s[...] = (wide * rms(wide) * gain_row(gres_ref)).astype(BF16)
    for load in loads[:2]:
        finish(load)
    acts = []
    for i in range(wg.shape[1] // COLS):
        cols = span(i, COLS)
        acts.append((jax.nn.silu(mm(a_s[...], wg[:, cols])) * mm(a_s[...], wu[:, cols])).astype(BF16))
    act = jnp.concatenate(acts, axis=1)
    finish(loads[2])
    for i in range(dim // COLS):
        cols = span(i, COLS)
        own[:, cols] = mm(act, wd[:, cols])

    for g in range(GROUPS):
        for q, device in enumerate([to_right, to_left]):
            links.recv(RING + 6 * g + q)
            relay_x[g, 2 + q] = (ring[1 + q, :, :, part_of(g, q)].astype(F32) + relay_x[g, q].astype(F32)).astype(BF16)
            links.send(RING + 6 * g + 4 + q, at(relay_x, g, 2 + q), device, at(got_x, g, q, q))
        if g + 1 < GROUPS:
            for side in range(2):
                direct(g + 1, side)

    def arrived(g, j):
        return jnp.concatenate(
            [ring[3, j, :, part_of(g, q)].astype(F32) + got_x[g, 0, q, j].astype(F32) + got_x[g, 1, q, j].astype(F32)
             for q in range(2)], axis=1)

    def columns(half, g):
        return pl.ds(pl.multiple_of(half * halfd + g * width, width), width)

    def view(ref, g):
        return lambda here: jnp.concatenate([ref[here, columns(half, g)] for half in range(2)], axis=1)

    buffers = [(full_a, part_a, relay_a, got_a), (full_b, part_b, relay_b, got_b)]
    last = [RowSum(links, LAST + 12 * g, "tp", *buffers[g]) for g in range(GROUPS)]

    def add_half(g, half, value):
        own[:, columns(half, g)] += value
        buffers[g][1][:, pl.ds(pl.multiple_of(half * width, width), width)] = own[:, columns(half, g)].astype(BF16)

    def come(g):
        links.recv(*range(RING + 6 * g + 2, RING + 6 * g + 6))
        swap[g, 0] = arrived(g, 1 - core).astype(BF16)
        links.send(SWAP + g, at(swap, g, 0), to_partner, at(swap, g, 1))
        add_half(g, core, arrived(g, core))

    def go(g):
        links.recv(SWAP + g)
        add_half(g, 1 - core, swap[g, 1].astype(F32))
        last[g].start()

    def collect(g):
        last[g].collect(view(own, g), view(hid, g))
        last[g].spread()

    come(0)
    go(0)
    last[0].pass_on()
    come(1)
    collect(0)
    go(1)
    last[0].forward()
    last[1].pass_on()
    last[0].finish()
    collect(1)
    last[1].forward()
    last[1].finish()
    for g in range(GROUPS):
        for half in range(2):
            out_ref[:, columns(half, g)] = buffers[g][0][:, span(half, width)]
    links.drain()


def back(h_sum, g_res, place, srt, w_gate, w_up, w_down, tp):
    tokens, dim = h_sum.shape[0] * tp, h_sum.shape[1]
    ep = place.shape[0]
    chips, halfd = ep // 2, dim // 2
    width = halfd // GROUPS
    return pl.pallas_call(
        back_kernel,
        name="back",
        out_shape=jax.ShapeDtypeStruct((tokens, dim), BF16),
        in_specs=[VMEM, VMEM, VMEM] + [ANY] * 4,
        out_specs=VMEM,
        scratch_shapes=[
            pltpu.VMEM(srt.shape, BF16), pltpu.VMEM((ep, tokens, dim), BF16), pltpu.VMEM((ep, tokens, tokens), F32),
            *[pltpu.VMEM(w.shape, BF16) for w in (w_gate, w_up, w_down)],
            pltpu.VMEM((tokens, dim), BF16), pltpu.VMEM((tokens, dim), F32),
            pltpu.VMEM((chips, 2, tokens, halfd), BF16), pltpu.VMEM((chips, 2, tokens, halfd), BF16),
            pltpu.VMEM((GROUPS, 4, 2, tokens, width // 2), BF16), pltpu.VMEM((GROUPS, 2, 2, 2, tokens, width // 2), BF16),
            pltpu.VMEM((GROUPS, 2, tokens, width), BF16), pltpu.VMEM((tokens, dim), BF16),
            *row_sum_scratch(tokens, 2 * width, tp), *row_sum_scratch(tokens, 2 * width, tp),
            pltpu.SemaphoreType.DMA((BACK_COPIES,)), pltpu.SemaphoreType.DMA((BACK_COPIES,)),
            pltpu.SemaphoreType.DMA((4, PARTS))],
        compiler_params=pltpu.CompilerParams(collective_id=1, has_side_effects=True, vmem_limit_bytes=VMEM_LIMIT),
    )(h_sum, g_res, place, srt, w_gate, w_up, w_down)


def solution(mesh):
    ep, tp = mesh.shape['ep'], mesh.shape['tp']
    row_spec = P(('dp', 'ep'), None)
    cache_spec = P(('dp', 'ep'), None, 'tp', None)
    col_split = P(None, 'tp')
    row_split = P('tp', None)
    in_specs = (row_spec, P(('dp', 'ep')), row_spec, cache_spec, cache_spec, P(None), P(None), P(None), col_split, col_split, col_split, row_split, col_split, col_split, row_split, P(None, None), P('ep', None, 'tp'), P('ep', None, 'tp'), P('ep', 'tp', None))
    out_specs = (row_spec, cache_spec, cache_spec)

    def local_layer(hidden_in, positions, expert_ids, k_cache, v_cache, norm_in, norm_res, norm_post, w_q, w_k, w_v, w_o, w_gate, w_up, w_down, w_router, e_gate, e_up, e_down):
        tokens, dim = hidden_in.shape
        slots, head = k_cache.shape[1], k_cache.shape[3]
        kc, vc = (cache.reshape(tokens, slots, head) for cache in (k_cache, v_cache))
        h_sum, k_new, v_new, place, plan, wt_slot, srt = front(
            hidden_in, expert_ids.T, positions, norm_in, norm_post, w_router, kc, vc, w_q, w_k, w_v, w_o,
            e_down.shape[0], ep, tp)
        out, k_out, v_out = experts(
            plan, positions, wt_slot, k_new, v_new, kc, vc, srt, jnp.swapaxes(e_gate, 1, 2), jnp.swapaxes(e_up, 1, 2), e_down)
        hidden_out = back(h_sum, norm_res, place, out, w_gate, w_up, w_down, tp)
        return hidden_out, k_out.reshape(k_cache.shape), v_out.reshape(v_cache.shape)

    return jax.shard_map(local_layer, mesh=mesh, in_specs=in_specs, out_specs=out_specs, check_vma=False)
```

```python
import functools

import jax
import jax.numpy as jnp
import numpy as np
from jax import lax
from jax.experimental import pallas as pl
from jax.experimental.pallas import tpu as pltpu
from jax.sharding import PartitionSpec as P

NORM_EPS = 1e-5
ROPE_BASE = 10000.0
MESH = pl.DeviceIdType.MESH
F32 = jnp.float32
BF16 = jnp.bfloat16
WIN = 64
ALIGN = 16
AHEAD = 6
COLS = 512
PARTS = 4
VMEM_LIMIT = 67000000

ANY = pl.BlockSpec(memory_space=pl.ANY)
VMEM = pl.BlockSpec(memory_space=pltpu.VMEM)
SMEM = pl.BlockSpec(memory_space=pltpu.SMEM)


def nt_dot(a, b):
    return lax.dot_general(a, b, (((1,), (1,)), ((), ())), preferred_element_type=F32)


def mm(a, b):
    return jnp.dot(a, b, preferred_element_type=F32)


def span(i, width):
    return slice(i * width, (i + 1) * width)


def total(v, axis):
    return jnp.sum(v, axis=axis, keepdims=True)


def exp_rows(v):
    return jnp.exp(v - jnp.max(v, axis=-1, keepdims=True))


def rms(wide):
    return lax.rsqrt(jnp.mean(wide * wide, axis=-1, keepdims=True) + NORM_EPS)


def iota(shape, dim):
    return lax.broadcasted_iota(jnp.int32, shape, dim)


def gain_row(ref):
    return ref[...].astype(F32).reshape(1, ref.shape[0])


class Links:
    def __init__(self, send_sems, recv_sems):
        self.send_sems, self.recv_sems, self.started, self.unsent = send_sems, recv_sems, {}, []

    def copy(self, i):
        src, dst, device = self.started[i]
        return pltpu.make_async_remote_copy(
            src_ref=src(), dst_ref=dst(), send_sem=self.send_sems.at[i], recv_sem=self.recv_sems.at[i],
            device_id=device, device_id_type=MESH)

    def send(self, i, src, device, dst=None):
        self.started[i] = (src, dst or src, device)
        self.copy(i).start()
        self.unsent.append(i)

    def recv(self, *ids):
        for i in ids:
            self.copy(i).wait_recv()

    def drain(self):
        for i in self.unsent:
            self.copy(i).wait_send()
        self.unsent = []


def pieces_of(src, dst, sems, i, parts):
    size = src.shape[0] // parts
    copies = [pltpu.make_async_copy(src.at[pl.ds(n * size, size)], dst.at[pl.ds(n * size, size)], sems.at[i, n])
              for n in range(parts)]
    for copy in copies:
        copy.start()
    return copies


def finish(copies):
    for copy in copies:
        copy.wait()


def at(ref, *index):
    return lambda: ref.at[index]


class RowSum:
    def __init__(self, links, base, axis, full, part=None, relay=None, got=None):
        self.links, self.base, self.part, self.relay, self.got, self.full = links, base, part, relay, got, full
        self.size = lax.axis_size(axis)
        self.me = lax.axis_index(axis)
        self.right = lax.rem(self.me + 1, self.size)
        self.left = lax.rem(self.me + self.size - 1, self.size)
        self.far = lax.rem(self.me + 2, self.size)
        self.to_right, self.to_left = {axis: self.right}, {axis: self.left}
        self.block = full.shape[0] // self.size
        self.half = self.block // 2

    def rows(self, rank, half):
        if half is None:
            return pl.ds(pl.multiple_of(rank * self.block, self.block), self.block)
        return pl.ds(pl.multiple_of(rank * self.block + half * self.half, self.half), self.half)

    def send(self, i, device, src, dst=None):
        buf, *rows = src
        self.links.send(self.base + i, (lambda: buf.at[self.rows(*rows)]) if rows else (lambda: buf), device, dst)

    def recv(self, *ids):
        self.links.recv(*[self.base + i for i in ids])

    def start(self):
        part, relay, got = self.part, self.relay, self.got
        self.send(0, self.to_right, (part, self.far, 0), at(relay, 0))
        self.send(1, self.to_left, (part, self.far, 1), at(relay, 1))
        self.send(2, self.to_right, (part, self.right, 1), at(got, 0, 1))
        self.send(3, self.to_left, (part, self.left, 0), at(got, 1, 0))

    def pass_on(self):
        part, relay = self.part, self.relay
        for n, (dest, device) in enumerate([(self.right, self.to_right), (self.left, self.to_left)]):
            self.recv(n)
            relay[2 + n] = (part[self.rows(dest, n), :].astype(F32) + relay[n].astype(F32)).astype(BF16)
            self.send(4 + n, device, (relay.at[2 + n],), at(self.got, n, n))

    def collect(self, own, rest):
        self.recv(2, 3, 4, 5)
        for half in range(2):
            here = self.rows(self.me, half)
            acc = own[here, :] + self.got[0, half].astype(F32) + self.got[1, half].astype(F32)
            self.full[here, :] = (rest[here, :].astype(F32) + acc).astype(BF16)

    def spread(self):
        for n, device in enumerate([self.to_right, self.to_left]):
            self.send(6 + n, device, (self.full, self.me, n))
        for n, device in enumerate([self.to_right, self.to_left]):
            self.send(8 + n, device, (self.full, self.me, 1 - n))

    def forward(self):
        for n, (block, device) in enumerate([(self.left, self.to_right), (self.right, self.to_left)]):
            self.recv(6 + n)
            self.send(10 + n, device, (self.full, block, n))

    def finish(self):
        self.recv(8, 9, 10, 11)


def row_sum_scratch(rows, cols, tp):
    half = rows // tp // 2
    return [pltpu.VMEM((rows, cols), BF16), pltpu.VMEM((4, half, cols), BF16),
            pltpu.VMEM((2, 2, half, cols), BF16), pltpu.VMEM((rows, cols), BF16)]


def ring_ids():
    ep = lax.axis_size("ep")
    me = lax.axis_index("ep")
    core = lax.rem(me, 2)
    partner = me + 1 - 2 * core
    return ep, me, core, partner, lax.rem(me + 2, ep), lax.rem(me + ep - 2, ep), lax.rem(me + 4, ep)


ROWS, ATT, FAR, META, TWIN, FRONT_COPIES = 0, 5, 17, 20, 28, 34
GIVE, RING, SWAP, LAST, MID, BACK_COPIES = 0, 4, 10, 11, 23, 35


def front_kernel(x_ref, ids_ref, pos_ref, gin_ref, gpost_ref, wr_ref, kc_hbm, vc_hbm, wq_hbm, wk_hbm, wv_hbm, wo_hbm,
                 hsum_ref, knew_ref, vnew_ref, place_ref, plan_ref, wt_slot, srt,
                 mall, meta, a_s, own, pos_row, part, relay, got, hid, send_sems, recv_sems, load_sems):
    tokens, dim = x_ref.shape
    head = wk_hbm.shape[1]
    heads = wq_hbm.shape[1] // head
    slots = kc_hbm.shape[1]
    count = plan_ref.shape[0] // 2
    ep, me, core, partner, right, left, far = ring_ids()
    tp, mt = lax.axis_size("tp"), lax.axis_index("tp")
    to_right, to_left, to_partner = {"ep": right}, {"ep": left}, {"ep": partner}
    peers = [lax.rem(me + i, ep) for i in range(1, ep)]
    barrier = pltpu.get_barrier_semaphore()
    for peer in peers:
        pl.semaphore_signal(barrier, inc=1, device_id={"ep": peer}, device_id_type=MESH)
    for peer in (lax.rem(mt + 1, tp), lax.rem(mt + tp - 1, tp)):
        pl.semaphore_signal(barrier, inc=1, device_id={"tp": peer}, device_id_type=MESH)
    links = Links(send_sems, recv_sems)
    att_sum = RowSum(links, ATT, "tp", hid, part, relay, got)
    hrow = tokens // 2

    def half(i, h):
        return at(mall, i, pl.ds(h * hrow, hrow))

    def twin(i):
        return i + 1 - 2 * lax.rem(i, 2)

    def attention(kc, vc, wq, wk, wv, wo, q_s, o_s, k_s, v_s, pcol):
        loads = [pieces_of(src, dst, load_sems, i, PARTS) for i, (src, dst) in enumerate(
            [(wq_hbm, wq), (wk_hbm, wk), (wv_hbm, wv), (kc_hbm, kc), (vc_hbm, vc), (wo_hbm, wo)])]
        wide = x_ref[...].astype(F32)
        inv = rms(wide)
        mall[me] = (wide * inv * gain_row(gpost_ref)).astype(BF16)
        a_s[...] = (wide * inv * gain_row(gin_ref)).astype(BF16)
        pl.semaphore_wait(barrier, len(peers) + 2)
        first = [(0, right), (1, left), (1, right), (0, left)]
        for n, (h, device) in enumerate(first):
            links.send(ROWS + n, half(me, h), {"ep": device})
        links.send(ROWS + len(first), at(mall, me), to_partner)

        logits = mm(mall[me], wr_ref[...])
        probs = exp_rows(logits)
        probs = probs / total(probs, 1)
        experts = logits.shape[1]
        ids = ids_ref[...].astype(F32)
        lane = iota((tokens, experts), 1).astype(F32)
        id_rows = [ids[k:k + 1, :] for k in range(2)]
        picked = [total(jnp.where(jnp.transpose(jnp.broadcast_to(row, (experts, tokens))) == lane, probs, 0.0), 1)
                  for row in id_rows]
        both = picked[0] + picked[1]
        sub = iota((8, tokens), 0)
        block = jnp.zeros((8, tokens), F32)
        wts = [jnp.transpose(jnp.broadcast_to(p / both, (tokens, tokens)))[0:8, :] for p in picked]
        for n, row in enumerate(id_rows + wts):
            block = jnp.where(sub == n, row, block)
        meta[me] = block
        for n, peer in enumerate(peers):
            links.send(META + n, at(meta, me), {"ep": peer})

        def pos_body(g, carry):
            row = iota((8, head), 0)
            acc = jnp.zeros((8, head), jnp.int32)
            for j in range(8):
                acc = jnp.where(row == j, pos_ref[g * 8 + j], acc)
            pcol[pl.ds(pl.multiple_of(g * 8, 8), 8), :] = acc
            return carry

        lax.fori_loop(0, tokens // 8, pos_body, 0)
        spot = iota((tokens, head), 1)
        power = lax.rem(spot, head // 2).astype(F32) * (-np.log(ROPE_BASE) / (head // 2))
        angles = pcol[...].astype(F32) * jnp.exp(power)
        cosine = jnp.cos(angles)
        sine = jnp.sin(angles)
        sine = jnp.where(spot < head // 2, -sine, sine)

        def rope(v):
            return (v * cosine + pltpu.roll(v, head // 2, 1) * sine).astype(BF16).astype(F32)

        for load in loads[:3]:
            finish(load)
        normed = a_s[...]
        k_s[...] = rope(mm(normed, wk[...]))
        v_s[...] = mm(normed, wv[...]).astype(BF16).astype(F32)
        knew_ref[...] = k_s[...].astype(BF16)
        vnew_ref[...] = v_s[...].astype(BF16)
        for i in range(heads // 2):
            q2 = mm(normed, wq[:, span(i, 2 * head)])
            for j in range(2):
                q_s[2 * i + j] = rope(q2[:, span(j, head)])
        for load in loads[3:5]:
            finish(load)

        def attend(g, carry):
            base = pl.multiple_of(g * 8, 8)
            slot = iota((slots, head), 0)
            pairs = []
            for new, old in ((k_s, kc), (v_s, vc)):
                pieces = [jnp.where(slot == pos_ref[g * 8 + j], new[pl.ds(base + j, 1), :], old[base + j].astype(F32))
                          for j in range(8)]
                pairs.append(jnp.concatenate([piece.astype(BF16) for piece in pieces], axis=0))
            keys, vals = pairs
            q8 = q_s[:, pl.ds(base, 8), :].reshape(heads * 8, head).astype(BF16)
            scores = nt_dot(q8, keys) * (head ** -0.5)
            each = (8, 8 * slots)
            col = iota(each, 1)
            row_pos = jnp.concatenate([pcol[pl.ds(base, 8), :]] * (8 * slots // head), axis=1)
            mask = (col // slots == iota(each, 0)) & (lax.rem(col, slots) <= row_pos)
            mask = jnp.broadcast_to(mask[None], (heads, *each)).reshape(heads * 8, 8 * slots)
            e = exp_rows(jnp.where(mask, scores, -1e30))
            o8 = mm((e / total(e, 1)).astype(BF16), vals)
            o_s[:, pl.ds(base, 8), :] = o8.reshape(heads, 8, head)
            return carry

        lax.fori_loop(0, tokens // 8, attend, 0)
        mix = jnp.concatenate([o_s[i].astype(BF16) for i in range(heads)], axis=1)
        finish(loads[5])
        for i in range(dim // COLS):
            cols = span(i, COLS)
            piece = mm(mix, wo[:, cols])
            own[:, cols] = piece
            part[:, cols] = piece.astype(BF16)
        att_sum.start()

    kv = pltpu.VMEM((tokens, head), F32)
    each_head = pltpu.VMEM((heads, tokens, head), F32)
    pl.run_scoped(
        attention, *[pltpu.VMEM(ref.shape, BF16) for ref in (kc_hbm, vc_hbm, wq_hbm, wk_hbm, wv_hbm, wo_hbm)],
        each_head, each_head, kv, kv, pltpu.VMEM((tokens, head), jnp.int32))

    cap = srt.shape[0]
    rows = cap // 2

    for n, (block, h, device) in enumerate([(left, 0, right), (right, 1, left)]):
        links.recv(ROWS + n)
        links.send(FAR + n, half(block, h), {"ep": device})
        links.send(TWIN + n, half(block, h), to_partner)

    links.recv(*range(META, META + len(peers)))
    begin = (me * count).astype(F32)
    before = (iota((tokens, tokens), 0) < iota((tokens, tokens), 1)).astype(F32).astype(BF16)
    expert = iota((count, tokens), 0).astype(F32)
    hots, ranks, local, wts = [], [], [], []
    seen = jnp.zeros((count, 1), F32)
    for s in range(ep):
        block = meta[s]
        one, two = block[0:1, :] - begin, block[1:2, :] - begin
        in_one = (one >= 0) & (one < count)
        in_two = (two >= 0) & (two < count)
        took = jnp.where(in_one, one, jnp.where(in_two, two, -1.0))
        wts.append(jnp.where(in_one, block[2:3, :], jnp.where(in_two, block[3:4, :], 0.0)))
        hot = (expert == took).astype(F32)
        hots.append(hot)
        local.append(took)
        ranks.append(mm(hot.astype(BF16), before) + seen)
        seen = seen + total(hot, 1)
    padded = jnp.broadcast_to(jnp.floor((seen + (ALIGN - 1)) * (1.0 / ALIGN)) * ALIGN, (count, tokens))
    earlier = (iota((count, count), 1) < iota((count, count), 0)).astype(F32).astype(BF16)
    start = mm(earlier, padded.astype(BF16))
    plan_ref[0:count, :] = jnp.broadcast_to(seen, (count, tokens)).astype(jnp.int32)
    plan_ref[count:, :] = start.astype(jnp.int32)
    for s in range(ep):
        place = total(hots[s] * (start + ranks[s]), 0)
        place = jnp.where(local[s] >= 0, place, -1.0)
        pos_row[s] = jnp.broadcast_to(place, (8, tokens))
        place_ref[s:s + 1, :] = place

    wt_slot[cap:, :] = jnp.zeros((WIN, tokens), F32)
    for c in range(cap // rows):
        slot = (iota((rows, tokens), 0) + c * rows).astype(F32)
        wt = jnp.zeros((rows, tokens), F32)
        for s in range(ep):
            wt = wt + jnp.where(slot == pos_row[s, 0:1, :], wts[s], 0.0)
        wt_slot[span(c, rows), :] = jnp.broadcast_to(total(wt, 1), (rows, tokens))

    def gather(one, fresh):
        two = twin(one)

        def body(c, carry):
            here = pl.ds(pl.multiple_of(c * rows, rows), rows)
            slot = (iota((rows, tokens), 0) + c * rows).astype(F32)
            pick = jnp.concatenate([(slot == pos_row[s, 0:1, :]).astype(F32).astype(BF16) for s in (one, two)], axis=1)
            for i in range(dim // COLS):
                cols = span(i, COLS)
                got_rows = mm(pick, jnp.concatenate([mall[one, :, cols], mall[two, :, cols]], axis=0))
                if not fresh:
                    got_rows = got_rows + srt[here, cols].astype(F32)
                srt[here, cols] = got_rows.astype(BF16)
            return carry

        lax.fori_loop(0, cap // rows, body, 0)

    links.recv(ROWS + 4)
    gather(me, True)
    att_sum.pass_on()
    for n, (block, h) in enumerate([(left, 1), (right, 0)]):
        links.recv(ROWS + 2 + n)
        links.send(TWIN + 2 + n, half(block, h), to_partner)
    att_sum.collect(own, x_ref)
    hsum_ref[...] = hid[att_sum.rows(mt, None), :]
    for n, block in enumerate([left, right]):
        links.recv(TWIN + n, TWIN + 2 + n)
        gather(block, False)
    for n in range(2):
        links.recv(FAR + n)
        links.send(TWIN + 4 + n, half(far, n), to_partner)
    links.recv(TWIN + 4, TWIN + 5)
    gather(far, False)
    links.drain()


def sorted_rows(ep, tokens, count):
    most = ep * tokens // 2 + count * (ALIGN - 1)
    return -(-most // (2 * tokens)) * 2 * tokens


def front(x, ids_t, pos, g_in, g_post, w_router, kc, vc, w_q, w_k, w_v, w_o, count, ep, tp):
    tokens, dim = x.shape
    head = w_k.shape[1]
    cap = sorted_rows(ep, tokens, count)
    shape = jax.ShapeDtypeStruct
    return pl.pallas_call(
        front_kernel,
        name="front",
        out_shape=(shape((tokens // tp, dim), BF16), shape((tokens, head), BF16), shape((tokens, head), BF16),
                   shape((ep, tokens), F32), shape((2 * count, tokens), jnp.int32), shape((cap + WIN, tokens), F32),
                   shape((cap, dim), BF16)),
        in_specs=[VMEM, VMEM, SMEM] + [VMEM] * 3 + [ANY] * 6,
        out_specs=(VMEM,) * 7,
        scratch_shapes=[
            pltpu.VMEM((ep, tokens, dim), BF16), pltpu.VMEM((ep, 8, tokens), F32), pltpu.VMEM((tokens, dim), BF16),
            pltpu.VMEM((tokens, dim), F32), pltpu.VMEM((ep, 8, tokens), F32), *row_sum_scratch(tokens, dim, tp),
            pltpu.SemaphoreType.DMA((FRONT_COPIES,)), pltpu.SemaphoreType.DMA((FRONT_COPIES,)),
            pltpu.SemaphoreType.DMA((6, PARTS))],
        compiler_params=pltpu.CompilerParams(collective_id=0, has_side_effects=True, vmem_limit_bytes=VMEM_LIMIT),
    )(x, ids_t, pos, g_in, g_post, w_router, kc, vc, w_q, w_k, w_v, w_o)


def expert_kernel(plan_ref, pos_ref, wt_slot, knew_ref, vnew_ref, kc_hbm, vc_hbm, srt_hbm, eg_hbm, eu_hbm, ed_hbm,
                  out_hbm, ko_hbm, vo_hbm, kc, vc, k_s, v_s, rows, out, gate_s, up_s, eg, eu, ed, rows_sem, cache_sems, w_sems):
    count = eg.shape[0]
    tokens, _, head = kc.shape
    cap, dim = srt_hbm.shape
    step = tokens // count
    news = ((k_s, kc, kc_hbm, ko_hbm), (v_s, vc, vc_hbm, vo_hbm))

    def some(e):
        return pl.ds(e * step, step)

    def comes(e):
        copies = [pltpu.make_async_copy(src.at[e], dst.at[e], w_sems.at[i, e])
                  for i, (src, dst) in enumerate([(eg_hbm, eg), (eu_hbm, eu), (ed_hbm, ed)])]
        return copies + [pltpu.make_async_copy(src.at[some(e)], buf.at[some(e)], cache_sems.at[i, e])
                         for i, (_, buf, src, _) in enumerate(news)]

    def goes(e):
        return [pltpu.make_async_copy(buf.at[some(e)], dst.at[some(e)], cache_sems.at[2 + i, e])
                for i, (_, buf, _, dst) in enumerate(news)]

    rows_copy = pltpu.make_async_copy(srt_hbm, rows.at[pl.ds(0, cap)], rows_sem.at[0])
    rows_copy.start()
    for e in range(AHEAD):
        for copy in comes(e):
            copy.start()
    k_s[...] = knew_ref[...].astype(F32)
    v_s[...] = vnew_ref[...].astype(F32)
    out[...] = jnp.zeros_like(out)
    rows_copy.wait()

    def new_rows(e):
        for new, buf, _, _ in news:
            for j in range(step):
                b = e * step + j
                spot = pos_ref[b]
                base = pl.multiple_of(spot // ALIGN * ALIGN, ALIGN)
                hit = iota((ALIGN, head), 0) == spot - base
                tile = buf[b, pl.ds(base, ALIGN), :].astype(F32)
                buf[b, pl.ds(base, ALIGN), :] = jnp.where(hit, new[pl.ds(b, 1), :], tile).astype(BF16)

    def window(e, p):
        return pl.ds(pl.multiple_of(plan_ref[count + e, 0] + p * WIN, ALIGN), WIN)

    def widen(e, here):
        x = rows[here, :]
        return nt_dot(eg[e], x), nt_dot(eu[e], x)

    def narrow(e, here, gate, up):
        act = jnp.transpose(jax.nn.silu(gate) * up).astype(BF16)
        wt = wt_slot[here, :][:, 0:1]
        for i in range(dim // COLS):
            cols = span(i, COLS)
            out[here, cols] = (mm(act, ed[e, :, cols]) * wt).astype(BF16)

    def others(e):
        def one(p, carry):
            narrow(e, window(e, p), *widen(e, window(e, p)))
            return carry

        lax.fori_loop(1, (plan_ref[e, 0] + (WIN - 1)) // WIN, one, 0)

    def begin(e):
        gate, up = widen(e, window(e, 0))
        gate_s[...] = gate
        up_s[...] = up

    finish(comes(0))
    begin(0)
    new_rows(0)
    for copy in goes(0):
        copy.start()

    def run(e, carry):
        @pl.when(e + (AHEAD - 1) < count)
        def _():
            for copy in comes(e + (AHEAD - 1)):
                copy.start()

        finish(comes(e))
        narrow(e - 1, window(e - 1, 0), gate_s[...], up_s[...])
        begin(e)
        new_rows(e)
        for copy in goes(e):
            copy.start()
        others(e - 1)
        return carry

    lax.fori_loop(1, count, run, 0)
    last = count - 1
    narrow(last, window(last, 0), gate_s[...], up_s[...])
    others(last)
    out_copy = pltpu.make_async_copy(out.at[pl.ds(0, cap)], out_hbm, rows_sem.at[1])
    out_copy.start()
    out_copy.wait()
    for e in range(count):
        finish(goes(e))


def experts(plan, pos, wt_slot, k_new, v_new, kc, vc, srt, eg_t, eu_t, ed):
    shape = jax.ShapeDtypeStruct
    count = ed.shape[0]
    room = (srt.shape[0] + WIN, srt.shape[1])
    return pl.pallas_call(
        expert_kernel,
        name="experts",
        out_shape=(shape(srt.shape, BF16), shape(kc.shape, BF16), shape(vc.shape, BF16)),
        in_specs=[SMEM, SMEM, VMEM, VMEM, VMEM] + [ANY] * 6,
        out_specs=(ANY, ANY, ANY),
        scratch_shapes=[
            pltpu.VMEM(kc.shape, BF16), pltpu.VMEM(vc.shape, BF16), pltpu.VMEM(k_new.shape, F32),
            pltpu.VMEM(v_new.shape, F32), pltpu.VMEM(room, BF16), pltpu.VMEM(room, BF16),
            pltpu.VMEM((eg_t.shape[1], WIN), F32), pltpu.VMEM((eg_t.shape[1], WIN), F32),
            *[pltpu.VMEM(w.shape, BF16) for w in (eg_t, eu_t, ed)],
            pltpu.SemaphoreType.DMA((2,)), pltpu.SemaphoreType.DMA((4, count)), pltpu.SemaphoreType.DMA((3, count))],
        compiler_params=pltpu.CompilerParams(vmem_limit_bytes=VMEM_LIMIT),
    )(plan, pos, wt_slot, k_new, v_new, kc, vc, srt, eg_t, eu_t, ed)


def back_kernel(hsum_ref, gres_ref, place_ref, srt_hbm, wg_hbm, wu_hbm, wd_hbm, out_ref,
                srt, sums, pos_col, wg, wu, wd, a_s, own, take, ring, relay_x, got_x, swap, hid,
                part_b, relay_b, got_b, full_b, send_sems, recv_sems, load_sems):
    tokens, dim = hid.shape
    cap = srt.shape[0]
    ep, me, core, partner, right, left, far = ring_ids()
    tp, mt = lax.axis_size("tp"), lax.axis_index("tp")
    to_right, to_left, to_partner = {"ep": right}, {"ep": left}, {"ep": partner}
    rows_in = pieces_of(srt_hbm, srt, load_sems, 3, 1)
    loads = [pieces_of(src, dst, load_sems, i, PARTS) for i, (src, dst) in enumerate(
        [(wg_hbm, wg), (wu_hbm, wu), (wd_hbm, wd)])]
    barrier = pltpu.get_barrier_semaphore()
    peers = [{"ep": i} for i in (partner, right, left)] + [{"tp": lax.rem(mt + i, tp)} for i in (1, tp - 1)]
    for peer in peers:
        pl.semaphore_signal(barrier, inc=1, device_id=peer, device_id_type=MESH)
    for s in range(ep):
        pos_col[s] = jnp.transpose(jnp.broadcast_to(place_ref[s:s + 1, :], (tokens, tokens)))
    pl.semaphore_wait(barrier, len(peers))
    links = Links(send_sems, recv_sems)
    mid = RowSum(links, MID, "tp", hid)
    hid[mid.rows(mt, None), :] = hsum_ref[...]
    mid.spread()
    chips = [far // 2, right // 2, left // 2, me // 2]
    halfd = dim // 2
    quart = halfd // 2
    mine = pl.ds(pl.multiple_of(core * halfd, halfd), halfd)
    other = pl.ds(pl.multiple_of((1 - core) * halfd, halfd), halfd)

    def chip_rows(chip):
        return pl.ds(chip * 2, 2)

    def add_pair(i):
        links.recv(GIVE + i)
        for q in range(2):
            cols = span(q, quart)
            ring[i, q] = (sums[i, core, :, :, cols].astype(F32) + take[i, :, :, cols].astype(F32)).astype(BF16)

    lane = iota((2 * tokens, tokens), 1).astype(F32)

    def scatter(i):
        where = pos_col[chip_rows(chips[i])].reshape(2 * tokens, tokens)
        pick = jnp.concatenate([(where == lane + j * tokens).astype(F32).astype(BF16)
                                for j in range(cap // tokens)], axis=1)
        for n in range(dim // COLS):
            cols = span(n, COLS)
            side, part = divmod(n, halfd // COLS)
            sums[i, side, :, :, span(part, COLS)] = mm(pick, srt[:, cols]).astype(BF16).reshape(2, tokens, COLS)
        links.send(GIVE + i, at(sums, i, 1 - core), to_partner, at(take, i))

    finish(rows_in[0:1])
    scatter(0)
    scatter(1)
    add_pair(0)
    links.send(RING, at(ring, 0, 0), to_right, at(relay_x, 0))
    links.send(RING + 1, at(ring, 0, 1), to_left, at(relay_x, 1))
    scatter(2)
    add_pair(1)
    links.send(RING + 2, at(ring, 1, 1), to_right, at(got_x, 0, 1))
    scatter(3)
    add_pair(2)
    links.send(RING + 3, at(ring, 2, 0), to_left, at(got_x, 1, 0))
    add_pair(3)
    mid.forward()
    mid.finish()
    wide = hid[...].astype(F32)
    a_s[...] = (wide * rms(wide) * gain_row(gres_ref)).astype(BF16)
    for load in loads[:2]:
        finish(load)
    acts = []
    for i in range(wg.shape[1] // COLS):
        cols = span(i, COLS)
        acts.append((jax.nn.silu(mm(a_s[...], wg[:, cols])) * mm(a_s[...], wu[:, cols])).astype(BF16))
    act = jnp.concatenate(acts, axis=1)
    finish(loads[2])
    for i in range(dim // COLS):
        cols = span(i, COLS)
        own[:, cols] = mm(act, wd[:, cols])

    for n, (dest, device, side) in enumerate([(1, to_right, 0), (2, to_left, 1)]):
        links.recv(RING + n)
        relay_x[2 + n] = (ring[dest, n].astype(F32) + relay_x[n].astype(F32)).astype(BF16)
        links.send(RING + 4 + n, at(relay_x, 2 + n), device, at(got_x, side, n))
    links.recv(*range(RING + 2, SWAP))

    def arrived(j):
        return jnp.concatenate(
            [ring[3, q, j].astype(F32) + got_x[0, q, j].astype(F32) + got_x[1, q, j].astype(F32)
             for q in range(2)], axis=1)

    swap[0] = arrived(1 - core).astype(BF16)
    links.send(SWAP, at(swap, 0), to_partner, at(swap, 1))
    last = RowSum(links, LAST, "tp", full_b, part_b, relay_b, got_b)
    own[:, mine] += arrived(core)
    part_b[:, mine] = own[:, mine].astype(BF16)
    links.recv(SWAP)
    own[:, other] += swap[1].astype(F32)
    part_b[:, other] = own[:, other].astype(BF16)
    last.start()
    last.pass_on()
    last.collect(own, hid)
    last.spread()
    last.forward()
    last.finish()
    out_ref[...] = full_b[...]
    links.drain()


def back(h_sum, g_res, place, srt, w_gate, w_up, w_down, tp):
    tokens, dim = h_sum.shape[0] * tp, h_sum.shape[1]
    ep = place.shape[0]
    chips, halfd, quart = ep // 2, dim // 2, dim // 4
    return pl.pallas_call(
        back_kernel,
        name="back",
        out_shape=jax.ShapeDtypeStruct((tokens, dim), BF16),
        in_specs=[VMEM, VMEM, VMEM] + [ANY] * 4,
        out_specs=VMEM,
        scratch_shapes=[
            pltpu.VMEM(srt.shape, BF16), pltpu.VMEM((chips, 2, 2, tokens, halfd), BF16), pltpu.VMEM((ep, tokens, tokens), F32),
            *[pltpu.VMEM(w.shape, BF16) for w in (w_gate, w_up, w_down)],
            pltpu.VMEM((tokens, dim), BF16), pltpu.VMEM((tokens, dim), F32),
            pltpu.VMEM((chips, 2, tokens, halfd), BF16), pltpu.VMEM((chips, 2, 2, tokens, quart), BF16),
            pltpu.VMEM((4, 2, tokens, quart), BF16), pltpu.VMEM((2, 2, 2, tokens, quart), BF16),
            pltpu.VMEM((2, tokens, halfd), BF16), pltpu.VMEM((tokens, dim), BF16), *row_sum_scratch(tokens, dim, tp),
            pltpu.SemaphoreType.DMA((BACK_COPIES,)), pltpu.SemaphoreType.DMA((BACK_COPIES,)),
            pltpu.SemaphoreType.DMA((4, PARTS))],
        compiler_params=pltpu.CompilerParams(collective_id=1, has_side_effects=True, vmem_limit_bytes=VMEM_LIMIT),
    )(h_sum, g_res, place, srt, w_gate, w_up, w_down)


def solution(mesh):
    ep, tp = mesh.shape['ep'], mesh.shape['tp']
    row_spec = P(('dp', 'ep'), None)
    cache_spec = P(('dp', 'ep'), None, 'tp', None)
    col_split = P(None, 'tp')
    row_split = P('tp', None)
    in_specs = (row_spec, P(('dp', 'ep')), row_spec, cache_spec, cache_spec, P(None), P(None), P(None), col_split, col_split, col_split, row_split, col_split, col_split, row_split, P(None, None), P('ep', None, 'tp'), P('ep', None, 'tp'), P('ep', 'tp', None))
    out_specs = (row_spec, cache_spec, cache_spec)

    def local_layer(hidden_in, positions, expert_ids, k_cache, v_cache, norm_in, norm_res, norm_post, w_q, w_k, w_v, w_o, w_gate, w_up, w_down, w_router, e_gate, e_up, e_down):
        tokens, dim = hidden_in.shape
        slots, head = k_cache.shape[1], k_cache.shape[3]
        kc, vc = (cache.reshape(tokens, slots, head) for cache in (k_cache, v_cache))
        h_sum, k_new, v_new, place, plan, wt_slot, srt = front(
            hidden_in, expert_ids.T, positions, norm_in, norm_post, w_router, kc, vc, w_q, w_k, w_v, w_o,
            e_down.shape[0], ep, tp)
        out, k_out, v_out = experts(
            plan, positions, wt_slot, k_new, v_new, kc, vc, srt, jnp.swapaxes(e_gate, 1, 2), jnp.swapaxes(e_up, 1, 2), e_down)
        hidden_out = back(h_sum, norm_res, place, out, w_gate, w_up, w_down, tp)
        return hidden_out, k_out.reshape(k_cache.shape), v_out.reshape(v_cache.shape)

    return jax.shard_map(local_layer, mesh=mesh, in_specs=in_specs, out_specs=out_specs, check_vma=False)
```
